8 devices in a mesh: dp: 1 (over z), ep: 8 (over y, x, core).
Axes of the slice: x: 2, y: 2, z: 1, core: 2. Of those that a mesh axis runs over, the one named last changes fastest.
Arguments:
- hidden: bfloat16 [2048, 2560], P(('dp', 'ep'))
- norm_gain: bfloat16 [2560], replicated
- w_gate: bfloat16 [2560, 64], replicated
- w1_shared: bfloat16 [2560, 3072], replicated
- w3_shared: bfloat16 [2560, 3072], replicated
- w2_shared: bfloat16 [3072, 2560], replicated
- w1_experts: bfloat16 [64, 2560, 1536], P('ep')
- w3_experts: bfloat16 [64, 2560, 1536], P('ep')
- w2_experts: bfloat16 [64, 1536, 2560], P('ep')
- topk_ids: int32 [2048, 6], P(('dp', 'ep'))
Outputs:
- output: bfloat16 [2048, 2560], P(('dp', 'ep'))
All inputs are finite; a program needn't handle non-finite values.
Results may differ from the reference program's by a relative error of at most 0.00584073.
Values are sent between devices in bfloat16 or wider.
A program may use at most 1 GiB of HBM per device.

```python
import jax
import jax.numpy as jnp
from jax import lax

HIDDEN = 2560
EXPERTS = 64
EXPERT_FF = 1536
SHARED_FF = 3072
TOP_K = 6
TOKENS_DEV = 256
TOKENS = 2048
GROUPS = 8
TOP_GROUPS = 3
ROUTE_SCALE = 16
NORM_EPS = 1e-6
GROUP_SIZE = EXPERTS // GROUPS


def draw_routing(route_key):
    blocks = TOKENS // TOKENS_DEV
    half_block = TOKENS_DEV // 2
    key_hot, key_cycle, key_perm, key_score, key_pick = jax.random.split(route_key, 5)
    hot_group = jax.random.randint(key_hot, (blocks, 1, 1), 0, GROUPS)
    cycle_off = jax.random.randint(key_cycle, (blocks, 1, 1), 0, GROUPS - 1)
    perm_keys = jax.random.split(key_perm, blocks)
    rank_in = jax.vmap(lambda sub_key: jax.random.permutation(sub_key, TOKENS_DEV))(perm_keys)[:, :, None]
    first_set = (rank_in * (TOP_GROUPS - 1) + jnp.arange(TOP_GROUPS - 1) + cycle_off) % (GROUPS - 1)
    first_groups = jnp.concatenate([jnp.broadcast_to(hot_group, (blocks, TOKENS_DEV, 1)), (hot_group + 1 + first_set) % GROUPS], axis=2)
    second_set = (rank_in * TOP_GROUPS + jnp.arange(TOP_GROUPS) + cycle_off) % (GROUPS - 1)
    second_groups = (hot_group + 1 + second_set) % GROUPS
    chosen = jnp.where(rank_in < half_block, first_groups, second_groups).reshape(TOKENS, TOP_GROUPS)
    scores = jax.random.randint(key_score, (TOKENS, TOP_GROUPS, GROUP_SIZE), 0, 2 ** 19) * 512
    scores = scores + jnp.arange(TOP_GROUPS * GROUP_SIZE).reshape(TOP_GROUPS, GROUP_SIZE)
    pick_idx = jax.random.randint(key_pick, (TOKENS, TOP_GROUPS, 1), 0, GROUP_SIZE)
    scores = scores + jnp.where(jnp.arange(GROUP_SIZE) == pick_idx, 2 ** 29, 0)
    cand_idx = lax.top_k(scores.reshape(TOKENS, TOP_GROUPS * GROUP_SIZE), TOP_K)[1]
    group_of = jnp.take_along_axis(chosen, cand_idx // GROUP_SIZE, axis=1)
    return (group_of * GROUP_SIZE + cand_idx % GROUP_SIZE).astype(jnp.int32)


def normal_bf16(sub_key, shape_in, scale_by):
    return (scale_by * jax.random.normal(sub_key, shape_in, jnp.float32)).astype(jnp.bfloat16)


def setup_inputs(seed: int = 0, part: int = 0) -> dict:
    part_key = jax.random.fold_in(jax.random.key(seed), part)
    weight_keys = jax.random.split(jax.random.key(seed + 1), 8)
    hidden = normal_bf16(jax.random.fold_in(part_key, 1), (TOKENS, HIDDEN), 0.5)
    norm_gain = (1.0 + 0.2 * jax.random.normal(weight_keys[0], (HIDDEN,), jnp.float32)).astype(jnp.bfloat16)
    w_gate = normal_bf16(weight_keys[1], (HIDDEN, EXPERTS), HIDDEN ** -0.5)
    w1_shared = normal_bf16(weight_keys[2], (HIDDEN, SHARED_FF), HIDDEN ** -0.5)
    w3_shared = normal_bf16(weight_keys[3], (HIDDEN, SHARED_FF), HIDDEN ** -0.5)
    w2_shared = normal_bf16(weight_keys[4], (SHARED_FF, HIDDEN), SHARED_FF ** -0.5)
    w1_experts = normal_bf16(weight_keys[5], (EXPERTS, HIDDEN, EXPERT_FF), HIDDEN ** -0.5)
    w3_experts = normal_bf16(weight_keys[6], (EXPERTS, HIDDEN, EXPERT_FF), HIDDEN ** -0.5)
    w2_experts = normal_bf16(weight_keys[7], (EXPERTS, EXPERT_FF, HIDDEN), EXPERT_FF ** -0.5)
    topk_ids = draw_routing(jax.random.fold_in(part_key, 2))
    return dict(hidden=hidden, norm_gain=norm_gain, w_gate=w_gate, w1_shared=w1_shared, w3_shared=w3_shared, w2_shared=w2_shared, w1_experts=w1_experts, w3_experts=w3_experts, w2_experts=w2_experts, topk_ids=topk_ids)


def rms_norm(hidden, norm_gain):
    rows_f = hidden.astype(jnp.float32)
    inv_rms = lax.rsqrt(jnp.mean(rows_f * rows_f, axis=-1, keepdims=True) + NORM_EPS)
    return (rows_f * inv_rms * norm_gain.astype(jnp.float32)).astype(jnp.bfloat16)


def swiglu(rows_in, w_up, w_lin, w_down):
    gate_act = jnp.dot(rows_in, w_up, preferred_element_type=jnp.float32)
    lin_act = jnp.dot(rows_in, w_lin, preferred_element_type=jnp.float32)
    inner_act = (jax.nn.silu(gate_act) * lin_act).astype(jnp.bfloat16)
    return jnp.dot(inner_act, w_down, preferred_element_type=jnp.float32).astype(jnp.bfloat16)


def reference(hidden, norm_gain, w_gate, w1_shared, w3_shared, w2_shared, w1_experts, w3_experts, w2_experts, topk_ids):
    normed = rms_norm(hidden, norm_gain)
    gate_probs = jax.nn.softmax(jnp.dot(normed, w_gate, preferred_element_type=jnp.float32), axis=-1)
    gate_wts = ROUTE_SCALE * jnp.take_along_axis(gate_probs, topk_ids, axis=1)
    shared_out = swiglu(normed, w1_shared, w3_shared, w2_shared)

    def expert_step(routed_acc, expert_in):
        w_up, w_lin, w_down, expert_id = expert_in
        column = jnp.sum(jnp.where(topk_ids == expert_id, gate_wts, 0.0), axis=1)
        expert_out = swiglu(normed, w_up, w_lin, w_down)
        return routed_acc + column[:, None] * expert_out.astype(jnp.float32), None

    routed = lax.scan(expert_step, jnp.zeros(hidden.shape, jnp.float32), (w1_experts, w3_experts, w2_experts, jnp.arange(EXPERTS)))[0]
    return (hidden.astype(jnp.float32) + shared_out.astype(jnp.float32) + routed).astype(jnp.bfloat16)
```

```python
import functools

import jax
import jax.numpy as jnp
from jax import lax
from jax.experimental import pallas as pl
from jax.experimental.pallas import tpu as pltpu
from jax.sharding import PartitionSpec as P

ROUTE_SCALE = 16
NORM_EPS = 1e-6
D = 2560
FF = 1536
EXPERTS = 64
NE = 8
NSB = 4
SB = 512
G = 16
TM = 256
XG = 432
XR = XG * G
SBR = 1792
FC = 512
NF = FF // FC
VMEM_LIMIT = 66000000
BF16 = jnp.bfloat16
F32 = jnp.float32


def rms_norm(hidden, norm_gain):
    rows_f = hidden.astype(F32)
    inv_rms = lax.rsqrt(jnp.mean(rows_f * rows_f, axis=-1, keepdims=True) + NORM_EPS)
    return (rows_f * inv_rms * norm_gain.astype(F32)).astype(BF16)


def offsets(cnt_ref, ng, eoff, est, boff, nsb_g):
    run = jnp.int32(0)
    for e in range(NE):
        est[e] = run
        for s in range(NSB):
            n = (cnt_ref[s, e] + (G - 1)) // G
            ng[s * NE + e] = n
            eoff[s * NE + e] = run
            run = run + n
    est[NE] = run
    for s in range(NSB):
        b = jnp.int32(0)
        for e in range(NE):
            boff[s * NE + e] = b
            b = b + ng[s * NE + e]
        nsb_g[s] = b


def up_kernel(cnt_ref, rank_ref, ball, w1, w3, h_out, xs, bbuf, pbuf, tbuf, wbuf, hbuf, ng, eoff, est, boff, nsb_g, dst, bsem, wsem, hsem):
    def w_copies(step, slot):
        e = step // NF
        f = step % NF
        cols = pl.ds(pl.multiple_of(f * FC, FC), FC)
        return (pltpu.make_async_copy(w1.at[e, :, cols], wbuf.at[slot, 0], wsem.at[slot, 0]),
                pltpu.make_async_copy(w3.at[e, :, cols], wbuf.at[slot, 1], wsem.at[slot, 1]))

    def b_copy(s, slot):
        return pltpu.make_async_copy(ball.at[pl.ds(s * SB, SB), :], bbuf.at[slot], bsem.at[slot])

    b_copy(0, 0).start()
    for c in w_copies(0, 0):
        c.start()
    for c in w_copies(1, 1):
        c.start()
    offsets(cnt_ref, ng, eoff, est, boff, nsb_g)
    rows16 = lax.broadcasted_iota(jnp.int32, (G, SB), 0)

    for s in range(NSB):
        slot = s % 2
        if s + 1 < NSB:
            b_copy(s + 1, 1 - slot).start()
        for e in range(NE):
            rk = jnp.broadcast_to(rank_ref[s, e:e + 1, :], (G, SB))

            def build(g, _, s=s, e=e, rk=rk):
                k = boff[s * NE + e] + g
                dst[k] = eoff[s * NE + e] + g
                hit = jnp.where(rk == rows16 + g * G, 1.0, 0.0)
                pbuf[pl.ds(pl.multiple_of(k * G, G), G), :] = hit.astype(BF16)
                return 0

            lax.fori_loop(0, ng[s * NE + e], build, 0)
        b_copy(s, slot).wait()

        def tile(m, _, s=s, slot=slot):
            prow = pbuf[pl.ds(pl.multiple_of(m * TM, TM), TM), :]
            for n in range(D // 512):
                cols = slice(n * 512, (n + 1) * 512)
                tbuf[:, cols] = jnp.dot(prow, bbuf[slot, :, cols], preferred_element_type=F32).astype(BF16)

            def put(j, _):
                row = pl.multiple_of(dst[m * (TM // G) + j] * G, G)
                xs[pl.ds(row, G), :] = tbuf[pl.ds(pl.multiple_of(j * G, G), G), :]
                return 0

            lax.fori_loop(0, jnp.minimum(TM // G, nsb_g[s] - m * (TM // G)), put, 0)
            return 0

        lax.fori_loop(0, (nsb_g[s] + TM // G - 1) // (TM // G), tile, 0)

    def h_copy(hs, row, col, size):
        return pltpu.make_async_copy(hbuf.at[hs, pl.ds(0, size), :], h_out.at[pl.ds(row, size), pl.ds(col, FC)], hsem.at[0])

    def step(st, k):
        slot = st % 2
        e = st // NF
        col = pl.multiple_of((st % NF) * FC, FC)
        for c in w_copies(st, slot):
            c.wait()
        base = est[e] * G
        rows = est[e + 1] * G - base

        def work(row, size, k):
            row = pl.multiple_of(row, G)
            hs = k % 2
            x = xs[pl.ds(row, size), :]
            gate = jnp.dot(x, wbuf[slot, 0], preferred_element_type=F32)
            lin = jnp.dot(x, wbuf[slot, 1], preferred_element_type=F32)
            hbuf[hs, pl.ds(0, size), :] = (jax.nn.silu(gate) * lin).astype(BF16)
            h_copy(hs, row, col, size).start()
            h_copy(hs, row, col, size).wait()

        full = rows // TM

        def body(m, k):
            work(base + m * TM, TM, k)
            return k + 1

        k = lax.fori_loop(0, full, body, k)
        rem = rows - full * TM
        at = base + full * TM
        for size in (64, 128, 192, 256):
            @pl.when((rem > size - 64) & (rem <= size))
            def _(size=size):
                work(at, size, k)

        @pl.when(st + 2 < NE * NF)
        def _():
            for c in w_copies(st + 2, slot):
                c.start()

        return k + 1

    lax.fori_loop(0, NE * NF, step, jnp.int32(0))


def up_call(cnt, rank, ball, w1, w3):
    any_spec = pl.BlockSpec(memory_space=pl.ANY)
    return pl.pallas_call(
        up_kernel,
        out_shape=jax.ShapeDtypeStruct((XR, FF), BF16),
        in_specs=[pl.BlockSpec(memory_space=pltpu.SMEM), pl.BlockSpec(memory_space=pltpu.VMEM), any_spec, any_spec, any_spec],
        out_specs=any_spec,
        scratch_shapes=[
            pltpu.VMEM((XR, D), BF16),
            pltpu.VMEM((2, SB, D), BF16),
            pltpu.VMEM((SBR, SB), BF16),
            pltpu.VMEM((TM, D), BF16),
            pltpu.VMEM((2, 2, D, FC), BF16),
            pltpu.VMEM((2, TM, FC), BF16),
            pltpu.SMEM((NSB * NE,), jnp.int32),
            pltpu.SMEM((NSB * NE,), jnp.int32),
            pltpu.SMEM((NE + 1,), jnp.int32),
            pltpu.SMEM((NSB * NE,), jnp.int32),
            pltpu.SMEM((NSB,), jnp.int32),
            pltpu.SMEM((SBR // G,), jnp.int32),
            pltpu.SemaphoreType.DMA((2,)),
            pltpu.SemaphoreType.DMA((2, 2)),
            pltpu.SemaphoreType.DMA((1,)),
        ],
        compiler_params=pltpu.CompilerParams(vmem_limit_bytes=VMEM_LIMIT),
        cost_estimate=pl.CostEstimate(flops=48_000_000_000, bytes_accessed=140_000_000, transcendentals=0),
        name="up",
    )(cnt, rank, ball, w1, w3)


def down_kernel(c0, cw, cnt_ref, core_ref, rank_ref, wt_ref, h, w2, mine, theirs,
                ebuf, kbuf, pbuf, hbuf, wbuf, abuf, wsplit, ng, eoff, est, boff, nsb_g, trow, hsem, wsem, osem):
    def w_copy(e, slot):
        return pltpu.make_async_copy(w2.at[e, :, pl.ds(c0, cw)], wbuf.at[slot], wsem.at[slot])

    def h_copy(t, slot):
        return pltpu.make_async_copy(h.at[pl.ds(pl.multiple_of(trow[t] * G, G), TM), :], hbuf.at[slot], hsem.at[slot])

    for e in range(3):
        w_copy(e, e).start()
    offsets(cnt_ref, ng, eoff, est, boff, nsb_g)
    trow[0] = 0
    h_copy(0, 0).start()

    def tiles_of(e):
        return jnp.maximum((est[e + 1] - est[e] + TM // G - 1) // (TM // G), 1)

    nt = jnp.int32(0)
    for e in range(NE):
        def note(m, _, e=e, nt=nt):
            trow[nt + m] = est[e] + m * (TM // G)
            return 0

        lax.fori_loop(0, tiles_of(e), note, 0)
        nt = nt + tiles_of(e)
    for s in range(NSB):
        w = wt_ref[s]
        hi = w.astype(BF16).astype(F32)
        mid = (w - hi).astype(BF16).astype(F32)
        wsplit[0, s] = hi
        wsplit[1, s] = mid
        wsplit[2, s] = w - hi - mid

    def expert(e, t):
        ws = e % 3
        w_copy(e, ws).wait()

        def body(m, t):
            slot = t % 2

            @pl.when(t + 1 < nt)
            def _():
                h_copy(t + 1, 1 - slot).start()

            h_copy(t, slot).wait()
            row = pl.multiple_of(trow[t] * G, G)
            ebuf[pl.ds(row, TM), :] = jnp.dot(hbuf[slot], wbuf[ws], preferred_element_type=F32).astype(BF16)
            return t + 1

        t = lax.fori_loop(0, tiles_of(e), body, t)

        @pl.when(e + 3 < NE)
        def _():
            w_copy(e + 3, ws).start()

        return t

    lax.fori_loop(0, NE, expert, jnp.int32(0))

    rows16 = lax.broadcasted_iota(jnp.int32, (G, SB), 0)
    core = core_ref[0]
    for s in range(NSB):
        for e in range(NE):
            rk = jnp.broadcast_to(rank_ref[s, e:e + 1, :], (G, SB))
            parts = [jnp.broadcast_to(wsplit[i, s, e:e + 1, :], (G, SB)) for i in range(3)]

            def build(g, _, s=s, e=e, rk=rk, parts=parts):
                row = pl.multiple_of((boff[s * NE + e] + g) * G, G)
                src = pl.multiple_of((eoff[s * NE + e] + g) * G, G)
                hit = rk == rows16 + g * G
                for i in range(3):
                    pbuf[i, pl.ds(row, G), :] = jnp.where(hit, parts[i], 0.0).astype(BF16)
                kbuf[pl.ds(row, G), :] = ebuf[pl.ds(src, G), :]
                return 0

            lax.fori_loop(0, ng[s * NE + e], build, 0)
        nk = (nsb_g[s] + TM // G - 1) // (TM // G)

        def clear(g, _):
            row = pl.multiple_of(g * G, G)
            for i in range(3):
                pbuf[i, pl.ds(row, G), :] = jnp.zeros((G, SB), BF16)
            kbuf[pl.ds(row, G), :] = jnp.zeros((G, cw), BF16)
            return 0

        lax.fori_loop(nsb_g[s], nk * (TM // G), clear, 0)
        slot = s % 2
        if s >= 2:
            for c in out_copies(s - 2, slot, core, abuf, mine, theirs, osem, core_ref):
                c.wait()
        abuf[slot] = jnp.zeros((SB, cw), F32)

        def tile(kt, _, slot=slot):
            rows = pl.ds(pl.multiple_of(kt * TM, TM), TM)
            ek = kbuf[rows, :]
            tot = abuf[slot]
            for i in range(3):
                tot = tot + lax.dot_general(pbuf[i, rows, :], ek, (((0,), (0,)), ((), ())), preferred_element_type=F32)
            abuf[slot] = tot
            return 0

        lax.fori_loop(0, nk, tile, 0)
        for c in out_copies(s, slot, core, abuf, mine, theirs, osem, core_ref):
            c.start()
    for s in (NSB - 2, NSB - 1):
        for c in out_copies(s, s % 2, core, abuf, mine, theirs, osem, core_ref):
            c.wait()


def out_copies(s, slot, core, abuf, mine, theirs, osem, core_ref):
    rel = core_ref[1 + s]
    keep = pl.multiple_of(core * 256, 256)
    give = pl.multiple_of(256 - core * 256, 256)
    return (pltpu.make_async_copy(abuf.at[slot, pl.ds(give, 256), :], theirs.at[rel], osem.at[slot, 1]),
            pltpu.make_async_copy(abuf.at[slot, pl.ds(keep, 256), :], mine.at[rel], osem.at[slot, 0]))


def down_call(c0, cw, cnt, core, rank, wts, h, w2):
    any_spec = pl.BlockSpec(memory_space=pl.ANY)
    smem = pl.BlockSpec(memory_space=pltpu.SMEM)
    vmem = pl.BlockSpec(memory_space=pltpu.VMEM)
    out = jax.ShapeDtypeStruct((NSB, 256, cw), F32)
    return pl.pallas_call(
        functools.partial(down_kernel, c0, cw),
        out_shape=(out, out),
        in_specs=[smem, smem, vmem, vmem, any_spec, any_spec],
        out_specs=(any_spec, any_spec),
        scratch_shapes=[
            pltpu.VMEM((XR, cw), BF16),
            pltpu.VMEM((SBR, cw), BF16),
            pltpu.VMEM((3, SBR, SB), BF16),
            pltpu.VMEM((2, TM, FF), BF16),
            pltpu.VMEM((3, FF, cw), BF16),
            pltpu.VMEM((2, SB, cw), F32),
            pltpu.VMEM((3, NSB, NE, SB), F32),
            pltpu.SMEM((NSB * NE,), jnp.int32),
            pltpu.SMEM((NSB * NE,), jnp.int32),
            pltpu.SMEM((NE + 1,), jnp.int32),
            pltpu.SMEM((NSB * NE,), jnp.int32),
            pltpu.SMEM((NSB,), jnp.int32),
            pltpu.SMEM((64,), jnp.int32),
            pltpu.SemaphoreType.DMA((2,)),
            pltpu.SemaphoreType.DMA((3,)),
            pltpu.SemaphoreType.DMA((2, 2)),
        ],
        compiler_params=pltpu.CompilerParams(vmem_limit_bytes=40000000),
        cost_estimate=pl.CostEstimate(flops=10_000_000_000, bytes_accessed=24_000_000, transcendentals=0),
        name="down%d" % c0,
    )(cnt, core, rank, wts, h, w2)


def swiglu(rows_in, w_up, w_lin, w_down):
    gate_act = jnp.dot(rows_in, w_up, preferred_element_type=F32)
    lin_act = jnp.dot(rows_in, w_lin, preferred_element_type=F32)
    inner_act = (jax.nn.silu(gate_act) * lin_act).astype(BF16)
    return jnp.dot(inner_act, w_down, preferred_element_type=F32).astype(BF16)


CHUNKS = ((0, 512), (512, 512), (1024, 512), (1536, 512), (2048, 512))


def return_sum(mine, theirs):
    def index(y, x, c):
        return (y * 2 + x) * 2 + c

    every = [(y, x, c) for y in range(2) for x in range(2) for c in range(2)]
    to_core = [(index(y, x, c), index(y, x, 1 - c)) for y, x, c in every]
    to_x = [(index(y, x, c), index(y, 1 - x, c)) for y, x, c in every]
    to_y = [(index(y, x, c), index(1 - y, x, c)) for y, x, c in every]
    got = lax.ppermute(theirs, 'ep', to_core)
    own = mine + got
    half = 128
    got_x = lax.ppermute(jnp.stack([own[1, :half], own[3, :half]]), 'ep', to_x)
    got_y = lax.ppermute(jnp.stack([own[2, half:], own[3, half:]]), 'ep', to_y)
    last_y = lax.ppermute(own[2, :half] + got_x[1], 'ep', to_y)
    last_x = lax.ppermute(own[1, half:] + got_y[1], 'ep', to_x)
    top = own[0, :half] + got_x[0] + last_y
    low = own[0, half:] + got_y[0] + last_x
    return jnp.concatenate([top, low], axis=0)


def solution(mesh):
    tok_spec = P(('dp', 'ep'), None)
    expert_spec = P('ep', None, None)

    def local_fn(hidden, norm_gain, w_gate, w1_shared, w3_shared, w2_shared, w1_experts, w3_experts, w2_experts, topk_ids):
        normed = rms_norm(hidden, norm_gain)
        probs = jax.nn.softmax(jnp.dot(normed, w_gate, preferred_element_type=F32), axis=-1)
        chosen = jnp.any(topk_ids[:, :, None] == jnp.arange(EXPERTS), axis=1)
        gate_wts = jnp.where(chosen, ROUTE_SCALE * probs, -1.0)
        ball = lax.all_gather(normed, 'ep', axis=0, tiled=True)
        wall = lax.all_gather(gate_wts, 'ep', axis=0, tiled=True)
        me = lax.axis_index('ep')
        wsb = lax.dynamic_slice_in_dim(wall, me * NE, NE, axis=1).reshape(NSB, SB, NE).transpose(0, 2, 1)
        sel = wsb >= 0.0
        cnt = jnp.sum(sel, axis=2, dtype=jnp.int32)
        before = jnp.arange(SB)[:, None] < jnp.arange(SB)[None, :]
        rank = jnp.einsum('set,tu->seu', sel.astype(BF16), before.astype(BF16), preferred_element_type=F32)
        rank = jnp.where(sel, rank.astype(jnp.int32), -1)
        chip = me // 2
        core = jnp.concatenate([(me % 2)[None], (jnp.arange(NSB) // 2 != chip // 2) * 2 + (jnp.arange(NSB) % 2 != chip % 2)]).astype(jnp.int32)
        shared_out = swiglu(normed, w1_shared, w3_shared, w2_shared)
        h = up_call(cnt, rank, ball, w1_experts, w3_experts)
        cols = []
        for c0, cw in CHUNKS:
            mine, theirs = down_call(c0, cw, cnt, core, rank, wsb, h, w2_experts)
            cols.append(return_sum(mine, theirs))
        routed = jnp.concatenate(cols, axis=1)
        return (hidden.astype(F32) + shared_out.astype(F32) + routed).astype(BF16)

    return jax.shard_map(local_fn, mesh=mesh, in_specs=(tok_spec, P(), P(), P(), P(), P(), expert_spec, expert_spec, expert_spec, tok_spec), out_specs=tok_spec, check_vma=False)
```

```python
import functools

import jax
import jax.numpy as jnp
from jax import lax
from jax.experimental import pallas as pl
from jax.experimental.pallas import tpu as pltpu
from jax.sharding import PartitionSpec as P

ROUTE_SCALE = 16
NORM_EPS = 1e-6
D = 2560
FF = 1536
EXPERTS = 64
NE = 8
NSB = 4
SB = 512
G = 16
TM = 256
XG = 432
XR = XG * G
SBR = 1792
FC = 512
NF = FF // FC
T = 256
SHARED = 3072
SF = 256
CW = 512
RC = 256
NC = D // RC
VMEM_LIMIT = 66000000
BF16 = jnp.bfloat16
F32 = jnp.float32


def rms_norm(hidden, norm_gain):
    rows_f = hidden.astype(F32)
    inv_rms = lax.rsqrt(jnp.mean(rows_f * rows_f, axis=-1, keepdims=True) + NORM_EPS)
    return (rows_f * inv_rms * norm_gain.astype(F32)).astype(BF16)


def offsets(cnt_ref, ng, eoff, est, boff, nsb_g):
    run = jnp.int32(0)
    for e in range(NE):
        est[e] = run
        for s in range(NSB):
            n = (cnt_ref[s, e] + (G - 1)) // G
            ng[s * NE + e] = n
            eoff[s * NE + e] = run
            run = run + n
    est[NE] = run
    for s in range(NSB):
        b = jnp.int32(0)
        for e in range(NE):
            boff[s * NE + e] = b
            b = b + ng[s * NE + e]
        nsb_g[s] = b


def up_kernel(cnt_ref, rank_ref, ball, w1, w3, h_out, xs, bbuf, pbuf, tbuf, wbuf, hbuf, ng, eoff, est, boff, nsb_g, dst, last, bsem, wsem, hsem):
    def w_copies(step, slot):
        e = step // NF
        f = step % NF
        cols = pl.ds(pl.multiple_of(f * FC, FC), FC)
        return (pltpu.make_async_copy(w1.at[e, :, cols], wbuf.at[slot, 0], wsem.at[slot, 0]),
                pltpu.make_async_copy(w3.at[e, :, cols], wbuf.at[slot, 1], wsem.at[slot, 1]))

    def b_copy(s, slot):
        return pltpu.make_async_copy(ball.at[pl.ds(s * SB, SB), :], bbuf.at[slot], bsem.at[slot])

    b_copy(0, 0).start()
    for c in w_copies(0, 0):
        c.start()
    for c in w_copies(1, 1):
        c.start()
    offsets(cnt_ref, ng, eoff, est, boff, nsb_g)
    rows16 = lax.broadcasted_iota(jnp.int32, (G, SB), 0)

    for s in range(NSB):
        slot = s % 2
        if s + 1 < NSB:
            b_copy(s + 1, 1 - slot).start()
        for e in range(NE):
            rk = jnp.broadcast_to(rank_ref[s, e:e + 1, :], (G, SB))

            def build(g, _, s=s, e=e, rk=rk):
                k = boff[s * NE + e] + g
                dst[k] = eoff[s * NE + e] + g
                hit = jnp.where(rk == rows16 + g * G, 1.0, 0.0)
                pbuf[pl.ds(pl.multiple_of(k * G, G), G), :] = hit.astype(BF16)
                return 0

            lax.fori_loop(0, ng[s * NE + e], build, 0)
        b_copy(s, slot).wait()

        def tile(m, _, s=s, slot=slot):
            prow = pbuf[pl.ds(pl.multiple_of(m * TM, TM), TM), :]
            for n in range(D // 512):
                cols = slice(n * 512, (n + 1) * 512)
                tbuf[:, cols] = jnp.dot(prow, bbuf[slot, :, cols], preferred_element_type=F32).astype(BF16)

            def put(j, _):
                row = pl.multiple_of(dst[m * (TM // G) + j] * G, G)
                xs[pl.ds(row, G), :] = tbuf[pl.ds(pl.multiple_of(j * G, G), G), :]
                return 0

            lax.fori_loop(0, jnp.minimum(TM // G, nsb_g[s] - m * (TM // G)), put, 0)
            return 0

        lax.fori_loop(0, (nsb_g[s] + TM // G - 1) // (TM // G), tile, 0)

    def h_copy(hs, row, col, size):
        return pltpu.make_async_copy(hbuf.at[hs, pl.ds(0, size), :], h_out.at[pl.ds(row, size), pl.ds(col, FC)], hsem.at[0])

    def wait_h(quarters):
        for q in range(1, 5):
            @pl.when(quarters == q)
            def _(q=q):
                h_copy(0, 0, 0, q * 64).wait()

    def step(st, k):
        slot = st % 2
        e = st // NF
        col = pl.multiple_of((st % NF) * FC, FC)
        for c in w_copies(st, slot):
            c.wait()
        base = est[e] * G
        rows = est[e + 1] * G - base

        def work(row, size, k):
            row = pl.multiple_of(row, G)
            hs = k % 2
            x = xs[pl.ds(row, size), :]
            gate = jnp.dot(x, wbuf[slot, 0], preferred_element_type=F32)
            lin = jnp.dot(x, wbuf[slot, 1], preferred_element_type=F32)
            hbuf[hs, pl.ds(0, size), :] = (jax.nn.silu(gate) * lin).astype(BF16)

            @pl.when(k > 0)
            def _():
                wait_h(last[0])

            last[0] = size // 64
            h_copy(hs, row, col, size).start()

        full = rows // TM

        def body(m, k):
            work(base + m * TM, TM, k)
            return k + 1

        k = lax.fori_loop(0, full, body, k)
        rem = rows - full * TM
        at = base + full * TM
        for size in (64, 128, 192, 256):
            @pl.when((rem > size - 64) & (rem <= size))
            def _(size=size):
                work(at, size, k)

        @pl.when(st + 2 < NE * NF)
        def _():
            for c in w_copies(st + 2, slot):
                c.start()

        return k + jnp.where(rem > 0, 1, 0)

    @pl.when(lax.fori_loop(0, NE * NF, step, jnp.int32(0)) > 0)
    def _():
        wait_h(last[0])


def up_call(cnt, rank, ball, w1, w3):
    any_spec = pl.BlockSpec(memory_space=pl.ANY)
    return pl.pallas_call(
        up_kernel,
        out_shape=jax.ShapeDtypeStruct((XR, FF), BF16),
        in_specs=[pl.BlockSpec(memory_space=pltpu.SMEM), pl.BlockSpec(memory_space=pltpu.VMEM), any_spec, any_spec, any_spec],
        out_specs=any_spec,
        scratch_shapes=[
            pltpu.VMEM((XR, D), BF16),
            pltpu.VMEM((2, SB, D), BF16),
            pltpu.VMEM((SBR, SB), BF16),
            pltpu.VMEM((TM, D), BF16),
            pltpu.VMEM((2, 2, D, FC), BF16),
            pltpu.VMEM((2, TM, FC), BF16),
            pltpu.SMEM((NSB * NE,), jnp.int32),
            pltpu.SMEM((NSB * NE,), jnp.int32),
            pltpu.SMEM((NE + 1,), jnp.int32),
            pltpu.SMEM((NSB * NE,), jnp.int32),
            pltpu.SMEM((NSB,), jnp.int32),
            pltpu.SMEM((SBR // G,), jnp.int32),
            pltpu.SMEM((1,), jnp.int32),
            pltpu.SemaphoreType.DMA((2,)),
            pltpu.SemaphoreType.DMA((2, 2)),
            pltpu.SemaphoreType.DMA((1,)),
        ],
        compiler_params=pltpu.CompilerParams(vmem_limit_bytes=VMEM_LIMIT),
        cost_estimate=pl.CostEstimate(flops=48_000_000_000, bytes_accessed=140_000_000, transcendentals=0),
        name="up",
    )(cnt, rank, ball, w1, w3)


def down_kernel(cnt_ref, core_ref, rank_ref, wt_ref, h, w2, mine, theirs,
                hs, ebuf, kbuf, pbuf, wbuf, abuf, wsplit, ng, eoff, est, boff, nsb_g, hsem, wsem, osem):
    steps = (D // CW) * NE

    def w_copy(st, slot):
        col = pl.multiple_of((st // NE) * CW, CW)
        return pltpu.make_async_copy(w2.at[st % NE, :, pl.ds(col, CW)], wbuf.at[slot], wsem.at[slot])

    def h_copy(t):
        rows = pl.ds(pl.multiple_of(t * TM, TM), TM)
        return pltpu.make_async_copy(h.at[rows, :], hs.at[rows, :], hsem.at[0])

    for st in range(3):
        w_copy(st, st).start()
    offsets(cnt_ref, ng, eoff, est, boff, nsb_g)
    nh = (est[NE] + TM // G - 1) // (TM // G)

    def h_start(t, _):
        h_copy(t).start()
        return 0

    def h_wait(t, _):
        h_copy(t).wait()
        return 0

    lax.fori_loop(0, nh, h_start, 0)
    for s in range(NSB):
        w = wt_ref[s]
        hi = w.astype(BF16).astype(F32)
        mid = (w - hi).astype(BF16).astype(F32)
        wsplit[0, s] = hi
        wsplit[1, s] = mid
        wsplit[2, s] = w - hi - mid
    rows16 = lax.broadcasted_iota(jnp.int32, (G, SB), 0)
    for s in range(NSB):
        for e in range(NE):
            rk = jnp.broadcast_to(rank_ref[s, e:e + 1, :], (G, SB))
            parts = [jnp.broadcast_to(wsplit[i, s, e:e + 1, :], (G, SB)) for i in range(3)]

            def build(g, _, s=s, e=e, rk=rk, parts=parts):
                row = pl.multiple_of((boff[s * NE + e] + g) * G, G)
                hit = rk == rows16 + g * G
                for i in range(3):
                    pbuf[s, i, pl.ds(row, G), :] = jnp.where(hit, parts[i], 0.0).astype(BF16)
                return 0

            lax.fori_loop(0, ng[s * NE + e], build, 0)

        def clear(g, _, s=s):
            row = pl.multiple_of(g * G, G)
            for i in range(3):
                pbuf[s, i, pl.ds(row, G), :] = jnp.zeros((G, SB), BF16)
            return 0

        lax.fori_loop(nsb_g[s], -(-nsb_g[s] // (TM // G)) * (TM // G), clear, 0)
    kbuf[...] = jnp.zeros_like(kbuf)
    lax.fori_loop(0, nh, h_wait, 0)

    core = core_ref[0]

    def out_copies(c, s, slot):
        rel = core_ref[1 + s]
        keep = pl.multiple_of(core * 256, 256)
        give = pl.multiple_of(256 - core * 256, 256)
        out = []
        for i in range(CW // RC):
            cols = pl.ds(i * RC, RC)
            j = c * (CW // RC) + i
            out.append(pltpu.make_async_copy(abuf.at[slot, pl.ds(give, 256), cols], theirs.at[j, rel], osem.at[slot, i, 0]))
            out.append(pltpu.make_async_copy(abuf.at[slot, pl.ds(keep, 256), cols], mine.at[j, rel], osem.at[slot, i, 1]))
        return out

    def column(c, _):
        def expert(e, _):
            st = c * NE + e
            ws = st % 3
            w_copy(st, ws).wait()
            base = est[e] * G
            rows = est[e + 1] * G - base

            def work(row, size):
                row = pl.multiple_of(row, G)
                ebuf[pl.ds(row, size), :] = jnp.dot(hs[pl.ds(row, size), :], wbuf[ws], preferred_element_type=F32).astype(BF16)

            full = rows // TM

            def body(m, _):
                work(base + m * TM, TM)
                return 0

            lax.fori_loop(0, full, body, 0)
            rem = rows - full * TM
            for size in (64, 128, 192, 256):
                @pl.when((rem > size - 64) & (rem <= size))
                def _(size=size):
                    work(base + full * TM, size)

            @pl.when(st + 3 < steps)
            def _():
                w_copy(st + 3, ws).start()

            return 0

        lax.fori_loop(0, NE, expert, 0)

        def block(s, _):
            slot = s % 2

            def segment(e, _):
                def move(g, _):
                    row = pl.multiple_of((boff[s * NE + e] + g) * G, G)
                    src = pl.multiple_of((eoff[s * NE + e] + g) * G, G)
                    kbuf[pl.ds(row, G), :] = ebuf[pl.ds(src, G), :]
                    return 0

                return lax.fori_loop(0, ng[s * NE + e], move, 0)

            lax.fori_loop(0, NE, segment, 0)
            nk = (nsb_g[s] + TM // G - 1) // (TM // G)

            @pl.when(c * NSB + s >= 2)
            def _():
                for cp in out_copies(c, s, slot):
                    cp.wait()

            abuf[slot] = jnp.zeros((SB, CW), F32)

            def tile(kt, _):
                rows = pl.ds(pl.multiple_of(kt * TM, TM), TM)
                ek = kbuf[rows, :]
                for half in range(2):
                    toks = slice(half * 256, half * 256 + 256)
                    tot = abuf[slot, toks, :]
                    for i in range(3):
                        tot = tot + lax.dot_general(pbuf[s, i, rows, toks], ek, (((0,), (0,)), ((), ())), preferred_element_type=F32)
                    abuf[slot, toks, :] = tot
                return 0

            lax.fori_loop(0, nk, tile, 0)
            for cp in out_copies(c, s, slot):
                cp.start()
            return 0

        return lax.fori_loop(0, NSB, block, 0)

    lax.fori_loop(0, D // CW, column, 0)
    for s in (NSB - 2, NSB - 1):
        for cp in out_copies(D // CW - 1, s, s % 2):
            cp.wait()


def down_call(cnt, core, rank, wts, h, w2):
    any_spec = pl.BlockSpec(memory_space=pl.ANY)
    smem = pl.BlockSpec(memory_space=pltpu.SMEM)
    vmem = pl.BlockSpec(memory_space=pltpu.VMEM)
    out = jax.ShapeDtypeStruct((NC, NSB, 256, RC), F32)
    return pl.pallas_call(
        down_kernel,
        out_shape=(out, out),
        in_specs=[smem, smem, vmem, vmem, any_spec, any_spec],
        out_specs=(any_spec, any_spec),
        scratch_shapes=[
            pltpu.VMEM((XR, FF), BF16),
            pltpu.VMEM((XR, CW), BF16),
            pltpu.VMEM((SBR, CW), BF16),
            pltpu.VMEM((NSB, 3, SBR, SB), BF16),
            pltpu.VMEM((3, FF, CW), BF16),
            pltpu.VMEM((2, SB, CW), F32),
            pltpu.VMEM((3, NSB, NE, SB), F32),
            pltpu.SMEM((NSB * NE,), jnp.int32),
            pltpu.SMEM((NSB * NE,), jnp.int32),
            pltpu.SMEM((NE + 1,), jnp.int32),
            pltpu.SMEM((NSB * NE,), jnp.int32),
            pltpu.SMEM((NSB,), jnp.int32),
            pltpu.SemaphoreType.DMA((1,)),
            pltpu.SemaphoreType.DMA((3,)),
            pltpu.SemaphoreType.DMA((2, CW // RC, 2)),
        ],
        compiler_params=pltpu.CompilerParams(vmem_limit_bytes=VMEM_LIMIT),
        cost_estimate=pl.CostEstimate(flops=40_000_000_000, bytes_accessed=100_000_000, transcendentals=0),
        name="down",
    )(cnt, core, rank, wts, h, w2)


def neighbours():
    me = lax.axis_index('ep')
    core = me + 1 - 2 * (me % 2)
    x = me + 2 - 4 * ((me // 2) % 2)
    y = me + 4 - 8 * (me // 4)
    return me, core, x, y


def remote(src, dst, send, recv, dev):
    return pltpu.make_async_remote_copy(src_ref=src, dst_ref=dst, send_sem=send, recv_sem=recv, device_id={'ep': dev}, device_id_type=pl.DeviceIdType.MESH)


def enter(others):
    barrier = pltpu.get_barrier_semaphore()
    for dev in others:
        pl.semaphore_signal(barrier, inc=1, device_id={'ep': dev}, device_id_type=pl.DeviceIdType.MESH)
    pl.semaphore_wait(barrier, len(others))


def gather_kernel(b_any, b_ref, wts_ref, w1, w3, w2, ball, wall, s_ref, w13buf, w2buf, acc, send, recv, wsend, wrecv, local, wsem):
    me, pn, xn, yn = neighbours()
    diag = xn + yn - me
    half = T // 2

    def rows(dev, h):
        return pl.ds(pl.multiple_of(dev * T + h * half, half), half)

    def own(k, h, dev):
        return remote(b_any.at[pl.ds(h * half, half), :], ball.at[rows(me, h), :], send.at[k], recv.at[k], dev)

    def relay(k, owner, h, dev):
        return remote(ball.at[rows(owner, h), :], ball.at[rows(owner, h), :], send.at[k], recv.at[k], dev)

    def w_copies(st, slot):
        cols = pl.ds(pl.multiple_of(st * SF, SF), SF)
        return (pltpu.make_async_copy(w1.at[:, cols], w13buf.at[slot, 0], wsem.at[slot, 0]),
                pltpu.make_async_copy(w3.at[:, cols], w13buf.at[slot, 1], wsem.at[slot, 1]),
                pltpu.make_async_copy(w2.at[cols, :], w2buf.at[slot], wsem.at[slot, 2]))

    for st in range(3):
        for c in w_copies(st, st):
            c.start()
    others = [lax.rem(me + k, 8) for k in range(1, 8)]
    enter(others)
    first = [own(0, 0, xn), own(2, 1, yn), own(1, 1, xn), own(3, 0, yn), own(4, 0, pn), own(5, 1, pn)]
    for c in first:
        c.start()
    lanes = pl.ds(pl.multiple_of((me % 2) * T, T), T)
    small = []
    for k, dev in enumerate(others):
        small.append(remote(wts_ref.at[pl.ds(pl.multiple_of(dev * NE, NE), NE), :], wall.at[me // 2, :, lanes], wsend.at[k], wrecv.at[k], dev))
        small[-1].start()
    keep = [pltpu.make_async_copy(b_ref, ball.at[pl.ds(pl.multiple_of(me * T, T), T), :], local.at[0]),
            pltpu.make_async_copy(wts_ref.at[pl.ds(pl.multiple_of(me * NE, NE), NE), :], wall.at[me // 2, :, lanes], local.at[1])]
    for c in keep:
        c.start()
    acc[...] = jnp.zeros_like(acc)

    def step(st, _):
        slot = lax.rem(st, 3)
        for c in w_copies(st, slot):
            c.wait()
        x = b_ref[...]
        gate = jnp.dot(x, w13buf[slot, 0], preferred_element_type=F32)
        lin = jnp.dot(x, w13buf[slot, 1], preferred_element_type=F32)
        inner = (jax.nn.silu(gate) * lin).astype(BF16)
        for n in range(D // 512):
            cols = slice(n * 512, n * 512 + 512)
            acc[:, cols] += jnp.dot(inner, w2buf[slot, :, cols], preferred_element_type=F32)

        return 0

    def refill(st, _):
        step(st, 0)
        for c in w_copies(st + 3, lax.rem(st, 3)):
            c.start()
        return 0

    lax.fori_loop(0, 8, refill, 0)
    first[0].wait_recv()
    first[1].wait_recv()
    second = [relay(6, xn, 0, yn), relay(7, yn, 1, xn), relay(8, xn, 0, pn), relay(9, yn, 1, pn)]
    for c in second:
        c.start()
    lax.fori_loop(8, SHARED // SF - 3, refill, 0)
    lax.fori_loop(SHARED // SF - 3, SHARED // SF, step, 0)
    s_ref[...] = acc[...].astype(BF16)
    first[2].wait_recv()
    first[3].wait_recv()
    third = [relay(10, xn, 1, pn), relay(11, yn, 0, pn)]
    for c in third:
        c.start()
    second[0].wait_recv()
    second[1].wait_recv()
    fourth = [relay(12, diag, 0, pn), relay(13, diag, 1, pn)]
    for c in fourth:
        c.start()
    for c in (first[4], first[5], second[2], second[3], *third, *fourth):
        c.wait_recv()
    for c in (*first, *second, *third, *fourth):
        c.wait_send()
    for c in small:
        c.wait()
    for c in keep:
        c.wait()


def gather_call(b, wts, w1, w3, w2):
    any_spec = pl.BlockSpec(memory_space=pl.ANY)
    vmem = pl.BlockSpec(memory_space=pltpu.VMEM)
    return pl.pallas_call(
        gather_kernel,
        out_shape=(jax.ShapeDtypeStruct((8 * T, D), BF16), jax.ShapeDtypeStruct((NSB, NE, SB), F32), jax.ShapeDtypeStruct((T, D), BF16)),
        in_specs=[any_spec, vmem, vmem, any_spec, any_spec, any_spec],
        out_specs=(any_spec, any_spec, vmem),
        scratch_shapes=[
            pltpu.VMEM((3, 2, D, SF), BF16),
            pltpu.VMEM((3, SF, D), BF16),
            pltpu.VMEM((T, D), F32),
            pltpu.SemaphoreType.DMA((14,)),
            pltpu.SemaphoreType.DMA((14,)),
            pltpu.SemaphoreType.DMA((7,)),
            pltpu.SemaphoreType.DMA((7,)),
            pltpu.SemaphoreType.DMA((2,)),
            pltpu.SemaphoreType.DMA((3, 3)),
        ],
        compiler_params=pltpu.CompilerParams(collective_id=0, has_side_effects=True, vmem_limit_bytes=VMEM_LIMIT),
        cost_estimate=pl.CostEstimate(flops=12_000_000_000, bytes_accessed=60_000_000, transcendentals=0),
        name="gather",
    )(b, b, wts, w1, w3, w2)


def return_kernel(mine, theirs, y_ref, s_ref, out_ref, own, r1, r2x, r2y, r3x, r3y, send, recv, load):
    me, pn, xn, yn = neighbours()
    half = T // 2
    top, low = pl.ds(0, half), pl.ds(half, half)

    def load_of(j):
        return pltpu.make_async_copy(mine.at[j], own.at[j], load.at[j])

    def core_of(j):
        return remote(theirs.at[j], r1.at[j], send.at[0, j], recv.at[0, j], pn)

    def x_of(j):
        return remote(own.at[j, pl.ds(1, 2), top, :], r2x.at[j], send.at[1, j], recv.at[1, j], xn)

    def y_of(j):
        return remote(own.at[j, pl.ds(2, 2), low, :], r2y.at[j], send.at[2, j], recv.at[2, j], yn)

    def y_last(j):
        return remote(own.at[j, 3, top, :], r3y.at[j], send.at[3, j], recv.at[3, j], yn)

    def x_last(j):
        return remote(own.at[j, 1, low, :], r3x.at[j], send.at[4, j], recv.at[4, j], xn)

    def each(body):
        def run(j, _):
            body(j)
            return 0

        lax.fori_loop(0, NC, run, 0)

    def begin(j):
        load_of(j).start()
        core_of(j).start()

    def pair(j):
        load_of(j).wait()
        core_of(j).wait_recv()
        own[j, 1:] = own[j, 1:] + r1[j, 1:]
        x_of(j).start()
        y_of(j).start()
        own[j, 0] = own[j, 0] + r1[j, 0]

    def onward(j):
        x_of(j).wait_recv()
        own[j, 3, :half] = own[j, 3, :half] + r2x[j, 1]
        y_last(j).start()
        y_of(j).wait_recv()
        own[j, 1, half:] = own[j, 1, half:] + r2y[j, 0]
        x_last(j).start()

    def finish(j):
        cols = pl.ds(pl.multiple_of(j * RC, RC), RC)
        y_last(j).wait_recv()
        x_last(j).wait_recv()
        base = y_ref[:, cols].astype(F32) + s_ref[:, cols].astype(F32)
        out_ref[:half, cols] = (base[:half] + (own[j, 0, :half] + r2x[j, 0] + r3y[j])).astype(BF16)
        out_ref[half:, cols] = (base[half:] + (own[j, 0, half:] + r2y[j, 1] + r3x[j])).astype(BF16)

    def drain(j):
        for c in (core_of(j), x_of(j), y_of(j), y_last(j), x_last(j)):
            c.wait_send()

    enter([pn, xn, yn])
    each(begin)
    each(pair)
    each(onward)
    each(finish)
    each(drain)


def return_call(mine, theirs, hidden, shared_out):
    any_spec = pl.BlockSpec(memory_space=pl.ANY)
    vmem = pl.BlockSpec(memory_space=pltpu.VMEM)
    half = T // 2
    return pl.pallas_call(
        return_kernel,
        out_shape=jax.ShapeDtypeStruct((T, D), BF16),
        in_specs=[any_spec, any_spec, vmem, vmem],
        out_specs=vmem,
        scratch_shapes=[
            pltpu.VMEM((NC, NSB, T, RC), F32),
            pltpu.VMEM((NC, NSB, T, RC), F32),
            pltpu.VMEM((NC, 2, half, RC), F32),
            pltpu.VMEM((NC, 2, half, RC), F32),
            pltpu.VMEM((NC, half, RC), F32),
            pltpu.VMEM((NC, half, RC), F32),
            pltpu.SemaphoreType.DMA((5, NC)),
            pltpu.SemaphoreType.DMA((5, NC)),
            pltpu.SemaphoreType.DMA((NC,)),
        ],
        compiler_params=pltpu.CompilerParams(collective_id=1, has_side_effects=True, vmem_limit_bytes=VMEM_LIMIT),
        name="return_sum",
    )(mine, theirs, hidden, shared_out)


def solution(mesh):
    tok_spec = P(('dp', 'ep'), None)
    expert_spec = P('ep', None, None)

    def local_fn(hidden, norm_gain, w_gate, w1_shared, w3_shared, w2_shared, w1_experts, w3_experts, w2_experts, topk_ids):
        normed = rms_norm(hidden, norm_gain)
        probs = jax.nn.softmax(jnp.dot(normed, w_gate, preferred_element_type=F32), axis=-1)
        chosen = jnp.any(topk_ids[:, :, None] == jnp.arange(EXPERTS), axis=1)
        gate_wts = jnp.where(chosen, ROUTE_SCALE * probs, -1.0).T
        ball, wsb, shared_out = gather_call(normed, gate_wts, w1_shared, w3_shared, w2_shared)
        me = lax.axis_index('ep')
        sel = wsb >= 0.0
        cnt = jnp.sum(sel, axis=2, dtype=jnp.int32)
        before = jnp.arange(SB)[:, None] < jnp.arange(SB)[None, :]
        rank = jnp.einsum('set,tu->seu', sel.astype(BF16), before.astype(BF16), preferred_element_type=F32)
        rank = jnp.where(sel, rank.astype(jnp.int32), -1)
        chip, at = me // 2, jnp.arange(NSB)
        other_x, other_y = at % 2 != chip % 2, at // 2 != chip // 2
        place = jnp.where(other_x, jnp.where(other_y, 2, 1), jnp.where(other_y, 3, 0))
        core = jnp.concatenate([(me % 2)[None], place]).astype(jnp.int32)
        h = up_call(cnt, rank, ball, w1_experts, w3_experts)
        mine, theirs = down_call(cnt, core, rank, wsb, h, w2_experts)
        return return_call(mine, theirs, hidden, shared_out)

    return jax.shard_map(local_fn, mesh=mesh, in_specs=(tok_spec, P(), P(), P(), P(), P(), expert_spec, expert_spec, expert_spec, tok_spec), out_specs=tok_spec, check_vma=False)
```

```python
import functools

import jax
import jax.numpy as jnp
from jax import lax
from jax.experimental import pallas as pl
from jax.experimental.pallas import tpu as pltpu
from jax.sharding import PartitionSpec as P

ROUTE_SCALE = 16
NORM_EPS = 1e-6
D = 2560
FF = 1536
EXPERTS = 64
NE = 8
NSB = 4
SB = 512
G = 16
TM = 256
XG = 432
XR = XG * G
SBR = 1792
FC = 512
NF = FF // FC
T = 256
SHARED = 3072
SF = 256
CW = 512
RC = 256
NC = D // RC
KC = 768
KX = SBR - KC
VMEM_LIMIT = 66000000
BF16 = jnp.bfloat16
F32 = jnp.float32


def rms_norm(hidden, norm_gain):
    rows_f = hidden.astype(F32)
    inv_rms = lax.rsqrt(jnp.mean(rows_f * rows_f, axis=-1, keepdims=True) + NORM_EPS)
    return (rows_f * inv_rms * norm_gain.astype(F32)).astype(BF16)


def offsets(cnt_ref, ng, eoff, est, boff, nsb_g):
    run = jnp.int32(0)
    for e in range(NE):
        est[e] = run
        for s in range(NSB):
            n = (cnt_ref[s, e] + (G - 1)) // G
            ng[s * NE + e] = n
            eoff[s * NE + e] = run
            run = run + n
    est[NE] = run
    for s in range(NSB):
        b = jnp.int32(0)
        for e in range(NE):
            boff[s * NE + e] = b
            b = b + ng[s * NE + e]
        nsb_g[s] = b


def up_kernel(cnt_ref, rank_ref, ball, w1, w3, h_out, xs, bbuf, pbuf, tbuf, wbuf, hbuf, ng, eoff, est, boff, nsb_g, dst, last, bsem, wsem, hsem):
    def w_copies(step, slot):
        e = step // NF
        f = step % NF
        cols = pl.ds(pl.multiple_of(f * FC, FC), FC)
        return (pltpu.make_async_copy(w1.at[e, :, cols], wbuf.at[slot, 0], wsem.at[slot, 0]),
                pltpu.make_async_copy(w3.at[e, :, cols], wbuf.at[slot, 1], wsem.at[slot, 1]))

    def b_copy(s, slot):
        return pltpu.make_async_copy(ball.at[pl.ds(s * SB, SB), :], bbuf.at[slot], bsem.at[slot])

    b_copy(0, 0).start()
    for c in w_copies(0, 0):
        c.start()
    for c in w_copies(1, 1):
        c.start()
    offsets(cnt_ref, ng, eoff, est, boff, nsb_g)
    rows16 = lax.broadcasted_iota(jnp.int32, (G, SB), 0)

    for s in range(NSB):
        slot = s % 2
        if s + 1 < NSB:
            b_copy(s + 1, 1 - slot).start()
        for e in range(NE):
            rk = jnp.broadcast_to(rank_ref[s, e:e + 1, :], (G, SB))

            def build(g, _, s=s, e=e, rk=rk):
                k = boff[s * NE + e] + g
                dst[k] = eoff[s * NE + e] + g
                hit = jnp.where(rk == rows16 + g * G, 1.0, 0.0)
                pbuf[pl.ds(pl.multiple_of(k * G, G), G), :] = hit.astype(BF16)
                return 0

            lax.fori_loop(0, ng[s * NE + e], build, 0)
        b_copy(s, slot).wait()

        def tile(m, _, s=s, slot=slot):
            prow = pbuf[pl.ds(pl.multiple_of(m * TM, TM), TM), :]
            for n in range(D // 512):
                cols = slice(n * 512, (n + 1) * 512)
                tbuf[:, cols] = jnp.dot(prow, bbuf[slot, :, cols], preferred_element_type=F32).astype(BF16)

            def put(j, _):
                row = pl.multiple_of(dst[m * (TM // G) + j] * G, G)
                xs[pl.ds(row, G), :] = tbuf[pl.ds(pl.multiple_of(j * G, G), G), :]
                return 0

            lax.fori_loop(0, jnp.minimum(TM // G, nsb_g[s] - m * (TM // G)), put, 0)
            return 0

        lax.fori_loop(0, (nsb_g[s] + TM // G - 1) // (TM // G), tile, 0)

    def h_copy(hs, row, col, size):
        return pltpu.make_async_copy(hbuf.at[hs, pl.ds(0, size), :], h_out.at[pl.ds(row, size), pl.ds(col, FC)], hsem.at[0])

    def wait_h(quarters):
        for q in range(1, 5):
            @pl.when(quarters == q)
            def _(q=q):
                h_copy(0, 0, 0, q * 64).wait()

    def step(st, k):
        slot = st % 2
        e = st // NF
        col = pl.multiple_of((st % NF) * FC, FC)
        for c in w_copies(st, slot):
            c.wait()
        base = est[e] * G
        rows = est[e + 1] * G - base

        def work(row, size, k):
            row = pl.multiple_of(row, G)
            hs = k % 2
            x = xs[pl.ds(row, size), :]
            gate = jnp.dot(x, wbuf[slot, 0], preferred_element_type=F32)
            lin = jnp.dot(x, wbuf[slot, 1], preferred_element_type=F32)
            hbuf[hs, pl.ds(0, size), :] = (jax.nn.silu(gate) * lin).astype(BF16)

            @pl.when(k > 0)
            def _():
                wait_h(last[0])

            last[0] = size // 64
            h_copy(hs, row, col, size).start()

        full = rows // TM

        def body(m, k):
            work(base + m * TM, TM, k)
            return k + 1

        k = lax.fori_loop(0, full, body, k)
        rem = rows - full * TM
        at = base + full * TM
        for size in (64, 128, 192, 256):
            @pl.when((rem > size - 64) & (rem <= size))
            def _(size=size):
                work(at, size, k)

        @pl.when(st + 2 < NE * NF)
        def _():
            for c in w_copies(st + 2, slot):
                c.start()

        return k + jnp.where(rem > 0, 1, 0)

    @pl.when(lax.fori_loop(0, NE * NF, step, jnp.int32(0)) > 0)
    def _():
        wait_h(last[0])


def up_call(cnt, rank, ball, w1, w3):
    any_spec = pl.BlockSpec(memory_space=pl.ANY)
    return pl.pallas_call(
        up_kernel,
        out_shape=jax.ShapeDtypeStruct((XR, FF), BF16),
        in_specs=[pl.BlockSpec(memory_space=pltpu.SMEM), pl.BlockSpec(memory_space=pltpu.VMEM), any_spec, any_spec, any_spec],
        out_specs=any_spec,
        scratch_shapes=[
            pltpu.VMEM((XR, D), BF16),
            pltpu.VMEM((2, SB, D), BF16),
            pltpu.VMEM((SBR, SB), BF16),
            pltpu.VMEM((TM, D), BF16),
            pltpu.VMEM((2, 2, D, FC), BF16),
            pltpu.VMEM((2, TM, FC), BF16),
            pltpu.SMEM((NSB * NE,), jnp.int32),
            pltpu.SMEM((NSB * NE,), jnp.int32),
            pltpu.SMEM((NE + 1,), jnp.int32),
            pltpu.SMEM((NSB * NE,), jnp.int32),
            pltpu.SMEM((NSB,), jnp.int32),
            pltpu.SMEM((SBR // G,), jnp.int32),
            pltpu.SMEM((1,), jnp.int32),
            pltpu.SemaphoreType.DMA((2,)),
            pltpu.SemaphoreType.DMA((2, 2)),
            pltpu.SemaphoreType.DMA((1,)),
        ],
        compiler_params=pltpu.CompilerParams(vmem_limit_bytes=VMEM_LIMIT),
        cost_estimate=pl.CostEstimate(flops=48_000_000_000, bytes_accessed=140_000_000, transcendentals=0),
        name="up",
    )(cnt, rank, ball, w1, w3)


def down_kernel(cnt_ref, core_ref, rank_ref, wt_ref, h, w2, eblk, mine, theirs,
                hs, ebuf, kbuf, pbuf, wbuf, abuf, wsplit, ng, eoff, est, boff, nsb_g, hsem, wsem, osem, ksem):
    steps = (D // CW) * NE

    def w_copy(st, slot):
        col = pl.multiple_of((st // NE) * CW, CW)
        return pltpu.make_async_copy(w2.at[st % NE, :, pl.ds(col, CW)], wbuf.at[slot], wsem.at[slot])

    def h_copy(t):
        rows = pl.ds(pl.multiple_of(t * TM, TM), TM)
        return pltpu.make_async_copy(h.at[rows, :], hs.at[rows, :], hsem.at[0])

    for st in range(3):
        w_copy(st, st).start()
    offsets(cnt_ref, ng, eoff, est, boff, nsb_g)
    nh = (est[NE] + TM // G - 1) // (TM // G)

    def h_start(t, _):
        h_copy(t).start()
        return 0

    def h_wait(t, _):
        h_copy(t).wait()
        return 0

    lax.fori_loop(0, nh, h_start, 0)
    most = jnp.maximum(jnp.maximum(nsb_g[0], nsb_g[1]), jnp.maximum(nsb_g[2], nsb_g[3]))
    over = most > KC // G

    @pl.when(over)
    def _():
        rows16 = lax.broadcasted_iota(jnp.int32, (G, SB), 0)
        pbuf[...] = jnp.zeros_like(pbuf)
        for s in range(NSB):
            w = wt_ref[s]
            hi = w.astype(BF16).astype(F32)
            mid = (w - hi).astype(BF16).astype(F32)
            wsplit[0, s] = hi
            wsplit[1, s] = mid
            wsplit[2, s] = w - hi - mid

        def segment(q, _):
            s, e = q // NE, q % NE
            rk = jnp.broadcast_to(rank_ref[s, pl.ds(e, 1), :], (G, SB))
            parts = [jnp.broadcast_to(wsplit[i, s, pl.ds(e, 1), :], (G, SB)) for i in range(3)]

            def build(g, _):
                k = boff[q] + g

                @pl.when(k >= KC // G)
                def _():
                    row = pl.multiple_of((k - KC // G) * G, G)
                    hit = rk == rows16 + g * G
                    for i in range(3):
                        pbuf[s, i, pl.ds(row, G), :] = jnp.where(hit, parts[i], 0.0).astype(BF16)

                return 0

            return lax.fori_loop(0, ng[q], build, 0)

        lax.fori_loop(0, NSB * NE, segment, 0)

    kbuf[...] = jnp.zeros_like(kbuf)
    lax.fori_loop(0, nh, h_wait, 0)

    core = core_ref[0]

    def out_copies(c, s):
        rel = core_ref[1 + s]
        keep = pl.multiple_of(core * 256, 256)
        give = pl.multiple_of(256 - core * 256, 256)
        out = []
        for i in range(CW // RC):
            cols = pl.ds(i * RC, RC)
            j = c * (CW // RC) + i
            out.append(pltpu.make_async_copy(abuf.at[pl.ds(give, 256), cols], theirs.at[j, rel], osem.at[i, 0]))
            out.append(pltpu.make_async_copy(abuf.at[pl.ds(keep, 256), cols], mine.at[j, rel], osem.at[i, 1]))
        return out

    def k_copies(c, s, slot):
        return [pltpu.make_async_copy(kbuf.at[slot, pl.ds(0, KC), pl.ds(i * RC, RC)], eblk.at[c * (CW // RC) + i, s], ksem.at[slot, i]) for i in range(CW // RC)]

    def column(c, _):
        def expert(e, _):
            st = c * NE + e
            ws = st % 3
            w_copy(st, ws).wait()
            base = est[e] * G
            rows = est[e + 1] * G - base

            def work(row, size):
                row = pl.multiple_of(row, G)
                ebuf[pl.ds(row, size), :] = jnp.dot(hs[pl.ds(row, size), :], wbuf[ws], preferred_element_type=F32).astype(BF16)

            full = rows // TM

            def body(m, _):
                work(base + m * TM, TM)
                return 0

            lax.fori_loop(0, full, body, 0)
            rem = rows - full * TM
            for size in (64, 128, 192, 256):
                @pl.when((rem > size - 64) & (rem <= size))
                def _(size=size):
                    work(base + full * TM, size)

            @pl.when(st + 3 < steps)
            def _():
                w_copy(st + 3, ws).start()

            return 0

        lax.fori_loop(0, NE, expert, 0)

        def block(s, _):
            slot = s % 2

            @pl.when(c * NSB + s >= 2)
            def _():
                for cp in k_copies(c, s, slot):
                    cp.wait()

            def segment(e, _):
                def move(g, _):
                    row = pl.multiple_of((boff[s * NE + e] + g) * G, G)
                    src = pl.multiple_of((eoff[s * NE + e] + g) * G, G)
                    kbuf[slot, pl.ds(row, G), :] = ebuf[pl.ds(src, G), :]
                    return 0

                return lax.fori_loop(0, ng[s * NE + e], move, 0)

            lax.fori_loop(0, NE, segment, 0)
            for cp in k_copies(c, s, slot):
                cp.start()

            @pl.when(over)
            def _():
                nk = (nsb_g[s] + TM // G - 1) // (TM // G)
                abuf[...] = jnp.zeros_like(abuf)

                def tile(kt, _):
                    ek = kbuf[slot, pl.ds(pl.multiple_of(kt * TM, TM), TM), :]
                    rows = pl.ds(pl.multiple_of(kt * TM - KC, TM), TM)
                    for i in range(3):
                        abuf[...] += lax.dot_general(pbuf[s, i, rows, :], ek, (((0,), (0,)), ((), ())), preferred_element_type=F32)
                    return 0

                lax.fori_loop(KC // TM, nk, tile, 0)
                for cp in out_copies(c, s):
                    cp.start()
                for cp in out_copies(c, s):
                    cp.wait()

            return 0

        return lax.fori_loop(0, NSB, block, 0)

    lax.fori_loop(0, D // CW, column, 0)
    for s in (NSB - 2, NSB - 1):
        for cp in k_copies(D // CW - 1, s, s % 2):
            cp.wait()


def down_call(cnt, core, rank, wts, h, w2):
    any_spec = pl.BlockSpec(memory_space=pl.ANY)
    smem = pl.BlockSpec(memory_space=pltpu.SMEM)
    vmem = pl.BlockSpec(memory_space=pltpu.VMEM)
    out = jax.ShapeDtypeStruct((NC, NSB, 256, RC), F32)
    return pl.pallas_call(
        down_kernel,
        out_shape=(jax.ShapeDtypeStruct((NC, NSB, KC, RC), BF16), out, out),
        in_specs=[smem, smem, vmem, vmem, any_spec, any_spec],
        out_specs=(any_spec, any_spec, any_spec),
        scratch_shapes=[
            pltpu.VMEM((XR, FF), BF16),
            pltpu.VMEM((XR, CW), BF16),
            pltpu.VMEM((2, SBR, CW), BF16),
            pltpu.VMEM((NSB, 3, KX, SB), BF16),
            pltpu.VMEM((3, FF, CW), BF16),
            pltpu.VMEM((SB, CW), F32),
            pltpu.VMEM((3, NSB, NE, SB), F32),
            pltpu.SMEM((NSB * NE,), jnp.int32),
            pltpu.SMEM((NSB * NE,), jnp.int32),
            pltpu.SMEM((NE + 1,), jnp.int32),
            pltpu.SMEM((NSB * NE,), jnp.int32),
            pltpu.SMEM((NSB,), jnp.int32),
            pltpu.SemaphoreType.DMA((1,)),
            pltpu.SemaphoreType.DMA((3,)),
            pltpu.SemaphoreType.DMA((CW // RC, 2)),
            pltpu.SemaphoreType.DMA((2, CW // RC)),
        ],
        compiler_params=pltpu.CompilerParams(vmem_limit_bytes=VMEM_LIMIT),
        cost_estimate=pl.CostEstimate(flops=40_000_000_000, bytes_accessed=100_000_000, transcendentals=0),
        name="down",
    )(cnt, core, rank, wts, h, w2)


def neighbours():
    me = lax.axis_index('ep')
    core = me + 1 - 2 * (me % 2)
    x = me + 2 - 4 * ((me // 2) % 2)
    y = me + 4 - 8 * (me // 4)
    return me, core, x, y


def remote(src, dst, send, recv, dev):
    return pltpu.make_async_remote_copy(src_ref=src, dst_ref=dst, send_sem=send, recv_sem=recv, device_id={'ep': dev}, device_id_type=pl.DeviceIdType.MESH)


def enter(others):
    barrier = pltpu.get_barrier_semaphore()
    for dev in others:
        pl.semaphore_signal(barrier, inc=1, device_id={'ep': dev}, device_id_type=pl.DeviceIdType.MESH)
    pl.semaphore_wait(barrier, len(others))


def gather_kernel(b_any, b_ref, wts_ref, w1, w3, w2, ball, wall_out, rank_ref, cnt_ref, pt, s_ref, wall, ptbuf, cols_buf, w13buf, w2buf, acc, send, recv, wsend, wrecv, local, wsem, psem):
    me, pn, xn, yn = neighbours()
    diag = xn + yn - me
    half = T // 2

    def rows(dev, h):
        return pl.ds(pl.multiple_of(dev * T + h * half, half), half)

    def own(k, h, dev):
        return remote(b_any.at[pl.ds(h * half, half), :], ball.at[rows(me, h), :], send.at[k], recv.at[k], dev)

    def relay(k, owner, h, dev):
        return remote(ball.at[rows(owner, h), :], ball.at[rows(owner, h), :], send.at[k], recv.at[k], dev)

    def w_copies(st, slot):
        cols = pl.ds(pl.multiple_of(st * SF, SF), SF)
        return (pltpu.make_async_copy(w1.at[:, cols], w13buf.at[slot, 0], wsem.at[slot, 0]),
                pltpu.make_async_copy(w3.at[:, cols], w13buf.at[slot, 1], wsem.at[slot, 1]),
                pltpu.make_async_copy(w2.at[cols, :], w2buf.at[slot], wsem.at[slot, 2]))

    for st in range(3):
        for c in w_copies(st, st):
            c.start()
    others = [lax.rem(me + k, 8) for k in range(1, 8)]
    enter(others)
    first = [own(0, 0, xn), own(2, 1, yn), own(1, 1, xn), own(3, 0, yn), own(4, 0, pn), own(5, 1, pn)]
    for c in first:
        c.start()
    lanes = pl.ds(pl.multiple_of((me % 2) * T, T), T)
    small = []
    for k, dev in enumerate(others):
        small.append(remote(wts_ref.at[pl.ds(pl.multiple_of(dev * NE, NE), NE), :], wall.at[me // 2, :, lanes], wsend.at[k], wrecv.at[k], dev))
        small[-1].start()
    keep = [pltpu.make_async_copy(b_ref, ball.at[pl.ds(pl.multiple_of(me * T, T), T), :], local.at[0]),
            pltpu.make_async_copy(wts_ref.at[pl.ds(pl.multiple_of(me * NE, NE), NE), :], wall.at[me // 2, :, lanes], local.at[1])]
    for c in keep:
        c.start()
    acc[...] = jnp.zeros_like(acc)

    def step(st, _):
        slot = lax.rem(st, 3)
        for c in w_copies(st, slot):
            c.wait()
        x = b_ref[...]
        gate = jnp.dot(x, w13buf[slot, 0], preferred_element_type=F32)
        lin = jnp.dot(x, w13buf[slot, 1], preferred_element_type=F32)
        inner = (jax.nn.silu(gate) * lin).astype(BF16)
        for n in range(D // 512):
            cols = slice(n * 512, n * 512 + 512)
            acc[:, cols] += jnp.dot(inner, w2buf[slot, :, cols], preferred_element_type=F32)

        return 0

    def refill(st, _):
        step(st, 0)
        for c in w_copies(st + 3, lax.rem(st, 3)):
            c.start()
        return 0

    lax.fori_loop(0, 8, refill, 0)
    first[0].wait_recv()
    first[1].wait_recv()
    second = [relay(6, xn, 0, yn), relay(7, yn, 1, xn), relay(8, xn, 0, pn), relay(9, yn, 1, pn)]
    for c in second:
        c.start()
    lax.fori_loop(8, SHARED // SF - 3, refill, 0)
    lax.fori_loop(SHARED // SF - 3, SHARED // SF, step, 0)
    s_ref[...] = acc[...].astype(BF16)
    first[2].wait_recv()
    first[3].wait_recv()
    third = [relay(10, xn, 1, pn), relay(11, yn, 0, pn)]
    for c in third:
        c.start()
    for c in small:
        c.wait_recv()
    keep[1].wait()
    before = jnp.where(lax.broadcasted_iota(jnp.int32, (SB, SB), 0) < lax.broadcasted_iota(jnp.int32, (SB, SB), 1), 1.0, 0.0).astype(BF16)
    row = lax.broadcasted_iota(jnp.int32, (1, KC), 1)
    puts = []
    for s in range(NSB):
        slot = s % 2
        w = wall[s]
        wall_out[s] = w
        sel = jnp.where(w >= 0.0, 1.0, 0.0)
        rank = jnp.where(w >= 0.0, jnp.dot(sel.astype(BF16), before, preferred_element_type=F32), -1.0)
        rank_ref[s] = rank.astype(jnp.int32)
        count = jnp.sum(sel, axis=1, keepdims=True).astype(jnp.int32)
        cnt_ref[s] = jnp.broadcast_to(count, (NE, 128))
        wide = jnp.broadcast_to(count, (NE, KC))
        start = jnp.zeros((1, KC), jnp.int32)
        local_row = []
        for e in range(NE):
            n = wide[e:e + 1]
            at = row - start
            local_row.append(jnp.where((at >= 0) & (at < n), at, -2).astype(F32))
            start = start + (n + (G - 1)) // G * G
        pad = jnp.zeros((128 - NE, SB), F32)
        cols_buf[0] = jnp.concatenate([rank, pad], axis=0).T
        cols_buf[1] = jnp.concatenate([w, pad], axis=0).T
        if s >= 2:
            puts[s - 2].wait()

        def fill(tb, _, slot=slot, local_row=local_row):
            toks = pl.ds(pl.multiple_of(tb * 32, 32), 32)
            rk = cols_buf[0, toks, :]
            wt = cols_buf[1, toks, :]
            total = jnp.zeros((32, KC), F32)
            for e in range(NE):
                total = jnp.where(rk[:, e:e + 1] == local_row[e], wt[:, e:e + 1], total)
            hi = total.astype(BF16)
            rest = total - hi.astype(F32)
            mid = rest.astype(BF16)
            ptbuf[slot, 0, toks, :] = hi
            ptbuf[slot, 1, toks, :] = mid
            ptbuf[slot, 2, toks, :] = (rest - mid.astype(F32)).astype(BF16)
            return 0

        lax.fori_loop(0, SB // 32, fill, 0)
        puts.append(pltpu.make_async_copy(ptbuf.at[slot], pt.at[s], psem.at[slot]))
        puts[s].start()
    second[0].wait_recv()
    second[1].wait_recv()
    fourth = [relay(12, diag, 0, pn), relay(13, diag, 1, pn)]
    for c in fourth:
        c.start()
    for c in (first[4], first[5], second[2], second[3], *third, *fourth):
        c.wait_recv()
    for c in (*first, *second, *third, *fourth):
        c.wait_send()
    for c in small:
        c.wait_send()
    keep[0].wait()
    puts[2].wait()
    puts[3].wait()


def gather_call(b, wts, w1, w3, w2):
    any_spec = pl.BlockSpec(memory_space=pl.ANY)
    vmem = pl.BlockSpec(memory_space=pltpu.VMEM)
    return pl.pallas_call(
        gather_kernel,
        out_shape=(
            jax.ShapeDtypeStruct((8 * T, D), BF16),
            jax.ShapeDtypeStruct((NSB, NE, SB), F32),
            jax.ShapeDtypeStruct((NSB, NE, SB), jnp.int32),
            jax.ShapeDtypeStruct((NSB, NE, 128), jnp.int32),
            jax.ShapeDtypeStruct((NSB, 3, SB, KC), BF16),
            jax.ShapeDtypeStruct((T, D), BF16),
        ),
        in_specs=[any_spec, vmem, vmem, any_spec, any_spec, any_spec],
        out_specs=(any_spec, vmem, vmem, vmem, any_spec, vmem),
        scratch_shapes=[
            pltpu.VMEM((NSB, NE, SB), F32),
            pltpu.VMEM((2, 3, SB, KC), BF16),
            pltpu.VMEM((2, SB, 128), F32),
            pltpu.VMEM((3, 2, D, SF), BF16),
            pltpu.VMEM((3, SF, D), BF16),
            pltpu.VMEM((T, D), F32),
            pltpu.SemaphoreType.DMA((14,)),
            pltpu.SemaphoreType.DMA((14,)),
            pltpu.SemaphoreType.DMA((7,)),
            pltpu.SemaphoreType.DMA((7,)),
            pltpu.SemaphoreType.DMA((2,)),
            pltpu.SemaphoreType.DMA((3, 3)),
            pltpu.SemaphoreType.DMA((2,)),
        ],
        compiler_params=pltpu.CompilerParams(collective_id=0, has_side_effects=True, vmem_limit_bytes=VMEM_LIMIT),
        cost_estimate=pl.CostEstimate(flops=12_000_000_000, bytes_accessed=60_000_000, transcendentals=0),
        name="gather",
    )(b, b, wts, w1, w3, w2)


def return_kernel(cnt_ref, pt, eblk, mine, theirs, y_ref, s_ref, out_ref, ptv, ev, own, give, r1, r2x, r2y, r3x, r3y, send, recv, load, esem, psem):
    me, pn, xn, yn = neighbours()
    half = T // 2
    top, low = pl.ds(0, half), pl.ds(half, half)

    def load_of(j):
        return (pltpu.make_async_copy(theirs.at[j], give.at[j], load.at[0, j]), pltpu.make_async_copy(mine.at[j], own.at[j], load.at[1, j]))

    def e_of(j, slot):
        return pltpu.make_async_copy(eblk.at[j], ev.at[slot], esem.at[slot])

    def core_of(j):
        return remote(give.at[j], r1.at[j], send.at[0, j], recv.at[0, j], pn)

    def x_of(j):
        return remote(own.at[j, pl.ds(1, 2), top, :], r2x.at[j], send.at[1, j], recv.at[1, j], xn)

    def y_of(j):
        return remote(own.at[j, pl.ds(2, 2), low, :], r2y.at[j], send.at[2, j], recv.at[2, j], yn)

    def y_last(j):
        return remote(own.at[j, 3, top, :], r3y.at[j], send.at[3, j], recv.at[3, j], yn)

    def x_last(j):
        return remote(own.at[j, 1, low, :], r3x.at[j], send.at[4, j], recv.at[4, j], xn)

    def each(body):
        def run(j, _):
            body(j)
            return 0

        lax.fori_loop(0, NC, run, 0)

    rows_over = jnp.int32(0)
    for s in range(NSB):
        n = jnp.int32(0)
        for e in range(NE):
            n = n + (cnt_ref[s, e] + (G - 1)) // G
        rows_over = jnp.maximum(rows_over, n - KC // G)
    over = jnp.full((T, RC), rows_over, jnp.int32) > 0

    def begin(j):
        for c in load_of(j):
            c.start()

    def add_up(j, buf, first_tok):
        slot = lax.rem(j, 2)
        toks = pl.ds(pl.multiple_of(first_tok, T), T)

        def block(s, _):
            dx = lax.rem(lax.rem(s, 2) + lax.rem(me // 2, 2), 2)
            dy = lax.rem(s // 2 + me // 4, 2)
            place = dx + 3 * dy - 2 * dx * dy
            total = jnp.where(over, buf[j, place], 0.0)
            ek = ev[slot, s]
            for i in range(3):
                total = total + jnp.dot(ptv[s, i, toks, :], ek, preferred_element_type=F32)
            buf[j, place] = total
            return 0

        lax.fori_loop(0, NSB, block, 0)

    def make(j):
        e_of(j, lax.rem(j, 2)).wait()
        for c in load_of(j):
            c.wait()
        add_up(j, give, T - lax.rem(me, 2) * T)
        core_of(j).start()
        add_up(j, own, lax.rem(me, 2) * T)

    def pair(j):
        core_of(j).wait_recv()
        own[j, 1:] = own[j, 1:] + r1[j, 1:]
        x_of(j).start()
        y_of(j).start()
        own[j, 0] = own[j, 0] + r1[j, 0]

    def onward(j):
        x_of(j).wait_recv()
        own[j, 3, :half] = own[j, 3, :half] + r2x[j, 1]
        y_last(j).start()
        y_of(j).wait_recv()
        own[j, 1, half:] = own[j, 1, half:] + r2y[j, 0]
        x_last(j).start()

    def finish(j):
        cols = pl.ds(pl.multiple_of(j * RC, RC), RC)
        y_last(j).wait_recv()
        x_last(j).wait_recv()
        base = y_ref[:, cols].astype(F32) + s_ref[:, cols].astype(F32)
        out_ref[:half, cols] = (base[:half] + (own[j, 0, :half] + r2x[j, 0] + r3y[j])).astype(BF16)
        out_ref[half:, cols] = (base[half:] + (own[j, 0, half:] + r2y[j, 1] + r3x[j])).astype(BF16)

    def drain(j):
        for c in (core_of(j), x_of(j), y_of(j), y_last(j), x_last(j)):
            c.wait_send()

    e_of(0, 0).start()
    pt_copies = [pltpu.make_async_copy(pt.at[s], ptv.at[s], psem.at[s]) for s in range(NSB)]
    for c in pt_copies:
        c.start()
    e_of(1, 1).start()
    enter([pn, xn, yn])
    each(begin)
    for c in pt_copies:
        c.wait()

    def steady(j, _):
        make(j)

        @pl.when(j + 2 < NC)
        def _():
            e_of(j + 2, lax.rem(j, 2)).start()

        pair(j)
        return 0

    lax.fori_loop(0, NC, steady, 0)
    each(onward)
    each(finish)
    each(drain)


def return_call(cnt, pt, eblk, mine, theirs, hidden, shared_out):
    any_spec = pl.BlockSpec(memory_space=pl.ANY)
    vmem = pl.BlockSpec(memory_space=pltpu.VMEM)
    half = T // 2
    return pl.pallas_call(
        return_kernel,
        out_shape=jax.ShapeDtypeStruct((T, D), BF16),
        in_specs=[pl.BlockSpec(memory_space=pltpu.SMEM), any_spec, any_spec, any_spec, any_spec, vmem, vmem],
        out_specs=vmem,
        scratch_shapes=[
            pltpu.VMEM((NSB, 3, SB, KC), BF16),
            pltpu.VMEM((2, NSB, KC, RC), BF16),
            pltpu.VMEM((NC, NSB, T, RC), F32),
            pltpu.VMEM((NC, NSB, T, RC), F32),
            pltpu.VMEM((NC, NSB, T, RC), F32),
            pltpu.VMEM((NC, 2, half, RC), F32),
            pltpu.VMEM((NC, 2, half, RC), F32),
            pltpu.VMEM((NC, half, RC), F32),
            pltpu.VMEM((NC, half, RC), F32),
            pltpu.SemaphoreType.DMA((5, NC)),
            pltpu.SemaphoreType.DMA((5, NC)),
            pltpu.SemaphoreType.DMA((2, NC)),
            pltpu.SemaphoreType.DMA((2,)),
            pltpu.SemaphoreType.DMA((NSB,)),
        ],
        compiler_params=pltpu.CompilerParams(collective_id=1, has_side_effects=True, vmem_limit_bytes=VMEM_LIMIT),
        name="return_sum",
    )(cnt, pt, eblk, mine, theirs, hidden, shared_out)


def solution(mesh):
    tok_spec = P(('dp', 'ep'), None)
    expert_spec = P('ep', None, None)

    def local_fn(hidden, norm_gain, w_gate, w1_shared, w3_shared, w2_shared, w1_experts, w3_experts, w2_experts, topk_ids):
        normed = rms_norm(hidden, norm_gain)
        probs = jax.nn.softmax(jnp.dot(normed, w_gate, preferred_element_type=F32), axis=-1)
        chosen = jnp.any(topk_ids[:, :, None] == jnp.arange(EXPERTS), axis=1)
        gate_wts = jnp.where(chosen, ROUTE_SCALE * probs, -1.0).T
        ball, wsb, rank, counts, pt, shared_out = gather_call(normed, gate_wts, w1_shared, w3_shared, w2_shared)
        cnt = counts[:, :, 0]
        me = lax.axis_index('ep')
        chip, at = me // 2, jnp.arange(NSB)
        other_x, other_y = at % 2 != chip % 2, at // 2 != chip // 2
        place = jnp.where(other_x, jnp.where(other_y, 2, 1), jnp.where(other_y, 3, 0))
        core = jnp.concatenate([(me % 2)[None], place]).astype(jnp.int32)
        h = up_call(cnt, rank, ball, w1_experts, w3_experts)
        eblk, mine, theirs = down_call(cnt, core, rank, wsb, h, w2_experts)
        return return_call(cnt, pt, eblk, mine, theirs, hidden, shared_out)

    return jax.shard_map(local_fn, mesh=mesh, in_specs=(tok_spec, P(), P(), P(), P(), P(), expert_spec, expert_spec, expert_spec, tok_spec), out_specs=tok_spec, check_vma=False)
```

```python
import functools

import jax
import jax.numpy as jnp
from jax import lax
from jax.experimental import pallas as pl
from jax.experimental.pallas import tpu as pltpu
from jax.sharding import PartitionSpec as P

ROUTE_SCALE = 16
NORM_EPS = 1e-6
D = 2560
FF = 1536
EXPERTS = 64
NE = 8
NSB = 4
SB = 512
G = 16
TM = 256
XG = 432
XR = XG * G
SBR = 1792
FC = 512
NF = FF // FC
DH = D // 2
T = 256
SHARED = 3072
SF = 256
CW = 512
RC = 256
NC = D // RC
KC = 768
KX = SBR - KC
VMEM_LIMIT = 66000000
BF16 = jnp.bfloat16
F32 = jnp.float32


def rms_norm(hidden, norm_gain):
    rows_f = hidden.astype(F32)
    inv_rms = lax.rsqrt(jnp.mean(rows_f * rows_f, axis=-1, keepdims=True) + NORM_EPS)
    return (rows_f * inv_rms * norm_gain.astype(F32)).astype(BF16)


def offsets(cnt_ref, ng, eoff, est, boff, nsb_g):
    run = jnp.int32(0)
    for e in range(NE):
        est[e] = run
        for s in range(NSB):
            n = (cnt_ref[s, e] + (G - 1)) // G
            ng[s * NE + e] = n
            eoff[s * NE + e] = run
            run = run + n
    est[NE] = run
    for s in range(NSB):
        b = jnp.int32(0)
        for e in range(NE):
            boff[s * NE + e] = b
            b = b + ng[s * NE + e]
        nsb_g[s] = b


def up_kernel(cnt_ref, rank_ref, ball, w1, w3, h_out, xs, bbuf, pbuf, tbuf, wbuf, hbuf, ng, eoff, est, boff, nsb_g, dst, last, bsem, wsem, hsem):
    def w_copies(step, slot):
        e = step // NF
        f = step % NF
        cols = pl.ds(pl.multiple_of(f * FC, FC), FC)
        return (pltpu.make_async_copy(w1.at[e, :, cols], wbuf.at[slot, 0], wsem.at[slot, 0]),
                pltpu.make_async_copy(w3.at[e, :, cols], wbuf.at[slot, 1], wsem.at[slot, 1]))

    def b_copy(s, half):
        return pltpu.make_async_copy(ball.at[pl.ds(s * SB, SB), pl.ds(half * DH, DH)], bbuf.at[half], bsem.at[half])

    b_copy(0, 0).start()
    b_copy(0, 1).start()
    for st in range(3):
        for c in w_copies(st, st):
            c.start()
    offsets(cnt_ref, ng, eoff, est, boff, nsb_g)
    rows16 = lax.broadcasted_iota(jnp.int32, (G, SB), 0)

    for s in range(NSB):
        for e in range(NE):
            rk = jnp.broadcast_to(rank_ref[s, e:e + 1, :], (G, SB))

            def build(g, _, s=s, e=e, rk=rk):
                k = boff[s * NE + e] + g
                dst[k] = eoff[s * NE + e] + g
                hit = jnp.where(rk == rows16 + g * G, 1.0, 0.0)
                pbuf[pl.ds(pl.multiple_of(k * G, G), G), :] = hit.astype(BF16)
                return 0

            lax.fori_loop(0, ng[s * NE + e], build, 0)
        for half in range(2):
            b_copy(s, half).wait()

            def tile(m, _, s=s, half=half):
                prow = pbuf[pl.ds(pl.multiple_of(m * TM, TM), TM), :]
                for n in range(5):
                    cols = slice(n * 256, (n + 1) * 256)
                    tbuf[:, cols] = jnp.dot(prow, bbuf[half, :, cols], preferred_element_type=F32).astype(BF16)

                def put(j, _):
                    row = pl.multiple_of(dst[m * (TM // G) + j] * G, G)
                    xs[pl.ds(row, G), half * DH:(half + 1) * DH] = tbuf[pl.ds(pl.multiple_of(j * G, G), G), :]
                    return 0

                lax.fori_loop(0, jnp.minimum(TM // G, nsb_g[s] - m * (TM // G)), put, 0)
                return 0

            lax.fori_loop(0, (nsb_g[s] + TM // G - 1) // (TM // G), tile, 0)
            if s + 1 < NSB:
                b_copy(s + 1, half).start()

    def h_copy(hs, row, col, size):
        return pltpu.make_async_copy(hbuf.at[hs, pl.ds(0, size), :], h_out.at[pl.ds(row, size), pl.ds(col, FC)], hsem.at[0])

    def wait_h(quarters):
        for q in range(1, 5):
            @pl.when(quarters == q)
            def _(q=q):
                h_copy(0, 0, 0, q * 64).wait()

    def step(st, k):
        slot = lax.rem(st, 3)
        e = st // NF
        col = pl.multiple_of((st % NF) * FC, FC)
        for c in w_copies(st, slot):
            c.wait()
        base = est[e] * G
        rows = est[e + 1] * G - base

        def work(row, size, k):
            row = pl.multiple_of(row, G)
            hs = k % 2
            for n in range(FC // 256):
                cols = slice(n * 256, (n + 1) * 256)
                x = xs[pl.ds(row, size), :]
                gate = jnp.dot(x, wbuf[slot, 0, :, cols], preferred_element_type=F32)
                lin = jnp.dot(x, wbuf[slot, 1, :, cols], preferred_element_type=F32)
                hbuf[hs, pl.ds(0, size), cols] = (jax.nn.silu(gate) * lin).astype(BF16)

            @pl.when(k > 0)
            def _():
                wait_h(last[0])

            last[0] = size // 64
            h_copy(hs, row, col, size).start()

        full = rows // TM

        def body(m, k):
            work(base + m * TM, TM, k)
            return k + 1

        k = lax.fori_loop(0, full, body, k)
        rem = rows - full * TM
        at = base + full * TM
        for size in (64, 128, 192, 256):
            @pl.when((rem > size - 64) & (rem <= size))
            def _(size=size):
                work(at, size, k)

        @pl.when(st + 3 < NE * NF)
        def _():
            for c in w_copies(st + 3, slot):
                c.start()

        return k + jnp.where(rem > 0, 1, 0)

    @pl.when(lax.fori_loop(0, NE * NF, step, jnp.int32(0)) > 0)
    def _():
        wait_h(last[0])


def up_call(cnt, rank, ball, w1, w3):
    any_spec = pl.BlockSpec(memory_space=pl.ANY)
    return pl.pallas_call(
        up_kernel,
        out_shape=jax.ShapeDtypeStruct((XR, FF), BF16),
        in_specs=[pl.BlockSpec(memory_space=pltpu.SMEM), pl.BlockSpec(memory_space=pltpu.VMEM), any_spec, any_spec, any_spec],
        out_specs=any_spec,
        scratch_shapes=[
            pltpu.VMEM((XR, D), BF16),
            pltpu.VMEM((2, SB, DH), BF16),
            pltpu.VMEM((SBR, SB), BF16),
            pltpu.VMEM((TM, DH), BF16),
            pltpu.VMEM((3, 2, D, FC), BF16),
            pltpu.VMEM((2, TM, FC), BF16),
            pltpu.SMEM((NSB * NE,), jnp.int32),
            pltpu.SMEM((NSB * NE,), jnp.int32),
            pltpu.SMEM((NE + 1,), jnp.int32),
            pltpu.SMEM((NSB * NE,), jnp.int32),
            pltpu.SMEM((NSB,), jnp.int32),
            pltpu.SMEM((SBR // G,), jnp.int32),
            pltpu.SMEM((1,), jnp.int32),
            pltpu.SemaphoreType.DMA((2,)),
            pltpu.SemaphoreType.DMA((3, 2)),
            pltpu.SemaphoreType.DMA((1,)),
        ],
        compiler_params=pltpu.CompilerParams(vmem_limit_bytes=VMEM_LIMIT),
        cost_estimate=pl.CostEstimate(flops=48_000_000_000, bytes_accessed=140_000_000, transcendentals=0),
        name="up",
    )(cnt, rank, ball, w1, w3)


def down_kernel(cnt_ref, core_ref, rank_ref, wt_ref, h, w2, eblk, eover, mine, theirs,
                hs, wbuf, tbuf, zbuf, kbuf, pbuf, abuf, wsplit, ng, eoff, est, boff, nsb_g, gdst, trow, tnum, hsem, wsem, gsem, zsem, osem, ksem):
    def w_copy(e, slot):
        return pltpu.make_async_copy(w2.at[e], wbuf.at[slot], wsem.at[slot])

    def h_copy(t, slot):
        return pltpu.make_async_copy(h.at[pl.ds(pl.multiple_of(trow[t] * G, G), TM), :], hs.at[slot], hsem.at[slot])

    def z_copy(s, k):
        return pltpu.make_async_copy(zbuf, eblk.at[s, pl.ds(pl.multiple_of(k * G, G), G), :], zsem.at[0])

    w_copy(0, 0).start()
    zbuf[...] = jnp.zeros_like(zbuf)
    offsets(cnt_ref, ng, eoff, est, boff, nsb_g)
    nt = jnp.int32(0)
    for e in range(NE):
        rows_g = est[e + 1] - est[e]
        tiles = (rows_g + TM // G - 1) // (TM // G)

        def note(m, _, e=e, nt=nt, rows_g=rows_g):
            trow[nt + m] = est[e] + m * (TM // G)
            tnum[nt + m] = jnp.minimum(rows_g - m * (TM // G), TM // G)
            return 0

        lax.fori_loop(0, tiles, note, 0)
        nt = nt + tiles

    @pl.when(nt > 0)
    def _():
        h_copy(0, 0).start()

    w_copy(1, 1).start()
    w_copy(2, 2).start()

    def seg_note(q, _):
        def one(g, _):
            gdst[eoff[q] + g] = (q // NE) * 256 + boff[q] + g
            return 0

        return lax.fori_loop(0, ng[q], one, 0)

    lax.fori_loop(0, NSB * NE, seg_note, 0)
    for s in range(NSB):
        def zero(k, _, s=s):
            z_copy(s, k).start()
            return 0

        lax.fori_loop(nsb_g[s], KC // G, zero, 0)

    most = jnp.maximum(jnp.maximum(nsb_g[0], nsb_g[1]), jnp.maximum(nsb_g[2], nsb_g[3]))
    over = most > KC // G

    def g_wait(slot, n):
        def one(j, _):
            pltpu.make_async_copy(tbuf.at[slot, pl.ds(0, G), :], eblk.at[0, pl.ds(0, G), :], gsem.at[slot]).wait()
            return 0

        lax.fori_loop(0, n, one, 0)

    def expert(e, t):
        ws = lax.rem(e, 3)
        w_copy(e, ws).wait()

        def tile(m, t):
            slot = lax.rem(t, 2)

            @pl.when(t + 1 < nt)
            def _():
                h_copy(t + 1, 1 - slot).start()

            @pl.when(t >= 2)
            def _():
                g_wait(slot, tnum[jnp.maximum(t - 2, 0)])

            h_copy(t, slot).wait()
            n = tnum[t]
            for size in (64, 128, 192, 256):
                @pl.when((n > size // G - 4) & (n <= size // G))
                def _(size=size):
                    for c in range(D // 512):
                        cols = slice(c * 512, c * 512 + 512)
                        tbuf[slot, :size, cols] = jnp.dot(hs[slot, :size, :], wbuf[ws, :, cols], preferred_element_type=F32).astype(BF16)

            def put(j, _):
                at = gdst[trow[t] + j]
                s, k = at // 256, at % 256
                src = tbuf.at[slot, pl.ds(pl.multiple_of(j * G, G), G), :]

                @pl.when(k < KC // G)
                def _():
                    pltpu.make_async_copy(src, eblk.at[s, pl.ds(pl.multiple_of(k * G, G), G), :], gsem.at[slot]).start()

                @pl.when(k >= KC // G)
                def _():
                    pltpu.make_async_copy(src, eover.at[s, pl.ds(pl.multiple_of(k * G - KC, G), G), :], gsem.at[slot]).start()

                return 0

            lax.fori_loop(0, n, put, 0)
            return t + 1

        t = lax.fori_loop(0, (est[e + 1] - est[e] + TM // G - 1) // (TM // G), tile, t)

        @pl.when(e + 3 < NE)
        def _():
            w_copy(e + 3, ws).start()

        return t

    lax.fori_loop(0, NE, expert, jnp.int32(0))
    for back in (1, 2):
        @pl.when(nt >= back)
        def _(back=back):
            t = jnp.maximum(nt - back, 0)
            g_wait(lax.rem(t, 2), tnum[t])

    for s in range(NSB):
        def zero_wait(k, _, s=s):
            z_copy(s, k).wait()
            return 0

        lax.fori_loop(nsb_g[s], KC // G, zero_wait, 0)

    @pl.when(over)
    def _():
        rows16 = lax.broadcasted_iota(jnp.int32, (G, SB), 0)
        pbuf[...] = jnp.zeros_like(pbuf)
        for s in range(NSB):
            w = wt_ref[s]
            hi = w.astype(BF16).astype(F32)
            mid = (w - hi).astype(BF16).astype(F32)
            wsplit[0, s] = hi
            wsplit[1, s] = mid
            wsplit[2, s] = w - hi - mid

        def segment(q, _):
            s, e = q // NE, q % NE
            rk = jnp.broadcast_to(rank_ref[s, pl.ds(e, 1), :], (G, SB))
            parts = [jnp.broadcast_to(wsplit[i, s, pl.ds(e, 1), :], (G, SB)) for i in range(3)]

            def build(g, _):
                k = boff[q] + g

                @pl.when(k >= KC // G)
                def _():
                    row = pl.multiple_of((k - KC // G) * G, G)
                    hit = rk == rows16 + g * G
                    for i in range(3):
                        pbuf[s, i, pl.ds(row, G), :] = jnp.where(hit, parts[i], 0.0).astype(BF16)

                return 0

            return lax.fori_loop(0, ng[q], build, 0)

        lax.fori_loop(0, NSB * NE, segment, 0)
        core = core_ref[0]
        keep = pl.multiple_of(core * 256, 256)
        give = pl.multiple_of(256 - core * 256, 256)

        def piece(q, _):
            s, c = q // (D // CW), q % (D // CW)
            rel = core_ref[1 + s]
            get = pltpu.make_async_copy(eover.at[s, :, pl.ds(pl.multiple_of(c * CW, CW), CW)], kbuf, ksem.at[0])
            get.start()
            get.wait()

            def clear(k, _):
                kbuf[pl.ds(pl.multiple_of(k * G, G), G), :] = jnp.zeros((G, CW), BF16)
                return 0

            lax.fori_loop(jnp.maximum(nsb_g[s] - KC // G, 0), KX // G, clear, 0)
            abuf[...] = jnp.zeros_like(abuf)

            def part(kt, _):
                rows = pl.ds(pl.multiple_of(kt * TM, TM), TM)
                for i in range(3):
                    abuf[...] += lax.dot_general(pbuf[s, i, rows, :], kbuf[rows, :], (((0,), (0,)), ((), ())), preferred_element_type=F32)
                return 0

            lax.fori_loop(0, KX // TM, part, 0)
            copies = []
            for i in range(CW // RC):
                cols = pl.ds(i * RC, RC)
                j = c * (CW // RC) + i
                copies.append(pltpu.make_async_copy(abuf.at[pl.ds(give, 256), cols], theirs.at[j, rel], osem.at[i, 0]))
                copies.append(pltpu.make_async_copy(abuf.at[pl.ds(keep, 256), cols], mine.at[j, rel], osem.at[i, 1]))
            for cp in copies:
                cp.start()
            for cp in copies:
                cp.wait()
            return 0

        lax.fori_loop(0, NSB * (D // CW), piece, 0)


def down_call(cnt, core, rank, wts, h, w2):
    any_spec = pl.BlockSpec(memory_space=pl.ANY)
    smem = pl.BlockSpec(memory_space=pltpu.SMEM)
    vmem = pl.BlockSpec(memory_space=pltpu.VMEM)
    out = jax.ShapeDtypeStruct((NC, NSB, 256, RC), F32)
    return pl.pallas_call(
        down_kernel,
        out_shape=(jax.ShapeDtypeStruct((NSB, KC, D), BF16), jax.ShapeDtypeStruct((NSB, KX, D), BF16), out, out),
        in_specs=[smem, smem, vmem, vmem, any_spec, any_spec],
        out_specs=(any_spec, any_spec, any_spec, any_spec),
        scratch_shapes=[
            pltpu.VMEM((2, TM, FF), BF16),
            pltpu.VMEM((3, FF, D), BF16),
            pltpu.VMEM((2, TM, D), BF16),
            pltpu.VMEM((G, D), BF16),
            pltpu.VMEM((KX, CW), BF16),
            pltpu.VMEM((NSB, 3, KX, SB), BF16),
            pltpu.VMEM((SB, CW), F32),
            pltpu.VMEM((3, NSB, NE, SB), F32),
            pltpu.SMEM((NSB * NE,), jnp.int32),
            pltpu.SMEM((NSB * NE,), jnp.int32),
            pltpu.SMEM((NE + 1,), jnp.int32),
            pltpu.SMEM((NSB * NE,), jnp.int32),
            pltpu.SMEM((NSB,), jnp.int32),
            pltpu.SMEM((XG,), jnp.int32),
            pltpu.SMEM((64,), jnp.int32),
            pltpu.SMEM((64,), jnp.int32),
            pltpu.SemaphoreType.DMA((2,)),
            pltpu.SemaphoreType.DMA((3,)),
            pltpu.SemaphoreType.DMA((2,)),
            pltpu.SemaphoreType.DMA((1,)),
            pltpu.SemaphoreType.DMA((CW // RC, 2)),
            pltpu.SemaphoreType.DMA((1,)),
        ],
        compiler_params=pltpu.CompilerParams(vmem_limit_bytes=VMEM_LIMIT),
        cost_estimate=pl.CostEstimate(flops=40_000_000_000, bytes_accessed=100_000_000, transcendentals=0),
        name="down",
    )(cnt, core, rank, wts, h, w2)


def neighbours():
    me = lax.axis_index('ep')
    core = me + 1 - 2 * (me % 2)
    x = me + 2 - 4 * ((me // 2) % 2)
    y = me + 4 - 8 * (me // 4)
    return me, core, x, y


def remote(src, dst, send, recv, dev):
    return pltpu.make_async_remote_copy(src_ref=src, dst_ref=dst, send_sem=send, recv_sem=recv, device_id={'ep': dev}, device_id_type=pl.DeviceIdType.MESH)


def enter(others):
    barrier = pltpu.get_barrier_semaphore()
    for dev in others:
        pl.semaphore_signal(barrier, inc=1, device_id={'ep': dev}, device_id_type=pl.DeviceIdType.MESH)
    pl.semaphore_wait(barrier, len(others))


def gather_kernel(b_any, b_ref, wts_ref, w1, w3, w2, ball, wall_out, rank_ref, cnt_ref, pt, s_ref, wall, ptbuf, cols_buf, w13buf, w2buf, acc, send, recv, wsend, wrecv, local, wsem, psem):
    me, pn, xn, yn = neighbours()
    diag = xn + yn - me
    half = T // 2

    def rows(dev, h):
        return pl.ds(pl.multiple_of(dev * T + h * half, half), half)

    def own(k, h, dev):
        return remote(b_any.at[pl.ds(h * half, half), :], ball.at[rows(me, h), :], send.at[k], recv.at[k], dev)

    def relay(k, owner, h, dev):
        return remote(ball.at[rows(owner, h), :], ball.at[rows(owner, h), :], send.at[k], recv.at[k], dev)

    def w_copies(st, slot):
        cols = pl.ds(pl.multiple_of(st * SF, SF), SF)
        return (pltpu.make_async_copy(w1.at[:, cols], w13buf.at[slot, 0], wsem.at[slot, 0]),
                pltpu.make_async_copy(w3.at[:, cols], w13buf.at[slot, 1], wsem.at[slot, 1]),
                pltpu.make_async_copy(w2.at[cols, :], w2buf.at[slot], wsem.at[slot, 2]))

    for st in range(3):
        for c in w_copies(st, st):
            c.start()
    others = [lax.rem(me + k, 8) for k in range(1, 8)]
    enter(others)
    first = [own(0, 0, xn), own(2, 1, yn), own(1, 1, xn), own(3, 0, yn), own(4, 0, pn), own(5, 1, pn)]
    for c in first:
        c.start()
    lanes = pl.ds(pl.multiple_of((me % 2) * T, T), T)
    small = []
    for k, dev in enumerate(others):
        small.append(remote(wts_ref.at[pl.ds(pl.multiple_of(dev * NE, NE), NE), :], wall.at[me // 2, :, lanes], wsend.at[k], wrecv.at[k], dev))
        small[-1].start()
    keep = [pltpu.make_async_copy(b_ref, ball.at[pl.ds(pl.multiple_of(me * T, T), T), :], local.at[0]),
            pltpu.make_async_copy(wts_ref.at[pl.ds(pl.multiple_of(me * NE, NE), NE), :], wall.at[me // 2, :, lanes], local.at[1])]
    for c in keep:
        c.start()
    acc[...] = jnp.zeros_like(acc)

    def step(st, _):
        slot = lax.rem(st, 3)
        for c in w_copies(st, slot):
            c.wait()
        x = b_ref[...]
        gate = jnp.dot(x, w13buf[slot, 0], preferred_element_type=F32)
        lin = jnp.dot(x, w13buf[slot, 1], preferred_element_type=F32)
        inner = (jax.nn.silu(gate) * lin).astype(BF16)
        for n in range(D // 512):
            cols = slice(n * 512, n * 512 + 512)
            acc[:, cols] += jnp.dot(inner, w2buf[slot, :, cols], preferred_element_type=F32)

        return 0

    def refill(st, _):
        step(st, 0)
        for c in w_copies(st + 3, lax.rem(st, 3)):
            c.start()
        return 0

    lax.fori_loop(0, 8, refill, 0)
    first[0].wait_recv()
    first[1].wait_recv()
    second = [relay(6, xn, 0, yn), relay(7, yn, 1, xn), relay(8, xn, 0, pn), relay(9, yn, 1, pn)]
    for c in second:
        c.start()
    lax.fori_loop(8, SHARED // SF - 3, refill, 0)
    lax.fori_loop(SHARED // SF - 3, SHARED // SF, step, 0)
    s_ref[...] = acc[...].astype(BF16)
    first[2].wait_recv()
    first[3].wait_recv()
    third = [relay(10, xn, 1, pn), relay(11, yn, 0, pn)]
    for c in third:
        c.start()
    for c in small:
        c.wait_recv()
    keep[1].wait()
    before = jnp.where(lax.broadcasted_iota(jnp.int32, (SB, SB), 0) < lax.broadcasted_iota(jnp.int32, (SB, SB), 1), 1.0, 0.0).astype(BF16)
    row = lax.broadcasted_iota(jnp.int32, (1, KC), 1)
    puts = []
    for s in range(NSB):
        slot = s % 2
        w = wall[s]
        wall_out[s] = w
        sel = jnp.where(w >= 0.0, 1.0, 0.0)
        rank = jnp.where(w >= 0.0, jnp.dot(sel.astype(BF16), before, preferred_element_type=F32), -1.0)
        rank_ref[s] = rank.astype(jnp.int32)
        count = jnp.sum(sel, axis=1, keepdims=True).astype(jnp.int32)
        cnt_ref[s] = jnp.broadcast_to(count, (NE, 128))
        wide = jnp.broadcast_to(count, (NE, KC))
        start = jnp.zeros((1, KC), jnp.int32)
        local_row = []
        for e in range(NE):
            n = wide[e:e + 1]
            at = row - start
            local_row.append(jnp.where((at >= 0) & (at < n), at, -2).astype(F32))
            start = start + (n + (G - 1)) // G * G
        pad = jnp.zeros((128 - NE, SB), F32)
        cols_buf[0] = jnp.concatenate([rank, pad], axis=0).T
        cols_buf[1] = jnp.concatenate([w, pad], axis=0).T
        if s >= 2:
            puts[s - 2].wait()

        def fill(tb, _, slot=slot, local_row=local_row):
            toks = pl.ds(pl.multiple_of(tb * 32, 32), 32)
            rk = cols_buf[0, toks, :]
            wt = cols_buf[1, toks, :]
            total = jnp.zeros((32, KC), F32)
            for e in range(NE):
                total = jnp.where(rk[:, e:e + 1] == local_row[e], wt[:, e:e + 1], total)
            hi = total.astype(BF16)
            rest = total - hi.astype(F32)
            mid = rest.astype(BF16)
            ptbuf[slot, 0, toks, :] = hi
            ptbuf[slot, 1, toks, :] = mid
            ptbuf[slot, 2, toks, :] = (rest - mid.astype(F32)).astype(BF16)
            return 0

        lax.fori_loop(0, SB // 32, fill, 0)
        puts.append(pltpu.make_async_copy(ptbuf.at[slot], pt.at[s], psem.at[slot]))
        puts[s].start()
    second[0].wait_recv()
    second[1].wait_recv()
    fourth = [relay(12, diag, 0, pn), relay(13, diag, 1, pn)]
    for c in fourth:
        c.start()
    for c in (first[4], first[5], second[2], second[3], *third, *fourth):
        c.wait_recv()
    for c in (*first, *second, *third, *fourth):
        c.wait_send()
    for c in small:
        c.wait_send()
    keep[0].wait()
    puts[2].wait()
    puts[3].wait()


def gather_call(b, wts, w1, w3, w2):
    any_spec = pl.BlockSpec(memory_space=pl.ANY)
    vmem = pl.BlockSpec(memory_space=pltpu.VMEM)
    return pl.pallas_call(
        gather_kernel,
        out_shape=(
            jax.ShapeDtypeStruct((8 * T, D), BF16),
            jax.ShapeDtypeStruct((NSB, NE, SB), F32),
            jax.ShapeDtypeStruct((NSB, NE, SB), jnp.int32),
            jax.ShapeDtypeStruct((NSB, NE, 128), jnp.int32),
            jax.ShapeDtypeStruct((NSB, 3, SB, KC), BF16),
            jax.ShapeDtypeStruct((T, D), BF16),
        ),
        in_specs=[any_spec, vmem, vmem, any_spec, any_spec, any_spec],
        out_specs=(any_spec, vmem, vmem, vmem, any_spec, vmem),
        scratch_shapes=[
            pltpu.VMEM((NSB, NE, SB), F32),
            pltpu.VMEM((2, 3, SB, KC), BF16),
            pltpu.VMEM((2, SB, 128), F32),
            pltpu.VMEM((3, 2, D, SF), BF16),
            pltpu.VMEM((3, SF, D), BF16),
            pltpu.VMEM((T, D), F32),
            pltpu.SemaphoreType.DMA((14,)),
            pltpu.SemaphoreType.DMA((14,)),
            pltpu.SemaphoreType.DMA((7,)),
            pltpu.SemaphoreType.DMA((7,)),
            pltpu.SemaphoreType.DMA((2,)),
            pltpu.SemaphoreType.DMA((3, 3)),
            pltpu.SemaphoreType.DMA((2,)),
        ],
        compiler_params=pltpu.CompilerParams(collective_id=0, has_side_effects=True, vmem_limit_bytes=VMEM_LIMIT),
        cost_estimate=pl.CostEstimate(flops=12_000_000_000, bytes_accessed=60_000_000, transcendentals=0),
        name="gather",
    )(b, b, wts, w1, w3, w2)


def return_kernel(cnt_ref, pt, eblk, mine, theirs, y_ref, s_ref, out_ref, ptv, ev, own, give, r1, r2x, r2y, r3x, r3y, send, recv, load, esem, psem):
    me, pn, xn, yn = neighbours()
    half = T // 2
    top, low = pl.ds(0, half), pl.ds(half, half)

    def load_of(j):
        return (pltpu.make_async_copy(theirs.at[j], give.at[j], load.at[0, j]), pltpu.make_async_copy(mine.at[j], own.at[j], load.at[1, j]))

    def e_of(j, slot):
        return pltpu.make_async_copy(eblk.at[:, :, pl.ds(pl.multiple_of(j * RC, RC), RC)], ev.at[slot], esem.at[slot])

    def core_of(j):
        return remote(give.at[j], r1.at[j], send.at[0, j], recv.at[0, j], pn)

    def x_of(j):
        return remote(own.at[j, pl.ds(1, 2), top, :], r2x.at[j], send.at[1, j], recv.at[1, j], xn)

    def y_of(j):
        return remote(own.at[j, pl.ds(2, 2), low, :], r2y.at[j], send.at[2, j], recv.at[2, j], yn)

    def y_last(j):
        return remote(own.at[j, 3, top, :], r3y.at[j], send.at[3, j], recv.at[3, j], yn)

    def x_last(j):
        return remote(own.at[j, 1, low, :], r3x.at[j], send.at[4, j], recv.at[4, j], xn)

    def each(body):
        def run(j, _):
            body(j)
            return 0

        lax.fori_loop(0, NC, run, 0)

    rows_over = jnp.int32(0)
    for s in range(NSB):
        n = jnp.int32(0)
        for e in range(NE):
            n = n + (cnt_ref[s, e] + (G - 1)) // G
        rows_over = jnp.maximum(rows_over, n - KC // G)
    over = jnp.full((T, RC), rows_over, jnp.int32) > 0

    def begin(j):
        for c in load_of(j):
            c.start()

    def add_up(j, buf, first_tok):
        slot = lax.rem(j, 2)
        toks = pl.ds(pl.multiple_of(first_tok, T), T)

        def block(s, _):
            dx = lax.rem(lax.rem(s, 2) + lax.rem(me // 2, 2), 2)
            dy = lax.rem(s // 2 + me // 4, 2)
            place = dx + 3 * dy - 2 * dx * dy
            total = jnp.where(over, buf[j, place], 0.0)
            ek = ev[slot, s]
            for i in range(3):
                total = total + jnp.dot(ptv[s, i, toks, :], ek, preferred_element_type=F32)
            buf[j, place] = total
            return 0

        lax.fori_loop(0, NSB, block, 0)

    def make(j):
        e_of(j, lax.rem(j, 2)).wait()
        for c in load_of(j):
            c.wait()
        add_up(j, give, T - lax.rem(me, 2) * T)
        core_of(j).start()
        add_up(j, own, lax.rem(me, 2) * T)

    def pair(j):
        core_of(j).wait_recv()
        own[j, 1:] = own[j, 1:] + r1[j, 1:]
        x_of(j).start()
        y_of(j).start()
        own[j, 0] = own[j, 0] + r1[j, 0]

    def onward(j):
        x_of(j).wait_recv()
        own[j, 3, :half] = own[j, 3, :half] + r2x[j, 1]
        y_last(j).start()
        y_of(j).wait_recv()
        own[j, 1, half:] = own[j, 1, half:] + r2y[j, 0]
        x_last(j).start()

    def finish(j):
        cols = pl.ds(pl.multiple_of(j * RC, RC), RC)
        y_last(j).wait_recv()
        x_last(j).wait_recv()
        base = y_ref[:, cols].astype(F32) + s_ref[:, cols].astype(F32)
        out_ref[:half, cols] = (base[:half] + (own[j, 0, :half] + r2x[j, 0] + r3y[j])).astype(BF16)
        out_ref[half:, cols] = (base[half:] + (own[j, 0, half:] + r2y[j, 1] + r3x[j])).astype(BF16)

    def drain(j):
        for c in (core_of(j), x_of(j), y_of(j), y_last(j), x_last(j)):
            c.wait_send()

    e_of(0, 0).start()
    pt_copies = [pltpu.make_async_copy(pt.at[s], ptv.at[s], psem.at[s]) for s in range(NSB)]
    for c in pt_copies:
        c.start()
    e_of(1, 1).start()
    enter([pn, xn, yn])
    each(begin)
    for c in pt_copies:
        c.wait()

    def steady(j, _):
        make(j)

        @pl.when(j + 2 < NC)
        def _():
            e_of(j + 2, lax.rem(j, 2)).start()

        pair(j)
        return 0

    lax.fori_loop(0, NC, steady, 0)
    each(onward)
    each(finish)
    each(drain)


def return_call(cnt, pt, eblk, mine, theirs, hidden, shared_out):
    any_spec = pl.BlockSpec(memory_space=pl.ANY)
    vmem = pl.BlockSpec(memory_space=pltpu.VMEM)
    half = T // 2
    return pl.pallas_call(
        return_kernel,
        out_shape=jax.ShapeDtypeStruct((T, D), BF16),
        in_specs=[pl.BlockSpec(memory_space=pltpu.SMEM), any_spec, any_spec, any_spec, any_spec, vmem, vmem],
        out_specs=vmem,
        scratch_shapes=[
            pltpu.VMEM((NSB, 3, SB, KC), BF16),
            pltpu.VMEM((2, NSB, KC, RC), BF16),
            pltpu.VMEM((NC, NSB, T, RC), F32),
            pltpu.VMEM((NC, NSB, T, RC), F32),
            pltpu.VMEM((NC, NSB, T, RC), F32),
            pltpu.VMEM((NC, 2, half, RC), F32),
            pltpu.VMEM((NC, 2, half, RC), F32),
            pltpu.VMEM((NC, half, RC), F32),
            pltpu.VMEM((NC, half, RC), F32),
            pltpu.SemaphoreType.DMA((5, NC)),
            pltpu.SemaphoreType.DMA((5, NC)),
            pltpu.SemaphoreType.DMA((2, NC)),
            pltpu.SemaphoreType.DMA((2,)),
            pltpu.SemaphoreType.DMA((NSB,)),
        ],
        compiler_params=pltpu.CompilerParams(collective_id=1, has_side_effects=True, vmem_limit_bytes=VMEM_LIMIT),
        name="return_sum",
    )(cnt, pt, eblk, mine, theirs, hidden, shared_out)


def solution(mesh):
    tok_spec = P(('dp', 'ep'), None)
    expert_spec = P('ep', None, None)

    def local_fn(hidden, norm_gain, w_gate, w1_shared, w3_shared, w2_shared, w1_experts, w3_experts, w2_experts, topk_ids):
        normed = rms_norm(hidden, norm_gain)
        probs = jax.nn.softmax(jnp.dot(normed, w_gate, preferred_element_type=F32), axis=-1)
        chosen = jnp.any(topk_ids[:, :, None] == jnp.arange(EXPERTS), axis=1)
        gate_wts = jnp.where(chosen, ROUTE_SCALE * probs, -1.0).T
        ball, wsb, rank, counts, pt, shared_out = gather_call(normed, gate_wts, w1_shared, w3_shared, w2_shared)
        cnt = counts[:, :, 0]
        me = lax.axis_index('ep')
        chip, at = me // 2, jnp.arange(NSB)
        other_x, other_y = at % 2 != chip % 2, at // 2 != chip // 2
        place = jnp.where(other_x, jnp.where(other_y, 2, 1), jnp.where(other_y, 3, 0))
        core = jnp.concatenate([(me % 2)[None], place]).astype(jnp.int32)
        h = up_call(cnt, rank, ball, w1_experts, w3_experts)
        eblk, _, mine, theirs = down_call(cnt, core, rank, wsb, h, w2_experts)
        return return_call(cnt, pt, eblk, mine, theirs, hidden, shared_out)

    return jax.shard_map(local_fn, mesh=mesh, in_specs=(tok_spec, P(), P(), P(), P(), P(), expert_spec, expert_spec, expert_spec, tok_spec), out_specs=tok_spec, check_vma=False)
```

```python
import functools

import jax
import jax.numpy as jnp
from jax import lax
from jax.experimental import pallas as pl
from jax.experimental.pallas import tpu as pltpu
from jax.sharding import PartitionSpec as P

ROUTE_SCALE = 16
NORM_EPS = 1e-6
D = 2560
FF = 1536
EXPERTS = 64
NE = 8
NSB = 4
SB = 512
G = 16
TM = 256
LM = 384
SIZES = tuple(range(64, LM + 1, 64))
XG = 440
XR = XG * G
SBR = 1792
FC = 512
NF = FF // FC
DH = D // 2
T = 256
SHARED = 3072
SF = 256
CW = 512
RC = 256
NC = D // RC
KC = 768
KX = SBR - KC
LAG = 2
VMEM_LIMIT = 66000000
BF16 = jnp.bfloat16
F32 = jnp.float32


def rms_norm(hidden, norm_gain):
    rows_f = hidden.astype(F32)
    inv_rms = lax.rsqrt(jnp.mean(rows_f * rows_f, axis=-1, keepdims=True) + NORM_EPS)
    return (rows_f * inv_rms * norm_gain.astype(F32)).astype(BF16)


def offsets(cnt_ref, ng, eoff, est, boff, nsb_g):
    run = jnp.int32(0)
    for e in range(NE):
        est[e] = run
        for s in range(NSB):
            n = (cnt_ref[s, e] + (G - 1)) // G
            ng[s * NE + e] = n
            eoff[s * NE + e] = run
            run = run + n
    est[NE] = run
    for s in range(NSB):
        b = jnp.int32(0)
        for e in range(NE):
            boff[s * NE + e] = b
            b = b + ng[s * NE + e]
        nsb_g[s] = b


def up_kernel(cnt_ref, rank_ref, ball, w1, w3, h_out, xs, bbuf, pbuf, tbuf, wbuf, hbuf, ng, eoff, est, boff, nsb_g, dst, last, bsem, wsem, hsem):
    def w_copies(step, slot):
        e = step // NF
        f = step % NF
        cols = pl.ds(pl.multiple_of(f * FC, FC), FC)
        return (pltpu.make_async_copy(w1.at[e, :, cols], wbuf.at[slot, 0], wsem.at[slot, 0]),
                pltpu.make_async_copy(w3.at[e, :, cols], wbuf.at[slot, 1], wsem.at[slot, 1]))

    def b_copy(s, half):
        return pltpu.make_async_copy(ball.at[pl.ds(s * SB, SB), pl.ds(half * DH, DH)], bbuf.at[half], bsem.at[half])

    b_copy(0, 0).start()
    b_copy(0, 1).start()
    for st in range(3):
        for c in w_copies(st, st):
            c.start()
    offsets(cnt_ref, ng, eoff, est, boff, nsb_g)
    rows16 = lax.broadcasted_iota(jnp.int32, (G, SB), 0)

    for s in range(NSB):
        for e in range(NE):
            rk = jnp.broadcast_to(rank_ref[s, e:e + 1, :], (G, SB))

            def build(g, _, s=s, e=e, rk=rk):
                k = boff[s * NE + e] + g
                dst[k] = eoff[s * NE + e] + g
                hit = jnp.where(rk == rows16 + g * G, 1.0, 0.0)
                pbuf[pl.ds(pl.multiple_of(k * G, G), G), :] = hit.astype(BF16)
                return 0

            lax.fori_loop(0, ng[s * NE + e], build, 0)
        for half in range(2):
            b_copy(s, half).wait()

            def tile(m, _, s=s, half=half):
                prow = pbuf[pl.ds(pl.multiple_of(m * TM, TM), TM), :]
                for n in range(5):
                    cols = slice(n * 256, (n + 1) * 256)
                    tbuf[:, cols] = jnp.dot(prow, bbuf[half, :, cols], preferred_element_type=F32).astype(BF16)

                def put(j, _):
                    row = pl.multiple_of(dst[m * (TM // G) + j] * G, G)
                    xs[pl.ds(row, G), half * DH:(half + 1) * DH] = tbuf[pl.ds(pl.multiple_of(j * G, G), G), :]
                    return 0

                lax.fori_loop(0, jnp.minimum(TM // G, nsb_g[s] - m * (TM // G)), put, 0)
                return 0

            lax.fori_loop(0, (nsb_g[s] + TM // G - 1) // (TM // G), tile, 0)
            if s + 1 < NSB:
                b_copy(s + 1, half).start()

    def h_copy(hs, row, col, size):
        return pltpu.make_async_copy(hbuf.at[hs, pl.ds(0, size), :], h_out.at[pl.ds(row, size), pl.ds(col, FC)], hsem.at[0])

    def wait_h(quarters):
        for q in range(1, LM // 64 + 1):
            @pl.when(quarters == q)
            def _(q=q):
                h_copy(0, 0, 0, q * 64).wait()

    def step(st, k):
        slot = lax.rem(st, 3)
        e = st // NF
        col = pl.multiple_of((st % NF) * FC, FC)
        for c in w_copies(st, slot):
            c.wait()
        base = est[e] * G
        rows = est[e + 1] * G - base

        def work(row, size, k):
            row = pl.multiple_of(row, G)
            hs = k % 2
            for n in range(FC // 256):
                cols = slice(n * 256, (n + 1) * 256)
                x = xs[pl.ds(row, size), :]
                gate = jnp.dot(x, wbuf[slot, 0, :, cols], preferred_element_type=F32)
                lin = jnp.dot(x, wbuf[slot, 1, :, cols], preferred_element_type=F32)
                hbuf[hs, pl.ds(0, size), cols] = (jax.nn.silu(gate) * lin).astype(BF16)

            @pl.when(k > 0)
            def _():
                wait_h(last[0])

            last[0] = size // 64
            h_copy(hs, row, col, size).start()

        full = jnp.maximum(rows - LM + TM - 1, 0) // TM

        def body(m, k):
            work(base + m * TM, TM, k)
            return k + 1

        k = lax.fori_loop(0, full, body, k)
        rem = rows - full * TM
        at = base + full * TM
        for size in SIZES:
            @pl.when((rem > size - 64) & (rem <= size))
            def _(size=size):
                work(at, size, k)

        @pl.when(st + 3 < NE * NF)
        def _():
            for c in w_copies(st + 3, slot):
                c.start()

        return k + jnp.where(rem > 0, 1, 0)

    @pl.when(lax.fori_loop(0, NE * NF, step, jnp.int32(0)) > 0)
    def _():
        wait_h(last[0])


def up_call(cnt, rank, ball, w1, w3):
    any_spec = pl.BlockSpec(memory_space=pl.ANY)
    return pl.pallas_call(
        up_kernel,
        out_shape=jax.ShapeDtypeStruct((XR, FF), BF16),
        in_specs=[pl.BlockSpec(memory_space=pltpu.SMEM), pl.BlockSpec(memory_space=pltpu.VMEM), any_spec, any_spec, any_spec],
        out_specs=any_spec,
        scratch_shapes=[
            pltpu.VMEM((XR, D), BF16),
            pltpu.VMEM((2, SB, DH), BF16),
            pltpu.VMEM((SBR, SB), BF16),
            pltpu.VMEM((TM, DH), BF16),
            pltpu.VMEM((3, 2, D, FC), BF16),
            pltpu.VMEM((2, LM, FC), BF16),
            pltpu.SMEM((NSB * NE,), jnp.int32),
            pltpu.SMEM((NSB * NE,), jnp.int32),
            pltpu.SMEM((NE + 1,), jnp.int32),
            pltpu.SMEM((NSB * NE,), jnp.int32),
            pltpu.SMEM((NSB,), jnp.int32),
            pltpu.SMEM((SBR // G,), jnp.int32),
            pltpu.SMEM((1,), jnp.int32),
            pltpu.SemaphoreType.DMA((2,)),
            pltpu.SemaphoreType.DMA((3, 2)),
            pltpu.SemaphoreType.DMA((1,)),
        ],
        compiler_params=pltpu.CompilerParams(vmem_limit_bytes=VMEM_LIMIT),
        cost_estimate=pl.CostEstimate(flops=48_000_000_000, bytes_accessed=140_000_000, transcendentals=0),
        name="up",
    )(cnt, rank, ball, w1, w3)


def down_kernel(cnt_ref, core_ref, rank_ref, wt_ref, h, w2, eblk, eover, mine, theirs,
                hs, wbuf, tbuf, zbuf, kbuf, pbuf, abuf, wsplit, ng, eoff, est, boff, nsb_g, gdst, trow, tnum, hsem, wsem, gsem, zsem, osem, ksem):
    def w_copy(e, slot):
        return pltpu.make_async_copy(w2.at[e], wbuf.at[slot], wsem.at[slot])

    def h_copy(t, slot):
        return pltpu.make_async_copy(h.at[pl.ds(pl.multiple_of(trow[t] * G, G), LM), :], hs.at[slot], hsem.at[slot])

    def z_copy(s, k):
        return pltpu.make_async_copy(zbuf, eblk.at[s, pl.ds(pl.multiple_of(k * G, G), G), :], zsem.at[0])

    def tiles_of(rows_g):
        return jnp.maximum(rows_g - LM // G + TM // G - 1, 0) // (TM // G) + jnp.where(rows_g > 0, 1, 0)

    w_copy(0, 0).start()
    zbuf[...] = jnp.zeros_like(zbuf)
    offsets(cnt_ref, ng, eoff, est, boff, nsb_g)
    nt = jnp.int32(0)
    for e in range(NE):
        rows_g = est[e + 1] - est[e]
        tiles = tiles_of(rows_g)

        def note(m, _, e=e, nt=nt, rows_g=rows_g, tiles=tiles):
            trow[nt + m] = est[e] + m * (TM // G)
            tnum[nt + m] = jnp.where(m == tiles - 1, rows_g - m * (TM // G), TM // G)
            return 0

        lax.fori_loop(0, tiles, note, 0)
        nt = nt + tiles

    @pl.when(nt > 0)
    def _():
        h_copy(0, 0).start()

    w_copy(1, 1).start()
    w_copy(2, 2).start()

    def seg_note(q, _):
        def one(g, _):
            gdst[eoff[q] + g] = (q // NE) * 256 + boff[q] + g
            return 0

        return lax.fori_loop(0, ng[q], one, 0)

    lax.fori_loop(0, NSB * NE, seg_note, 0)
    for s in range(NSB):
        def zero(k, _, s=s):
            z_copy(s, k).start()
            return 0

        lax.fori_loop(nsb_g[s], KC // G, zero, 0)

    most = jnp.maximum(jnp.maximum(nsb_g[0], nsb_g[1]), jnp.maximum(nsb_g[2], nsb_g[3]))
    over = most > KC // G

    def g_wait(slot, n):
        def one(j, _):
            pltpu.make_async_copy(tbuf.at[slot, pl.ds(0, G), :], eblk.at[0, pl.ds(0, G), :], gsem.at[slot]).wait()
            return 0

        lax.fori_loop(0, n, one, 0)

    def expert(e, t):
        ws = lax.rem(e, 3)
        w_copy(e, ws).wait()

        def tile(m, t):
            slot = lax.rem(t, 2)

            @pl.when(t + 1 < nt)
            def _():
                h_copy(t + 1, 1 - slot).start()

            @pl.when(t >= 2)
            def _():
                g_wait(slot, tnum[jnp.maximum(t - 2, 0)])

            h_copy(t, slot).wait()
            n = tnum[t]
            for size in SIZES:
                @pl.when((n > size // G - 4) & (n <= size // G))
                def _(size=size):
                    for c in range(D // 512):
                        cols = slice(c * 512, c * 512 + 512)
                        tbuf[slot, :size, cols] = jnp.dot(hs[slot, :size, :], wbuf[ws, :, cols], preferred_element_type=F32).astype(BF16)

            def put(j, _):
                at = gdst[trow[t] + j]
                s, k = at // 256, at % 256
                src = tbuf.at[slot, pl.ds(pl.multiple_of(j * G, G), G), :]

                @pl.when(k < KC // G)
                def _():
                    pltpu.make_async_copy(src, eblk.at[s, pl.ds(pl.multiple_of(k * G, G), G), :], gsem.at[slot]).start()

                @pl.when(k >= KC // G)
                def _():
                    pltpu.make_async_copy(src, eover.at[s, pl.ds(pl.multiple_of(k * G - KC, G), G), :], gsem.at[slot]).start()

                return 0

            lax.fori_loop(0, n, put, 0)
            return t + 1

        t = lax.fori_loop(0, tiles_of(est[e + 1] - est[e]), tile, t)

        @pl.when(e + 3 < NE)
        def _():
            w_copy(e + 3, ws).start()

        return t

    lax.fori_loop(0, NE, expert, jnp.int32(0))
    for back in (1, 2):
        @pl.when(nt >= back)
        def _(back=back):
            t = jnp.maximum(nt - back, 0)
            g_wait(lax.rem(t, 2), tnum[t])

    for s in range(NSB):
        def zero_wait(k, _, s=s):
            z_copy(s, k).wait()
            return 0

        lax.fori_loop(nsb_g[s], KC // G, zero_wait, 0)

    @pl.when(over)
    def _():
        rows16 = lax.broadcasted_iota(jnp.int32, (G, SB), 0)
        pbuf[...] = jnp.zeros_like(pbuf)
        for s in range(NSB):
            w = wt_ref[s]
            hi = w.astype(BF16).astype(F32)
            mid = (w - hi).astype(BF16).astype(F32)
            wsplit[0, s] = hi
            wsplit[1, s] = mid
            wsplit[2, s] = w - hi - mid

        def segment(q, _):
            s, e = q // NE, q % NE
            rk = jnp.broadcast_to(rank_ref[s, pl.ds(e, 1), :], (G, SB))
            parts = [jnp.broadcast_to(wsplit[i, s, pl.ds(e, 1), :], (G, SB)) for i in range(3)]

            def build(g, _):
                k = boff[q] + g

                @pl.when(k >= KC // G)
                def _():
                    row = pl.multiple_of((k - KC // G) * G, G)
                    hit = rk == rows16 + g * G
                    for i in range(3):
                        pbuf[s, i, pl.ds(row, G), :] = jnp.where(hit, parts[i], 0.0).astype(BF16)

                return 0

            return lax.fori_loop(0, ng[q], build, 0)

        lax.fori_loop(0, NSB * NE, segment, 0)
        core = core_ref[0]
        keep = pl.multiple_of(core * 256, 256)
        give = pl.multiple_of(256 - core * 256, 256)

        def piece(q, _):
            s, c = q // (D // CW), q % (D // CW)
            rel = core_ref[1 + s]
            get = pltpu.make_async_copy(eover.at[s, :, pl.ds(pl.multiple_of(c * CW, CW), CW)], kbuf, ksem.at[0])
            get.start()
            get.wait()

            def clear(k, _):
                kbuf[pl.ds(pl.multiple_of(k * G, G), G), :] = jnp.zeros((G, CW), BF16)
                return 0

            lax.fori_loop(jnp.maximum(nsb_g[s] - KC // G, 0), KX // G, clear, 0)
            abuf[...] = jnp.zeros_like(abuf)

            def part(kt, _):
                rows = pl.ds(pl.multiple_of(kt * TM, TM), TM)
                for i in range(3):
                    abuf[...] += lax.dot_general(pbuf[s, i, rows, :], kbuf[rows, :], (((0,), (0,)), ((), ())), preferred_element_type=F32)
                return 0

            lax.fori_loop(0, KX // TM, part, 0)
            copies = []
            for i in range(CW // RC):
                cols = pl.ds(i * RC, RC)
                j = c * (CW // RC) + i
                copies.append(pltpu.make_async_copy(abuf.at[pl.ds(give, 256), cols], theirs.at[j, rel], osem.at[i, 0]))
                copies.append(pltpu.make_async_copy(abuf.at[pl.ds(keep, 256), cols], mine.at[j, rel], osem.at[i, 1]))
            for cp in copies:
                cp.start()
            for cp in copies:
                cp.wait()
            return 0

        lax.fori_loop(0, NSB * (D // CW), piece, 0)


def down_call(cnt, core, rank, wts, h, w2):
    any_spec = pl.BlockSpec(memory_space=pl.ANY)
    smem = pl.BlockSpec(memory_space=pltpu.SMEM)
    vmem = pl.BlockSpec(memory_space=pltpu.VMEM)
    out = jax.ShapeDtypeStruct((NC, NSB, 256, RC), F32)
    return pl.pallas_call(
        down_kernel,
        out_shape=(jax.ShapeDtypeStruct((NSB, KC, D), BF16), jax.ShapeDtypeStruct((NSB, KX, D), BF16), out, out),
        in_specs=[smem, smem, vmem, vmem, any_spec, any_spec],
        out_specs=(any_spec, any_spec, any_spec, any_spec),
        scratch_shapes=[
            pltpu.VMEM((2, LM, FF), BF16),
            pltpu.VMEM((3, FF, D), BF16),
            pltpu.VMEM((2, LM, D), BF16),
            pltpu.VMEM((G, D), BF16),
            pltpu.VMEM((KX, CW), BF16),
            pltpu.VMEM((NSB, 3, KX, SB), BF16),
            pltpu.VMEM((SB, CW), F32),
            pltpu.VMEM((3, NSB, NE, SB), F32),
            pltpu.SMEM((NSB * NE,), jnp.int32),
            pltpu.SMEM((NSB * NE,), jnp.int32),
            pltpu.SMEM((NE + 1,), jnp.int32),
            pltpu.SMEM((NSB * NE,), jnp.int32),
            pltpu.SMEM((NSB,), jnp.int32),
            pltpu.SMEM((XG,), jnp.int32),
            pltpu.SMEM((64,), jnp.int32),
            pltpu.SMEM((64,), jnp.int32),
            pltpu.SemaphoreType.DMA((2,)),
            pltpu.SemaphoreType.DMA((3,)),
            pltpu.SemaphoreType.DMA((2,)),
            pltpu.SemaphoreType.DMA((1,)),
            pltpu.SemaphoreType.DMA((CW // RC, 2)),
            pltpu.SemaphoreType.DMA((1,)),
        ],
        compiler_params=pltpu.CompilerParams(vmem_limit_bytes=VMEM_LIMIT),
        cost_estimate=pl.CostEstimate(flops=40_000_000_000, bytes_accessed=100_000_000, transcendentals=0),
        name="down",
    )(cnt, core, rank, wts, h, w2)


def neighbours():
    me = lax.axis_index('ep')
    core = me + 1 - 2 * (me % 2)
    x = me + 2 - 4 * ((me // 2) % 2)
    y = me + 4 - 8 * (me // 4)
    return me, core, x, y


def remote(src, dst, send, recv, dev):
    return pltpu.make_async_remote_copy(src_ref=src, dst_ref=dst, send_sem=send, recv_sem=recv, device_id={'ep': dev}, device_id_type=pl.DeviceIdType.MESH)


def enter(others):
    barrier = pltpu.get_barrier_semaphore()
    for dev in others:
        pl.semaphore_signal(barrier, inc=1, device_id={'ep': dev}, device_id_type=pl.DeviceIdType.MESH)
    pl.semaphore_wait(barrier, len(others))


def gather_kernel(b_any, b_ref, wts_ref, w1, w3, w2, ball, wall_out, rank_ref, cnt_ref, pt, s_ref, wall, ptbuf, cols_buf, w13buf, w2buf, acc, send, recv, wsend, wrecv, local, wsem, psem):
    me, pn, xn, yn = neighbours()
    diag = xn + yn - me
    half = T // 2

    def rows(dev, h):
        return pl.ds(pl.multiple_of(dev * T + h * half, half), half)

    def own(k, h, dev):
        return remote(b_any.at[pl.ds(h * half, half), :], ball.at[rows(me, h), :], send.at[k], recv.at[k], dev)

    def relay(k, owner, h, dev):
        return remote(ball.at[rows(owner, h), :], ball.at[rows(owner, h), :], send.at[k], recv.at[k], dev)

    def w_copies(st, slot):
        cols = pl.ds(pl.multiple_of(st * SF, SF), SF)
        return (pltpu.make_async_copy(w1.at[:, cols], w13buf.at[slot, 0], wsem.at[slot, 0]),
                pltpu.make_async_copy(w3.at[:, cols], w13buf.at[slot, 1], wsem.at[slot, 1]),
                pltpu.make_async_copy(w2.at[cols, :], w2buf.at[slot], wsem.at[slot, 2]))

    for st in range(3):
        for c in w_copies(st, st):
            c.start()
    others = [lax.rem(me + k, 8) for k in range(1, 8)]
    enter(others)
    first = [own(0, 0, xn), own(2, 1, yn), own(1, 1, xn), own(3, 0, yn), own(4, 0, pn), own(5, 1, pn)]
    for c in first:
        c.start()
    lanes = pl.ds(pl.multiple_of((me % 2) * T, T), T)
    small = []
    for k, dev in enumerate(others):
        small.append(remote(wts_ref.at[pl.ds(pl.multiple_of(dev * NE, NE), NE), :], wall.at[me // 2, :, lanes], wsend.at[k], wrecv.at[k], dev))
        small[-1].start()
    keep = [pltpu.make_async_copy(b_ref, ball.at[pl.ds(pl.multiple_of(me * T, T), T), :], local.at[0]),
            pltpu.make_async_copy(wts_ref.at[pl.ds(pl.multiple_of(me * NE, NE), NE), :], wall.at[me // 2, :, lanes], local.at[1])]
    for c in keep:
        c.start()
    acc[...] = jnp.zeros_like(acc)

    def step(st, _):
        slot = lax.rem(st, 3)
        for c in w_copies(st, slot):
            c.wait()
        x = b_ref[...]
        gate = jnp.dot(x, w13buf[slot, 0], preferred_element_type=F32)
        lin = jnp.dot(x, w13buf[slot, 1], preferred_element_type=F32)
        inner = (jax.nn.silu(gate) * lin).astype(BF16)
        for n in range(D // 512):
            cols = slice(n * 512, n * 512 + 512)
            acc[:, cols] += jnp.dot(inner, w2buf[slot, :, cols], preferred_element_type=F32)

        return 0

    def refill(st, _):
        step(st, 0)
        for c in w_copies(st + 3, lax.rem(st, 3)):
            c.start()
        return 0

    lax.fori_loop(0, 8, refill, 0)
    first[0].wait_recv()
    first[1].wait_recv()
    second = [relay(6, xn, 0, yn), relay(7, yn, 1, xn), relay(8, xn, 0, pn), relay(9, yn, 1, pn)]
    for c in second:
        c.start()
    lax.fori_loop(8, SHARED // SF - 3, refill, 0)
    lax.fori_loop(SHARED // SF - 3, SHARED // SF, step, 0)
    s_ref[...] = acc[...].astype(BF16)
    first[2].wait_recv()
    first[3].wait_recv()
    third = [relay(10, xn, 1, pn), relay(11, yn, 0, pn)]
    for c in third:
        c.start()
    for c in small:
        c.wait_recv()
    keep[1].wait()
    before = jnp.where(lax.broadcasted_iota(jnp.int32, (SB, SB), 0) < lax.broadcasted_iota(jnp.int32, (SB, SB), 1), 1.0, 0.0).astype(BF16)
    row = lax.broadcasted_iota(jnp.int32, (1, KC), 1)
    puts = []
    for s in range(NSB):
        slot = s % 2
        w = wall[s]
        wall_out[s] = w
        sel = jnp.where(w >= 0.0, 1.0, 0.0)
        rank = jnp.where(w >= 0.0, jnp.dot(sel.astype(BF16), before, preferred_element_type=F32), -1.0)
        rank_ref[s] = rank.astype(jnp.int32)
        count = jnp.sum(sel, axis=1, keepdims=True).astype(jnp.int32)
        cnt_ref[s] = jnp.broadcast_to(count, (NE, 128))
        wide = jnp.broadcast_to(count, (NE, KC))
        start = jnp.zeros((1, KC), jnp.int32)
        local_row = []
        for e in range(NE):
            n = wide[e:e + 1]
            at = row - start
            local_row.append(jnp.where((at >= 0) & (at < n), at, -2).astype(F32))
            start = start + (n + (G - 1)) // G * G
        pad = jnp.zeros((128 - NE, SB), F32)
        cols_buf[0] = jnp.concatenate([rank, pad], axis=0).T
        cols_buf[1] = jnp.concatenate([w, pad], axis=0).T
        if s >= 2:
            puts[s - 2].wait()

        def fill(tb, _, slot=slot, local_row=local_row):
            toks = pl.ds(pl.multiple_of(tb * 32, 32), 32)
            rk = cols_buf[0, toks, :]
            wt = cols_buf[1, toks, :]
            total = jnp.zeros((32, KC), F32)
            for e in range(NE):
                total = jnp.where(rk[:, e:e + 1] == local_row[e], wt[:, e:e + 1], total)
            hi = total.astype(BF16)
            rest = total - hi.astype(F32)
            mid = rest.astype(BF16)
            ptbuf[slot, 0, toks, :] = hi
            ptbuf[slot, 1, toks, :] = mid
            ptbuf[slot, 2, toks, :] = (rest - mid.astype(F32)).astype(BF16)
            return 0

        lax.fori_loop(0, SB // 32, fill, 0)
        puts.append(pltpu.make_async_copy(ptbuf.at[slot], pt.at[s], psem.at[slot]))
        puts[s].start()
    second[0].wait_recv()
    second[1].wait_recv()
    fourth = [relay(12, diag, 0, pn), relay(13, diag, 1, pn)]
    for c in fourth:
        c.start()
    for c in (first[4], first[5], second[2], second[3], *third, *fourth):
        c.wait_recv()
    for c in (*first, *second, *third, *fourth):
        c.wait_send()
    for c in small:
        c.wait_send()
    keep[0].wait()
    puts[2].wait()
    puts[3].wait()


def gather_call(b, wts, w1, w3, w2):
    any_spec = pl.BlockSpec(memory_space=pl.ANY)
    vmem = pl.BlockSpec(memory_space=pltpu.VMEM)
    return pl.pallas_call(
        gather_kernel,
        out_shape=(
            jax.ShapeDtypeStruct((8 * T, D), BF16),
            jax.ShapeDtypeStruct((NSB, NE, SB), F32),
            jax.ShapeDtypeStruct((NSB, NE, SB), jnp.int32),
            jax.ShapeDtypeStruct((NSB, NE, 128), jnp.int32),
            jax.ShapeDtypeStruct((NSB, 3, SB, KC), BF16),
            jax.ShapeDtypeStruct((T, D), BF16),
        ),
        in_specs=[any_spec, vmem, vmem, any_spec, any_spec, any_spec],
        out_specs=(any_spec, vmem, vmem, vmem, any_spec, vmem),
        scratch_shapes=[
            pltpu.VMEM((NSB, NE, SB), F32),
            pltpu.VMEM((2, 3, SB, KC), BF16),
            pltpu.VMEM((2, SB, 128), F32),
            pltpu.VMEM((3, 2, D, SF), BF16),
            pltpu.VMEM((3, SF, D), BF16),
            pltpu.VMEM((T, D), F32),
            pltpu.SemaphoreType.DMA((14,)),
            pltpu.SemaphoreType.DMA((14,)),
            pltpu.SemaphoreType.DMA((7,)),
            pltpu.SemaphoreType.DMA((7,)),
            pltpu.SemaphoreType.DMA((2,)),
            pltpu.SemaphoreType.DMA((3, 3)),
            pltpu.SemaphoreType.DMA((2,)),
        ],
        compiler_params=pltpu.CompilerParams(collective_id=0, has_side_effects=True, vmem_limit_bytes=VMEM_LIMIT),
        cost_estimate=pl.CostEstimate(flops=12_000_000_000, bytes_accessed=60_000_000, transcendentals=0),
        name="gather",
    )(b, b, wts, w1, w3, w2)


def return_kernel(cnt_ref, pt, eblk, mine, theirs, y_ref, s_ref, out_ref, ptv, ev, own, give, r1, r2x, r2y, r3x, r3y, send, recv, load, esem, psem):
    me, pn, xn, yn = neighbours()
    half = T // 2
    top, low = pl.ds(0, half), pl.ds(half, half)

    def load_of(j):
        return (pltpu.make_async_copy(theirs.at[j], give.at[j], load.at[0, j]), pltpu.make_async_copy(mine.at[j], own.at[j], load.at[1, j]))

    def e_of(j, slot):
        return pltpu.make_async_copy(eblk.at[:, :, pl.ds(pl.multiple_of(j * RC, RC), RC)], ev.at[slot], esem.at[slot])

    def core_of(j):
        return remote(give.at[j], r1.at[j], send.at[0, j], recv.at[0, j], pn)

    def x_of(j):
        return remote(own.at[j, pl.ds(1, 2), top, :], r2x.at[j], send.at[1, j], recv.at[1, j], xn)

    def y_of(j):
        return remote(own.at[j, pl.ds(2, 2), low, :], r2y.at[j], send.at[2, j], recv.at[2, j], yn)

    def y_last(j):
        return remote(own.at[j, 3, top, :], r3y.at[j], send.at[3, j], recv.at[3, j], yn)

    def x_last(j):
        return remote(own.at[j, 1, low, :], r3x.at[j], send.at[4, j], recv.at[4, j], xn)

    def each(body):
        def run(j, _):
            body(j)
            return 0

        lax.fori_loop(0, NC, run, 0)

    rows_over = jnp.int32(0)
    for s in range(NSB):
        n = jnp.int32(0)
        for e in range(NE):
            n = n + (cnt_ref[s, e] + (G - 1)) // G
        rows_over = jnp.maximum(rows_over, n - KC // G)
    over = jnp.full((T, RC), rows_over, jnp.int32) > 0

    def begin(j):
        for c in load_of(j):
            c.start()

    def add_up(j, buf, first_tok):
        slot = lax.rem(j, 2)
        toks = pl.ds(pl.multiple_of(first_tok, T), T)

        def block(s, _):
            dx = lax.rem(lax.rem(s, 2) + lax.rem(me // 2, 2), 2)
            dy = lax.rem(s // 2 + me // 4, 2)
            place = dx + 3 * dy - 2 * dx * dy
            total = jnp.where(over, buf[j, place], 0.0)
            ek = ev[slot, s]
            for i in range(3):
                total = total + jnp.dot(ptv[s, i, toks, :], ek, preferred_element_type=F32)
            buf[j, place] = total
            return 0

        lax.fori_loop(0, NSB, block, 0)

    def make(j):
        e_of(j, lax.rem(j, 2)).wait()
        for c in load_of(j):
            c.wait()
        add_up(j, give, T - lax.rem(me, 2) * T)
        core_of(j).start()
        add_up(j, own, lax.rem(me, 2) * T)

    def pair(j):
        core_of(j).wait_recv()
        own[j, 1:] = own[j, 1:] + r1[j, 1:]
        x_of(j).start()
        y_of(j).start()
        own[j, 0] = own[j, 0] + r1[j, 0]

    def onward(j):
        x_of(j).wait_recv()
        own[j, 3, :half] = own[j, 3, :half] + r2x[j, 1]
        y_last(j).start()
        y_of(j).wait_recv()
        own[j, 1, half:] = own[j, 1, half:] + r2y[j, 0]
        x_last(j).start()

    def finish(j):
        cols = pl.ds(pl.multiple_of(j * RC, RC), RC)
        y_last(j).wait_recv()
        x_last(j).wait_recv()
        base = y_ref[:, cols].astype(F32) + s_ref[:, cols].astype(F32)
        out_ref[:half, cols] = (base[:half] + (own[j, 0, :half] + r2x[j, 0] + r3y[j])).astype(BF16)
        out_ref[half:, cols] = (base[half:] + (own[j, 0, half:] + r2y[j, 1] + r3x[j])).astype(BF16)

    def drain(j):
        for c in (core_of(j), x_of(j), y_of(j), y_last(j), x_last(j)):
            c.wait_send()

    e_of(0, 0).start()
    pt_copies = [pltpu.make_async_copy(pt.at[s], ptv.at[s], psem.at[s]) for s in range(NSB)]
    for c in pt_copies:
        c.start()
    e_of(1, 1).start()
    begin(0)
    begin(1)
    enter([pn, xn, yn])
    for c in pt_copies:
        c.wait()

    def steady(j, _):
        make(j)

        @pl.when(j + 2 < NC)
        def _():
            e_of(j + 2, lax.rem(j, 2)).start()
            begin(j + 2)

        pair(j)

        @pl.when(j >= LAG)
        def _():
            onward(j - LAG)

        return 0

    lax.fori_loop(0, NC, steady, 0)

    def last(j, _):
        onward(j)
        return 0

    lax.fori_loop(NC - LAG, NC, last, 0)
    each(finish)
    each(drain)


def return_call(cnt, pt, eblk, mine, theirs, hidden, shared_out):
    any_spec = pl.BlockSpec(memory_space=pl.ANY)
    vmem = pl.BlockSpec(memory_space=pltpu.VMEM)
    half = T // 2
    return pl.pallas_call(
        return_kernel,
        out_shape=jax.ShapeDtypeStruct((T, D), BF16),
        in_specs=[pl.BlockSpec(memory_space=pltpu.SMEM), any_spec, any_spec, any_spec, any_spec, vmem, vmem],
        out_specs=vmem,
        scratch_shapes=[
            pltpu.VMEM((NSB, 3, SB, KC), BF16),
            pltpu.VMEM((2, NSB, KC, RC), BF16),
            pltpu.VMEM((NC, NSB, T, RC), F32),
            pltpu.VMEM((NC, NSB, T, RC), F32),
            pltpu.VMEM((NC, NSB, T, RC), F32),
            pltpu.VMEM((NC, 2, half, RC), F32),
            pltpu.VMEM((NC, 2, half, RC), F32),
            pltpu.VMEM((NC, half, RC), F32),
            pltpu.VMEM((NC, half, RC), F32),
            pltpu.SemaphoreType.DMA((5, NC)),
            pltpu.SemaphoreType.DMA((5, NC)),
            pltpu.SemaphoreType.DMA((2, NC)),
            pltpu.SemaphoreType.DMA((2,)),
            pltpu.SemaphoreType.DMA((NSB,)),
        ],
        compiler_params=pltpu.CompilerParams(collective_id=1, has_side_effects=True, vmem_limit_bytes=VMEM_LIMIT),
        name="return_sum",
    )(cnt, pt, eblk, mine, theirs, hidden, shared_out)


def solution(mesh):
    tok_spec = P(('dp', 'ep'), None)
    expert_spec = P('ep', None, None)

    def local_fn(hidden, norm_gain, w_gate, w1_shared, w3_shared, w2_shared, w1_experts, w3_experts, w2_experts, topk_ids):
        normed = rms_norm(hidden, norm_gain)
        probs = jax.nn.softmax(jnp.dot(normed, w_gate, preferred_element_type=F32), axis=-1)
        chosen = jnp.any(topk_ids[:, :, None] == jnp.arange(EXPERTS), axis=1)
        gate_wts = jnp.where(chosen, ROUTE_SCALE * probs, -1.0).T
        ball, wsb, rank, counts, pt, shared_out = gather_call(normed, gate_wts, w1_shared, w3_shared, w2_shared)
        cnt = counts[:, :, 0]
        me = lax.axis_index('ep')
        chip, at = me // 2, jnp.arange(NSB)
        other_x, other_y = at % 2 != chip % 2, at // 2 != chip // 2
        place = jnp.where(other_x, jnp.where(other_y, 2, 1), jnp.where(other_y, 3, 0))
        core = jnp.concatenate([(me % 2)[None], place]).astype(jnp.int32)
        h = up_call(cnt, rank, ball, w1_experts, w3_experts)
        eblk, _, mine, theirs = down_call(cnt, core, rank, wsb, h, w2_experts)
        return return_call(cnt, pt, eblk, mine, theirs, hidden, shared_out)

    return jax.shard_map(local_fn, mesh=mesh, in_specs=(tok_spec, P(), P(), P(), P(), P(), expert_spec, expert_spec, expert_spec, tok_spec), out_specs=tok_spec, check_vma=False)
```

```python
import functools

import jax
import jax.numpy as jnp
from jax import lax
from jax.experimental import pallas as pl
from jax.experimental.pallas import tpu as pltpu
from jax.sharding import PartitionSpec as P

ROUTE_SCALE = 16
NORM_EPS = 1e-6
D = 2560
FF = 1536
EXPERTS = 64
NE = 8
NSB = 4
SB = 512
G = 16
TM = 256
LM = 384
SIZES = tuple(range(64, LM + 1, 64))
XG = 440
XR = XG * G
SBR = 1792
FC = 512
NF = FF // FC
DH = D // 2
T = 256
SHARED = 3072
SF = 256
CW = 512
RC = 256
NC = D // RC
KC = 768
HR = 1280
NK = KC // G
NOROW = NE * LM // G
WS = 4
LAG = 2
VMEM_LIMIT = 66000000
BF16 = jnp.bfloat16
F32 = jnp.float32


def rms_norm(hidden, norm_gain):
    rows_f = hidden.astype(F32)
    inv_rms = lax.rsqrt(jnp.mean(rows_f * rows_f, axis=-1, keepdims=True) + NORM_EPS)
    return (rows_f * inv_rms * norm_gain.astype(F32)).astype(BF16)


def offsets(cnt_ref, ng, eoff, est, boff, nsb_g):
    run = jnp.int32(0)
    for e in range(NE):
        est[e] = run
        for s in range(NSB):
            n = (cnt_ref[s, e] + (G - 1)) // G
            ng[s * NE + e] = n
            eoff[s * NE + e] = run
            run = run + n
    est[NE] = run
    for s in range(NSB):
        b = jnp.int32(0)
        for e in range(NE):
            boff[s * NE + e] = b
            b = b + ng[s * NE + e]
        nsb_g[s] = b


def up_kernel(cnt_ref, rank_ref, ball, w1, w3, h_out, table, xs, bbuf, pbuf, tbuf, wbuf, hbuf, ng, eoff, est, boff, nsb_g, dst, last, bsem, wsem, hsem):
    def w_copies(step, slot):
        e = step // NF
        f = step % NF
        cols = pl.ds(pl.multiple_of(f * FC, FC), FC)
        return (pltpu.make_async_copy(w1.at[e, :, cols], wbuf.at[slot, 0], wsem.at[slot, 0]),
                pltpu.make_async_copy(w3.at[e, :, cols], wbuf.at[slot, 1], wsem.at[slot, 1]))

    def b_copy(s, half):
        return pltpu.make_async_copy(ball.at[pl.ds(s * SB, SB), pl.ds(half * DH, DH)], bbuf.at[half], bsem.at[half])

    b_copy(0, 0).start()
    b_copy(0, 1).start()
    for st in range(3):
        for c in w_copies(st, st):
            c.start()
    offsets(cnt_ref, ng, eoff, est, boff, nsb_g)
    rows16 = lax.broadcasted_iota(jnp.int32, (G, SB), 0)

    for s in range(NSB):
        for e in range(NE):
            rk = jnp.broadcast_to(rank_ref[s, e:e + 1, :], (G, SB))

            def build(g, _, s=s, e=e, rk=rk):
                k = boff[s * NE + e] + g
                dst[k] = eoff[s * NE + e] + g
                hit = jnp.where(rk == rows16 + g * G, 1.0, 0.0)
                pbuf[pl.ds(pl.multiple_of(k * G, G), G), :] = hit.astype(BF16)
                return 0

            lax.fori_loop(0, ng[s * NE + e], build, 0)
        for half in range(2):
            b_copy(s, half).wait()

            def tile(m, _, s=s, half=half):
                prow = pbuf[pl.ds(pl.multiple_of(m * TM, TM), TM), :]
                for n in range(5):
                    cols = slice(n * 256, (n + 1) * 256)
                    tbuf[:, cols] = jnp.dot(prow, bbuf[half, :, cols], preferred_element_type=F32).astype(BF16)

                def put(j, _):
                    row = pl.multiple_of(dst[m * (TM // G) + j] * G, G)
                    xs[pl.ds(row, G), half * DH:(half + 1) * DH] = tbuf[pl.ds(pl.multiple_of(j * G, G), G), :]
                    return 0

                lax.fori_loop(0, jnp.minimum(TM // G, nsb_g[s] - m * (TM // G)), put, 0)
                return 0

            lax.fori_loop(0, (nsb_g[s] + TM // G - 1) // (TM // G), tile, 0)
            if s + 1 < NSB:
                b_copy(s + 1, half).start()

    def fill(k, _):
        table[k] = NOROW
        return 0

    lax.fori_loop(0, NSB * NK, fill, 0)
    over = jnp.int32(0)
    for e in range(NE):
        over = jnp.maximum(over, est[e + 1] - est[e] - LM // G)
    for s in range(NSB):
        over = jnp.maximum(over, nsb_g[s] - NK)
    table[NSB * NK] = over

    def segment(q, _):
        s, e = q // NE, q % NE
        first = eoff[q] - est[e]

        def one(g, _):
            k = boff[q] + g

            @pl.when((k < NK) & (first + g < LM // G))
            def _():
                table[s * NK + k] = e * (LM // G) + first + g

            return 0

        return lax.fori_loop(0, ng[q], one, 0)

    lax.fori_loop(0, NSB * NE, segment, 0)

    def h_copy(hs, e, row, col, size):
        return pltpu.make_async_copy(hbuf.at[hs, pl.ds(0, size), :], h_out.at[e, pl.ds(row, size), pl.ds(col, FC)], hsem.at[0])

    def wait_h(quarters):
        for q in range(1, LM // 64 + 1):
            @pl.when(quarters == q)
            def _(q=q):
                h_copy(0, 0, 0, 0, q * 64).wait()

    def step(st, k):
        slot = lax.rem(st, 3)
        e = st // NF
        col = pl.multiple_of((st % NF) * FC, FC)
        for c in w_copies(st, slot):
            c.wait()
        base = est[e] * G
        rows = est[e + 1] * G - base

        def work(row, size, k):
            row = pl.multiple_of(row, G)
            hs = k % 2
            for n in range(FC // 256):
                cols = slice(n * 256, (n + 1) * 256)
                x = xs[pl.ds(row, size), :]
                gate = jnp.dot(x, wbuf[slot, 0, :, cols], preferred_element_type=F32)
                lin = jnp.dot(x, wbuf[slot, 1, :, cols], preferred_element_type=F32)
                hbuf[hs, pl.ds(0, size), cols] = (jax.nn.silu(gate) * lin).astype(BF16)

            @pl.when(k > 0)
            def _():
                wait_h(last[0])

            last[0] = size // 64
            h_copy(hs, e, pl.multiple_of(row - base, G), col, size).start()

        full = jnp.maximum(rows - LM + TM - 1, 0) // TM

        def body(m, k):
            work(base + m * TM, TM, k)
            return k + 1

        k = lax.fori_loop(0, full, body, k)
        rem = rows - full * TM
        at = base + full * TM
        for size in SIZES:
            @pl.when((rem > size - 64) & (rem <= size))
            def _(size=size):
                work(at, size, k)

        @pl.when(st + 3 < NE * NF)
        def _():
            for c in w_copies(st + 3, slot):
                c.start()

        return k + jnp.where(rem > 0, 1, 0)

    @pl.when(lax.fori_loop(0, NE * NF, step, jnp.int32(0)) > 0)
    def _():
        wait_h(last[0])


def up_call(cnt, rank, ball, w1, w3):
    any_spec = pl.BlockSpec(memory_space=pl.ANY)
    return pl.pallas_call(
        up_kernel,
        out_shape=(jax.ShapeDtypeStruct((NE, HR, FF), BF16), jax.ShapeDtypeStruct((256,), jnp.int32)),
        in_specs=[pl.BlockSpec(memory_space=pltpu.SMEM), pl.BlockSpec(memory_space=pltpu.VMEM), any_spec, any_spec, any_spec],
        out_specs=(any_spec, pl.BlockSpec(memory_space=pltpu.SMEM)),
        scratch_shapes=[
            pltpu.VMEM((XR, D), BF16),
            pltpu.VMEM((2, SB, DH), BF16),
            pltpu.VMEM((SBR, SB), BF16),
            pltpu.VMEM((TM, DH), BF16),
            pltpu.VMEM((3, 2, D, FC), BF16),
            pltpu.VMEM((2, LM, FC), BF16),
            pltpu.SMEM((NSB * NE,), jnp.int32),
            pltpu.SMEM((NSB * NE,), jnp.int32),
            pltpu.SMEM((NE + 1,), jnp.int32),
            pltpu.SMEM((NSB * NE,), jnp.int32),
            pltpu.SMEM((NSB,), jnp.int32),
            pltpu.SMEM((SBR // G,), jnp.int32),
            pltpu.SMEM((1,), jnp.int32),
            pltpu.SemaphoreType.DMA((2,)),
            pltpu.SemaphoreType.DMA((3, 2)),
            pltpu.SemaphoreType.DMA((1,)),
        ],
        compiler_params=pltpu.CompilerParams(vmem_limit_bytes=VMEM_LIMIT),
        cost_estimate=pl.CostEstimate(flops=48_000_000_000, bytes_accessed=140_000_000, transcendentals=0),
        name="up",
    )(cnt, rank, ball, w1, w3)


def down_kernel(table, cnt_ref, core_ref, rank_ref, wt_ref, h, w2, mine, theirs, *scratch):
    @pl.when(table[NSB * NK] > 0)
    def _():
        down_all(cnt_ref, core_ref, rank_ref, wt_ref, h, w2, mine, theirs, *scratch)


def down_all(cnt_ref, core_ref, rank_ref, wt_ref, h, w2, mine, theirs,
                hs, ebuf, kbuf, pbuf, wbuf, abuf, wsplit, ng, eoff, est, boff, nsb_g, hsem, wsem, osem):
    steps = (D // CW) * NE

    def w_copy(st, slot):
        col = pl.multiple_of((st // NE) * CW, CW)
        return pltpu.make_async_copy(w2.at[st % NE, :, pl.ds(col, CW)], wbuf.at[slot], wsem.at[slot])

    for st in range(3):
        w_copy(st, st).start()
    offsets(cnt_ref, ng, eoff, est, boff, nsb_g)
    for e in range(NE):
        def fetch(m, _, e=e):
            to = pl.ds(pl.multiple_of(est[e] * G + m * TM, G), TM)
            copy = pltpu.make_async_copy(h.at[e, pl.ds(pl.multiple_of(m * TM, TM), TM), :], hs.at[to, :], hsem.at[0])
            copy.start()
            copy.wait()
            return 0

        lax.fori_loop(0, (est[e + 1] - est[e] + TM // G - 1) // (TM // G), fetch, 0)
    for s in range(NSB):
        w = wt_ref[s]
        hi = w.astype(BF16).astype(F32)
        mid = (w - hi).astype(BF16).astype(F32)
        wsplit[0, s] = hi
        wsplit[1, s] = mid
        wsplit[2, s] = w - hi - mid
    rows16 = lax.broadcasted_iota(jnp.int32, (G, SB), 0)
    for s in range(NSB):
        for e in range(NE):
            rk = jnp.broadcast_to(rank_ref[s, e:e + 1, :], (G, SB))
            parts = [jnp.broadcast_to(wsplit[i, s, e:e + 1, :], (G, SB)) for i in range(3)]

            def build(g, _, s=s, e=e, rk=rk, parts=parts):
                row = pl.multiple_of((boff[s * NE + e] + g) * G, G)
                hit = rk == rows16 + g * G
                for i in range(3):
                    pbuf[s, i, pl.ds(row, G), :] = jnp.where(hit, parts[i], 0.0).astype(BF16)
                return 0

            lax.fori_loop(0, ng[s * NE + e], build, 0)

        def clear(g, _, s=s):
            row = pl.multiple_of(g * G, G)
            for i in range(3):
                pbuf[s, i, pl.ds(row, G), :] = jnp.zeros((G, SB), BF16)
            return 0

        lax.fori_loop(nsb_g[s], -(-nsb_g[s] // (TM // G)) * (TM // G), clear, 0)
    kbuf[...] = jnp.zeros_like(kbuf)

    core = core_ref[0]

    def out_copies(c, s, slot):
        rel = core_ref[1 + s]
        keep = pl.multiple_of(core * 256, 256)
        give = pl.multiple_of(256 - core * 256, 256)
        out = []
        for i in range(CW // RC):
            cols = pl.ds(i * RC, RC)
            j = c * (CW // RC) + i
            out.append(pltpu.make_async_copy(abuf.at[slot, pl.ds(give, 256), cols], theirs.at[j, rel], osem.at[slot, i, 0]))
            out.append(pltpu.make_async_copy(abuf.at[slot, pl.ds(keep, 256), cols], mine.at[j, rel], osem.at[slot, i, 1]))
        return out

    def column(c, _):
        def expert(e, _):
            st = c * NE + e
            ws = st % 3
            w_copy(st, ws).wait()
            base = est[e] * G
            rows = est[e + 1] * G - base

            def work(row, size):
                row = pl.multiple_of(row, G)
                ebuf[pl.ds(row, size), :] = jnp.dot(hs[pl.ds(row, size), :], wbuf[ws], preferred_element_type=F32).astype(BF16)

            full = rows // TM

            def body(m, _):
                work(base + m * TM, TM)
                return 0

            lax.fori_loop(0, full, body, 0)
            rem = rows - full * TM
            for size in (128, 256):
                @pl.when((rem > size - 128) & (rem <= size))
                def _(size=size):
                    work(base + full * TM, size)

            @pl.when(st + 3 < steps)
            def _():
                w_copy(st + 3, ws).start()

            return 0

        lax.fori_loop(0, NE, expert, 0)

        def block(s, _):
            slot = s % 2

            def segment(e, _):
                def move(g, _):
                    row = pl.multiple_of((boff[s * NE + e] + g) * G, G)
                    src = pl.multiple_of((eoff[s * NE + e] + g) * G, G)
                    kbuf[pl.ds(row, G), :] = ebuf[pl.ds(src, G), :]
                    return 0

                return lax.fori_loop(0, ng[s * NE + e], move, 0)

            lax.fori_loop(0, NE, segment, 0)
            nk = (nsb_g[s] + TM // G - 1) // (TM // G)

            @pl.when(c * NSB + s >= 2)
            def _():
                for cp in out_copies(c, s, slot):
                    cp.wait()

            abuf[slot] = jnp.zeros((SB, CW), F32)

            def tile(kt, _):
                rows = pl.ds(pl.multiple_of(kt * TM, TM), TM)
                ek = kbuf[rows, :]
                for half in range(2):
                    toks = slice(half * 256, half * 256 + 256)
                    tot = abuf[slot, toks, :]
                    for i in range(3):
                        tot = tot + lax.dot_general(pbuf[s, i, rows, toks], ek, (((0,), (0,)), ((), ())), preferred_element_type=F32)
                    abuf[slot, toks, :] = tot
                return 0

            lax.fori_loop(0, nk, tile, 0)
            for cp in out_copies(c, s, slot):
                cp.start()
            return 0

        return lax.fori_loop(0, NSB, block, 0)

    lax.fori_loop(0, D // CW, column, 0)
    for s in (NSB - 2, NSB - 1):
        for cp in out_copies(D // CW - 1, s, s % 2):
            cp.wait()


def down_call(table, cnt, core, rank, wts, h, w2):
    any_spec = pl.BlockSpec(memory_space=pl.ANY)
    smem = pl.BlockSpec(memory_space=pltpu.SMEM)
    vmem = pl.BlockSpec(memory_space=pltpu.VMEM)
    out = jax.ShapeDtypeStruct((NC, NSB, 256, RC), F32)
    return pl.pallas_call(
        down_kernel,
        out_shape=(out, out),
        in_specs=[smem, smem, smem, vmem, vmem, any_spec, any_spec],
        out_specs=(any_spec, any_spec),
        scratch_shapes=[
            pltpu.VMEM((XR, FF), BF16),
            pltpu.VMEM((XR, CW), BF16),
            pltpu.VMEM((SBR, CW), BF16),
            pltpu.VMEM((NSB, 3, SBR, SB), BF16),
            pltpu.VMEM((3, FF, CW), BF16),
            pltpu.VMEM((2, SB, CW), F32),
            pltpu.VMEM((3, NSB, NE, SB), F32),
            pltpu.SMEM((NSB * NE,), jnp.int32),
            pltpu.SMEM((NSB * NE,), jnp.int32),
            pltpu.SMEM((NE + 1,), jnp.int32),
            pltpu.SMEM((NSB * NE,), jnp.int32),
            pltpu.SMEM((NSB,), jnp.int32),
            pltpu.SemaphoreType.DMA((1,)),
            pltpu.SemaphoreType.DMA((3,)),
            pltpu.SemaphoreType.DMA((2, CW // RC, 2)),
        ],
        compiler_params=pltpu.CompilerParams(vmem_limit_bytes=VMEM_LIMIT),
        cost_estimate=pl.CostEstimate(flops=40_000_000_000, bytes_accessed=100_000_000, transcendentals=0),
        name="down",
    )(table, cnt, core, rank, wts, h, w2)


def neighbours():
    me = lax.axis_index('ep')
    core = me + 1 - 2 * (me % 2)
    x = me + 2 - 4 * ((me // 2) % 2)
    y = me + 4 - 8 * (me // 4)
    return me, core, x, y


def remote(src, dst, send, recv, dev):
    return pltpu.make_async_remote_copy(src_ref=src, dst_ref=dst, send_sem=send, recv_sem=recv, device_id={'ep': dev}, device_id_type=pl.DeviceIdType.MESH)


def enter(others):
    barrier = pltpu.get_barrier_semaphore()
    for dev in others:
        pl.semaphore_signal(barrier, inc=1, device_id={'ep': dev}, device_id_type=pl.DeviceIdType.MESH)
    pl.semaphore_wait(barrier, len(others))


def gather_kernel(b_any, b_ref, wts_ref, w1, w3, w2, ball, wall_out, rank_ref, cnt_ref, pt, s_ref, wall, ptbuf, cols_buf, w13buf, w2buf, acc, send, recv, wsend, wrecv, local, wsem, psem):
    me, pn, xn, yn = neighbours()
    diag = xn + yn - me
    half = T // 2

    def rows(dev, h):
        return pl.ds(pl.multiple_of(dev * T + h * half, half), half)

    def own(k, h, dev):
        return remote(b_any.at[pl.ds(h * half, half), :], ball.at[rows(me, h), :], send.at[k], recv.at[k], dev)

    def relay(k, owner, h, dev):
        return remote(ball.at[rows(owner, h), :], ball.at[rows(owner, h), :], send.at[k], recv.at[k], dev)

    def w_copies(st, slot):
        cols = pl.ds(pl.multiple_of(st * SF, SF), SF)
        return (pltpu.make_async_copy(w1.at[:, cols], w13buf.at[slot, 0], wsem.at[slot, 0]),
                pltpu.make_async_copy(w3.at[:, cols], w13buf.at[slot, 1], wsem.at[slot, 1]),
                pltpu.make_async_copy(w2.at[cols, :], w2buf.at[slot], wsem.at[slot, 2]))

    for st in range(3):
        for c in w_copies(st, st):
            c.start()
    others = [lax.rem(me + k, 8) for k in range(1, 8)]
    enter(others)
    first = [own(0, 0, xn), own(2, 1, yn), own(1, 1, xn), own(3, 0, yn), own(4, 0, pn), own(5, 1, pn)]
    for c in first:
        c.start()
    lanes = pl.ds(pl.multiple_of((me % 2) * T, T), T)
    small = []
    for k, dev in enumerate(others):
        small.append(remote(wts_ref.at[pl.ds(pl.multiple_of(dev * NE, NE), NE), :], wall.at[me // 2, :, lanes], wsend.at[k], wrecv.at[k], dev))
        small[-1].start()
    keep = [pltpu.make_async_copy(b_ref, ball.at[pl.ds(pl.multiple_of(me * T, T), T), :], local.at[0]),
            pltpu.make_async_copy(wts_ref.at[pl.ds(pl.multiple_of(me * NE, NE), NE), :], wall.at[me // 2, :, lanes], local.at[1])]
    for c in keep:
        c.start()
    acc[...] = jnp.zeros_like(acc)

    def step(st, _):
        slot = lax.rem(st, 3)
        for c in w_copies(st, slot):
            c.wait()
        x = b_ref[...]
        gate = jnp.dot(x, w13buf[slot, 0], preferred_element_type=F32)
        lin = jnp.dot(x, w13buf[slot, 1], preferred_element_type=F32)
        inner = (jax.nn.silu(gate) * lin).astype(BF16)
        for n in range(D // 512):
            cols = slice(n * 512, n * 512 + 512)
            acc[:, cols] += jnp.dot(inner, w2buf[slot, :, cols], preferred_element_type=F32)

        return 0

    def refill(st, _):
        step(st, 0)
        for c in w_copies(st + 3, lax.rem(st, 3)):
            c.start()
        return 0

    lax.fori_loop(0, 8, refill, 0)
    first[0].wait_recv()
    first[1].wait_recv()
    second = [relay(6, xn, 0, yn), relay(7, yn, 1, xn), relay(8, xn, 0, pn), relay(9, yn, 1, pn)]
    for c in second:
        c.start()
    lax.fori_loop(8, SHARED // SF - 3, refill, 0)
    lax.fori_loop(SHARED // SF - 3, SHARED // SF, step, 0)
    s_ref[...] = acc[...].astype(BF16)
    first[2].wait_recv()
    first[3].wait_recv()
    third = [relay(10, xn, 1, pn), relay(11, yn, 0, pn)]
    for c in third:
        c.start()
    for c in small:
        c.wait_recv()
    keep[1].wait()
    before = jnp.where(lax.broadcasted_iota(jnp.int32, (SB, SB), 0) < lax.broadcasted_iota(jnp.int32, (SB, SB), 1), 1.0, 0.0).astype(BF16)
    row = lax.broadcasted_iota(jnp.int32, (1, KC), 1)
    puts = []
    for s in range(NSB):
        slot = s % 2
        w = wall[s]
        wall_out[s] = w
        sel = jnp.where(w >= 0.0, 1.0, 0.0)
        rank = jnp.where(w >= 0.0, jnp.dot(sel.astype(BF16), before, preferred_element_type=F32), -1.0)
        rank_ref[s] = rank.astype(jnp.int32)
        count = jnp.sum(sel, axis=1, keepdims=True).astype(jnp.int32)
        cnt_ref[s] = jnp.broadcast_to(count, (NE, 128))
        wide = jnp.broadcast_to(count, (NE, KC))
        start = jnp.zeros((1, KC), jnp.int32)
        local_row = []
        for e in range(NE):
            n = wide[e:e + 1]
            at = row - start
            local_row.append(jnp.where((at >= 0) & (at < n), at, -2).astype(F32))
            start = start + (n + (G - 1)) // G * G
        pad = jnp.zeros((128 - NE, SB), F32)
        cols_buf[0] = jnp.concatenate([rank, pad], axis=0).T
        cols_buf[1] = jnp.concatenate([w, pad], axis=0).T
        if s >= 2:
            puts[s - 2].wait()

        def fill(tb, _, slot=slot, local_row=local_row):
            toks = pl.ds(pl.multiple_of(tb * 32, 32), 32)
            rk = cols_buf[0, toks, :]
            wt = cols_buf[1, toks, :]
            total = jnp.zeros((32, KC), F32)
            for e in range(NE):
                total = jnp.where(rk[:, e:e + 1] == local_row[e], wt[:, e:e + 1], total)
            hi = total.astype(BF16)
            rest = total - hi.astype(F32)
            mid = rest.astype(BF16)
            ptbuf[slot, 0, toks, :] = hi
            ptbuf[slot, 1, toks, :] = mid
            ptbuf[slot, 2, toks, :] = (rest - mid.astype(F32)).astype(BF16)
            return 0

        lax.fori_loop(0, SB // 32, fill, 0)
        puts.append(pltpu.make_async_copy(ptbuf.at[slot], pt.at[s], psem.at[slot]))
        puts[s].start()
    second[0].wait_recv()
    second[1].wait_recv()
    fourth = [relay(12, diag, 0, pn), relay(13, diag, 1, pn)]
    for c in fourth:
        c.start()
    for c in (first[4], first[5], second[2], second[3], *third, *fourth):
        c.wait_recv()
    for c in (*first, *second, *third, *fourth):
        c.wait_send()
    for c in small:
        c.wait_send()
    keep[0].wait()
    puts[2].wait()
    puts[3].wait()


def gather_call(b, wts, w1, w3, w2):
    any_spec = pl.BlockSpec(memory_space=pl.ANY)
    vmem = pl.BlockSpec(memory_space=pltpu.VMEM)
    return pl.pallas_call(
        gather_kernel,
        out_shape=(
            jax.ShapeDtypeStruct((8 * T, D), BF16),
            jax.ShapeDtypeStruct((NSB, NE, SB), F32),
            jax.ShapeDtypeStruct((NSB, NE, SB), jnp.int32),
            jax.ShapeDtypeStruct((NSB, NE, 128), jnp.int32),
            jax.ShapeDtypeStruct((NSB, 3, SB, KC), BF16),
            jax.ShapeDtypeStruct((T, D), BF16),
        ),
        in_specs=[any_spec, vmem, vmem, any_spec, any_spec, any_spec],
        out_specs=(any_spec, vmem, vmem, vmem, any_spec, vmem),
        scratch_shapes=[
            pltpu.VMEM((NSB, NE, SB), F32),
            pltpu.VMEM((2, 3, SB, KC), BF16),
            pltpu.VMEM((2, SB, 128), F32),
            pltpu.VMEM((3, 2, D, SF), BF16),
            pltpu.VMEM((3, SF, D), BF16),
            pltpu.VMEM((T, D), F32),
            pltpu.SemaphoreType.DMA((14,)),
            pltpu.SemaphoreType.DMA((14,)),
            pltpu.SemaphoreType.DMA((7,)),
            pltpu.SemaphoreType.DMA((7,)),
            pltpu.SemaphoreType.DMA((2,)),
            pltpu.SemaphoreType.DMA((3, 3)),
            pltpu.SemaphoreType.DMA((2,)),
        ],
        compiler_params=pltpu.CompilerParams(collective_id=0, has_side_effects=True, vmem_limit_bytes=VMEM_LIMIT),
        cost_estimate=pl.CostEstimate(flops=12_000_000_000, bytes_accessed=60_000_000, transcendentals=0),
        name="gather",
    )(b, b, wts, w1, w3, w2)


def return_kernel(table, pt, h, w2, mine, theirs, y_ref, s_ref, out_ref, ptv, hv, wbuf, ebuf, kbuf, own, give, r1, r2x, r2y, r3x, r3y, send, recv, load, wsem, hsem, psem):
    me, pn, xn, yn = neighbours()
    half = T // 2
    top, low = pl.ds(0, half), pl.ds(half, half)

    def load_of(j):
        return (pltpu.make_async_copy(theirs.at[j], give.at[lax.rem(j, 3)], load.at[0, j]), pltpu.make_async_copy(mine.at[j], own.at[j], load.at[1, j]))

    def w_of(st):
        cols = pl.ds(pl.multiple_of((st // NE) * RC, RC), RC)
        return pltpu.make_async_copy(w2.at[lax.rem(st, NE), :, cols], wbuf.at[lax.rem(st, WS)], wsem.at[lax.rem(st, WS)])

    def core_of(j):
        return remote(give.at[lax.rem(j, 3)], r1.at[j], send.at[0, j], recv.at[0, j], pn)

    def x_of(j):
        return remote(own.at[j, pl.ds(1, 2), top, :], r2x.at[j], send.at[1, j], recv.at[1, j], xn)

    def y_of(j):
        return remote(own.at[j, pl.ds(2, 2), low, :], r2y.at[j], send.at[2, j], recv.at[2, j], yn)

    def y_last(j):
        return remote(own.at[j, 3, top, :], r3y.at[j], send.at[3, j], recv.at[3, j], yn)

    def x_last(j):
        return remote(own.at[j, 1, low, :], r3x.at[j], send.at[4, j], recv.at[4, j], xn)

    def each(body):
        def run(j, _):
            body(j)
            return 0

        lax.fori_loop(0, NC, run, 0)

    over = jnp.full((T, RC), table[NSB * NK], jnp.int32) > 0

    def begin(j):
        for c in load_of(j):
            c.start()

    def add_up(buf, at, first_tok):
        toks = pl.ds(pl.multiple_of(first_tok, T), T)

        def block(s, _):
            dx = lax.rem(lax.rem(s, 2) + lax.rem(me // 2, 2), 2)
            dy = lax.rem(s // 2 + me // 4, 2)
            place = dx + 3 * dy - 2 * dx * dy
            ek = kbuf[pl.ds(pl.multiple_of(s * KC, KC), KC), :]
            total = jnp.dot(ptv[s, 0, toks, :], ek, preferred_element_type=F32)
            for i in range(1, 3):
                total = total + jnp.dot(ptv[s, i, toks, :], ek, preferred_element_type=F32)
            buf[at, place] = jnp.where(over, buf[at, place], total)
            return 0

        lax.fori_loop(0, NSB, block, 0)

    def make(j):
        def expert(e, _):
            st = j * NE + e

            @pl.when(j == 0)
            def _():
                h_of(e).wait()

            w_of(st).wait()
            res = jnp.dot(hv[e], wbuf[lax.rem(st, WS)], preferred_element_type=F32).astype(BF16)
            ebuf[pl.ds(e * (LM // G), LM // G)] = res.reshape(LM // G, G, RC)

            @pl.when(st + WS < NC * NE)
            def _():
                w_of(st + WS).start()

            return 0

        lax.fori_loop(0, NE, expert, 0)

        def move(k, _):
            for i in range(8):
                kbuf[pl.ds(pl.multiple_of((k * 8 + i) * G, G), G), :] = ebuf[table[k * 8 + i]]
            return 0

        lax.fori_loop(0, NSB * NK // 8, move, 0)

        @pl.when(j == 0)
        def _():
            for c in pt_copies:
                c.wait()

        for c in load_of(j):
            c.wait()
        add_up(give, lax.rem(j, 3), T - lax.rem(me, 2) * T)
        core_of(j).start()
        add_up(own, j, lax.rem(me, 2) * T)

    def pair(j):
        core_of(j).wait_recv()
        own[j, 1:] = own[j, 1:] + r1[j, 1:]
        x_of(j).start()
        y_of(j).start()
        own[j, 0] = own[j, 0] + r1[j, 0]

    def onward(j):
        x_of(j).wait_recv()
        own[j, 3, :half] = own[j, 3, :half] + r2x[j, 1]
        y_last(j).start()
        y_of(j).wait_recv()
        own[j, 1, half:] = own[j, 1, half:] + r2y[j, 0]
        x_last(j).start()

    def finish(j):
        cols = pl.ds(pl.multiple_of(j * RC, RC), RC)
        y_last(j).wait_recv()
        x_last(j).wait_recv()
        base = y_ref[:, cols].astype(F32) + s_ref[:, cols].astype(F32)
        out_ref[:half, cols] = (base[:half] + (own[j, 0, :half] + r2x[j, 0] + r3y[j])).astype(BF16)
        out_ref[half:, cols] = (base[half:] + (own[j, 0, half:] + r2y[j, 1] + r3x[j])).astype(BF16)

    def drain(j):
        for c in (x_of(j), y_of(j), y_last(j), x_last(j)):
            c.wait_send()

    def h_of(e):
        return pltpu.make_async_copy(h.at[e, pl.ds(0, LM), :], hv.at[e], hsem.at[e])

    pt_copies = [pltpu.make_async_copy(pt.at[s], ptv.at[s], psem.at[s]) for s in range(NSB)]
    for e in range(NE):
        h_of(e).start()
        if e < WS:
            w_of(e).start()
    begin(0)
    begin(1)
    for c in pt_copies:
        c.start()
    ebuf[NOROW] = jnp.zeros((G, RC), BF16)
    enter([pn, xn, yn])

    def steady(j, _):
        @pl.when(j >= 2)
        def _():
            core_of(j - 2).wait_send()

        @pl.when((j >= 1) & (j + 1 < NC))
        def _():
            begin(j + 1)

        make(j)
        pair(j)

        @pl.when(j >= LAG)
        def _():
            onward(j - LAG)

        return 0

    lax.fori_loop(0, NC, steady, 0)

    def last(j, _):
        core_of(j).wait_send()
        onward(j)
        return 0

    lax.fori_loop(NC - LAG, NC, last, 0)
    each(finish)
    each(drain)


def return_call(table, pt, h, w2, mine, theirs, hidden, shared_out):
    any_spec = pl.BlockSpec(memory_space=pl.ANY)
    vmem = pl.BlockSpec(memory_space=pltpu.VMEM)
    half = T // 2
    return pl.pallas_call(
        return_kernel,
        out_shape=jax.ShapeDtypeStruct((T, D), BF16),
        in_specs=[pl.BlockSpec(memory_space=pltpu.SMEM), any_spec, any_spec, any_spec, any_spec, any_spec, vmem, vmem],
        out_specs=vmem,
        scratch_shapes=[
            pltpu.VMEM((NSB, 3, SB, KC), BF16),
            pltpu.VMEM((NE, LM, FF), BF16),
            pltpu.VMEM((WS, FF, RC), BF16),
            pltpu.VMEM((NOROW + 1, G, RC), BF16),
            pltpu.VMEM((NSB * KC, RC), BF16),
            pltpu.VMEM((NC, NSB, T, RC), F32),
            pltpu.VMEM((3, NSB, T, RC), F32),
            pltpu.VMEM((NC, NSB, T, RC), F32),
            pltpu.VMEM((NC, 2, half, RC), F32),
            pltpu.VMEM((NC, 2, half, RC), F32),
            pltpu.VMEM((NC, half, RC), F32),
            pltpu.VMEM((NC, half, RC), F32),
            pltpu.SemaphoreType.DMA((5, NC)),
            pltpu.SemaphoreType.DMA((5, NC)),
            pltpu.SemaphoreType.DMA((2, NC)),
            pltpu.SemaphoreType.DMA((WS,)),
            pltpu.SemaphoreType.DMA((NE,)),
            pltpu.SemaphoreType.DMA((NSB,)),
        ],
        compiler_params=pltpu.CompilerParams(collective_id=1, has_side_effects=True, vmem_limit_bytes=VMEM_LIMIT),
        name="return_sum",
    )(table, pt, h, w2, mine, theirs, hidden, shared_out)


def solution(mesh):
    tok_spec = P(('dp', 'ep'), None)
    expert_spec = P('ep', None, None)

    def local_fn(hidden, norm_gain, w_gate, w1_shared, w3_shared, w2_shared, w1_experts, w3_experts, w2_experts, topk_ids):
        normed = rms_norm(hidden, norm_gain)
        probs = jax.nn.softmax(jnp.dot(normed, w_gate, preferred_element_type=F32), axis=-1)
        chosen = jnp.any(topk_ids[:, :, None] == jnp.arange(EXPERTS), axis=1)
        gate_wts = jnp.where(chosen, ROUTE_SCALE * probs, -1.0).T
        ball, wsb, rank, counts, pt, shared_out = gather_call(normed, gate_wts, w1_shared, w3_shared, w2_shared)
        cnt = counts[:, :, 0]
        me = lax.axis_index('ep')
        chip, at = me // 2, jnp.arange(NSB)
        other_x, other_y = at % 2 != chip % 2, at // 2 != chip // 2
        place = jnp.where(other_x, jnp.where(other_y, 2, 1), jnp.where(other_y, 3, 0))
        core = jnp.concatenate([(me % 2)[None], place]).astype(jnp.int32)
        h, table = up_call(cnt, rank, ball, w1_experts, w3_experts)
        mine, theirs = down_call(table, cnt, core, rank, wsb, h, w2_experts)
        return return_call(table, pt, h, w2_experts, mine, theirs, hidden, shared_out)

    return jax.shard_map(local_fn, mesh=mesh, in_specs=(tok_spec, P(), P(), P(), P(), P(), expert_spec, expert_spec, expert_spec, tok_spec), out_specs=tok_spec, check_vma=False)
```

```python
import functools

import jax
import jax.numpy as jnp
from jax import lax
from jax.experimental import pallas as pl
from jax.experimental.pallas import tpu as pltpu
from jax.sharding import PartitionSpec as P

ROUTE_SCALE = 16
NORM_EPS = 1e-6
D = 2560
FF = 1536
EXPERTS = 64
NE = 8
NSB = 4
SB = 512
G = 16
TM = 256
LM = 384
SIZES = tuple(range(64, LM + 1, 64))
XG = 440
XR = XG * G
SBR = 1792
FC = 512
NF = FF // FC
DH = D // 2
T = 256
SHARED = 3072
SF = 256
CW = 512
RC = 256
NC = D // RC
KC = 768
HR = 1280
NK = KC // G
NOROW = NE * LM // G
WS = 4
LAG = 2
VMEM_LIMIT = 66000000
BF16 = jnp.bfloat16
F32 = jnp.float32


def offsets(cnt_ref, ng, eoff, est, boff, nsb_g):
    run = jnp.int32(0)
    for e in range(NE):
        est[e] = run
        for s in range(NSB):
            n = (cnt_ref[s, e] + (G - 1)) // G
            ng[s * NE + e] = n
            eoff[s * NE + e] = run
            run = run + n
    est[NE] = run
    for s in range(NSB):
        b = jnp.int32(0)
        for e in range(NE):
            boff[s * NE + e] = b
            b = b + ng[s * NE + e]
        nsb_g[s] = b


def up_kernel(cnt_ref, rank_ref, ball, w1, w3, h_out, table, xs, bbuf, pbuf, tbuf, wbuf, hbuf, ng, eoff, est, boff, nsb_g, dst, last, bsem, wsem, hsem):
    def w_copies(step, slot):
        e = step // NF
        f = step % NF
        cols = pl.ds(pl.multiple_of(f * FC, FC), FC)
        return (pltpu.make_async_copy(w1.at[e, :, cols], wbuf.at[slot, 0], wsem.at[slot, 0]),
                pltpu.make_async_copy(w3.at[e, :, cols], wbuf.at[slot, 1], wsem.at[slot, 1]))

    def b_copy(s, half):
        return pltpu.make_async_copy(ball.at[pl.ds(s * SB, SB), pl.ds(half * DH, DH)], bbuf.at[half], bsem.at[half])

    b_copy(0, 0).start()
    b_copy(0, 1).start()
    for st in range(3):
        for c in w_copies(st, st):
            c.start()
    offsets(cnt_ref, ng, eoff, est, boff, nsb_g)
    rows16 = lax.broadcasted_iota(jnp.int32, (G, SB), 0)

    for s in range(NSB):
        for e in range(NE):
            rk = jnp.broadcast_to(rank_ref[s, e:e + 1, :], (G, SB))

            def build(g, _, s=s, e=e, rk=rk):
                k = boff[s * NE + e] + g
                dst[k] = eoff[s * NE + e] + g
                hit = jnp.where(rk == rows16 + g * G, 1.0, 0.0)
                pbuf[pl.ds(pl.multiple_of(k * G, G), G), :] = hit.astype(BF16)
                return 0

            lax.fori_loop(0, ng[s * NE + e], build, 0)
        for half in range(2):
            b_copy(s, half).wait()

            def tile(m, _, s=s, half=half):
                prow = pbuf[pl.ds(pl.multiple_of(m * TM, TM), TM), :]
                for n in range(5):
                    cols = slice(n * 256, (n + 1) * 256)
                    tbuf[:, cols] = jnp.dot(prow, bbuf[half, :, cols], preferred_element_type=F32).astype(BF16)

                def put(j, _):
                    row = pl.multiple_of(dst[m * (TM // G) + j] * G, G)
                    xs[pl.ds(row, G), half * DH:(half + 1) * DH] = tbuf[pl.ds(pl.multiple_of(j * G, G), G), :]
                    return 0

                lax.fori_loop(0, jnp.minimum(TM // G, nsb_g[s] - m * (TM // G)), put, 0)
                return 0

            lax.fori_loop(0, (nsb_g[s] + TM // G - 1) // (TM // G), tile, 0)
            if s + 1 < NSB:
                b_copy(s + 1, half).start()

    def fill(k, _):
        table[k] = NOROW
        return 0

    lax.fori_loop(0, NSB * NK, fill, 0)
    over = jnp.int32(0)
    for e in range(NE):
        over = jnp.maximum(over, est[e + 1] - est[e] - LM // G)
    for s in range(NSB):
        over = jnp.maximum(over, nsb_g[s] - NK)
    table[NSB * NK] = over

    def segment(q, _):
        s, e = q // NE, q % NE
        first = eoff[q] - est[e]

        def one(g, _):
            k = boff[q] + g

            @pl.when((k < NK) & (first + g < LM // G))
            def _():
                table[s * NK + k] = e * (LM // G) + first + g

            return 0

        return lax.fori_loop(0, ng[q], one, 0)

    lax.fori_loop(0, NSB * NE, segment, 0)

    def h_copy(hs, e, row, col, size):
        return pltpu.make_async_copy(hbuf.at[hs, pl.ds(0, size), :], h_out.at[e, pl.ds(row, size), pl.ds(col, FC)], hsem.at[0])

    def wait_h(quarters):
        for q in range(1, LM // 64 + 1):
            @pl.when(quarters == q)
            def _(q=q):
                h_copy(0, 0, 0, 0, q * 64).wait()

    def step(st, k):
        slot = lax.rem(st, 3)
        e = st // NF
        col = pl.multiple_of((st % NF) * FC, FC)
        for c in w_copies(st, slot):
            c.wait()
        base = est[e] * G
        rows = est[e + 1] * G - base

        def work(row, size, k):
            row = pl.multiple_of(row, G)
            hs = k % 2
            for n in range(FC // 256):
                cols = slice(n * 256, (n + 1) * 256)
                x = xs[pl.ds(row, size), :]
                gate = jnp.dot(x, wbuf[slot, 0, :, cols], preferred_element_type=F32)
                lin = jnp.dot(x, wbuf[slot, 1, :, cols], preferred_element_type=F32)
                hbuf[hs, pl.ds(0, size), cols] = (jax.nn.silu(gate) * lin).astype(BF16)

            @pl.when(k > 0)
            def _():
                wait_h(last[0])

            last[0] = size // 64
            h_copy(hs, e, pl.multiple_of(row - base, G), col, size).start()

        full = jnp.maximum(rows - LM + TM - 1, 0) // TM

        def body(m, k):
            work(base + m * TM, TM, k)
            return k + 1

        k = lax.fori_loop(0, full, body, k)
        rem = rows - full * TM
        at = base + full * TM
        for size in SIZES:
            @pl.when((rem > size - 64) & (rem <= size))
            def _(size=size):
                work(at, size, k)

        @pl.when(st + 3 < NE * NF)
        def _():
            for c in w_copies(st + 3, slot):
                c.start()

        return k + jnp.where(rem > 0, 1, 0)

    @pl.when(lax.fori_loop(0, NE * NF, step, jnp.int32(0)) > 0)
    def _():
        wait_h(last[0])


def up_call(cnt, rank, ball, w1, w3):
    any_spec = pl.BlockSpec(memory_space=pl.ANY)
    return pl.pallas_call(
        up_kernel,
        out_shape=(jax.ShapeDtypeStruct((NE, HR, FF), BF16), jax.ShapeDtypeStruct((256,), jnp.int32)),
        in_specs=[pl.BlockSpec(memory_space=pltpu.SMEM), pl.BlockSpec(memory_space=pltpu.VMEM), any_spec, any_spec, any_spec],
        out_specs=(any_spec, pl.BlockSpec(memory_space=pltpu.SMEM)),
        scratch_shapes=[
            pltpu.VMEM((XR, D), BF16),
            pltpu.VMEM((2, SB, DH), BF16),
            pltpu.VMEM((SBR, SB), BF16),
            pltpu.VMEM((TM, DH), BF16),
            pltpu.VMEM((3, 2, D, FC), BF16),
            pltpu.VMEM((2, LM, FC), BF16),
            pltpu.SMEM((NSB * NE,), jnp.int32),
            pltpu.SMEM((NSB * NE,), jnp.int32),
            pltpu.SMEM((NE + 1,), jnp.int32),
            pltpu.SMEM((NSB * NE,), jnp.int32),
            pltpu.SMEM((NSB,), jnp.int32),
            pltpu.SMEM((SBR // G,), jnp.int32),
            pltpu.SMEM((1,), jnp.int32),
            pltpu.SemaphoreType.DMA((2,)),
            pltpu.SemaphoreType.DMA((3, 2)),
            pltpu.SemaphoreType.DMA((1,)),
        ],
        compiler_params=pltpu.CompilerParams(vmem_limit_bytes=VMEM_LIMIT),
        cost_estimate=pl.CostEstimate(flops=48_000_000_000, bytes_accessed=140_000_000, transcendentals=0),
        name="up",
    )(cnt, rank, ball, w1, w3)


def down_kernel(table, cnt_ref, core_ref, rank_ref, wt_ref, h, w2, mine, theirs, *scratch):
    @pl.when(table[NSB * NK] > 0)
    def _():
        down_all(cnt_ref, core_ref, rank_ref, wt_ref, h, w2, mine, theirs, *scratch)


def down_all(cnt_ref, core_ref, rank_ref, wt_ref, h, w2, mine, theirs,
                hs, ebuf, kbuf, pbuf, wbuf, abuf, wsplit, ng, eoff, est, boff, nsb_g, hsem, wsem, osem):
    steps = (D // CW) * NE

    def w_copy(st, slot):
        col = pl.multiple_of((st // NE) * CW, CW)
        return pltpu.make_async_copy(w2.at[st % NE, :, pl.ds(col, CW)], wbuf.at[slot], wsem.at[slot])

    for st in range(3):
        w_copy(st, st).start()
    offsets(cnt_ref, ng, eoff, est, boff, nsb_g)
    for e in range(NE):
        def fetch(m, _, e=e):
            to = pl.ds(pl.multiple_of(est[e] * G + m * TM, G), TM)
            copy = pltpu.make_async_copy(h.at[e, pl.ds(pl.multiple_of(m * TM, TM), TM), :], hs.at[to, :], hsem.at[0])
            copy.start()
            copy.wait()
            return 0

        lax.fori_loop(0, (est[e + 1] - est[e] + TM // G - 1) // (TM // G), fetch, 0)
    for s in range(NSB):
        w = wt_ref[s]
        hi = w.astype(BF16).astype(F32)
        mid = (w - hi).astype(BF16).astype(F32)
        wsplit[0, s] = hi
        wsplit[1, s] = mid
        wsplit[2, s] = w - hi - mid
    rows16 = lax.broadcasted_iota(jnp.int32, (G, SB), 0)
    for s in range(NSB):
        for e in range(NE):
            rk = jnp.broadcast_to(rank_ref[s, e:e + 1, :], (G, SB))
            parts = [jnp.broadcast_to(wsplit[i, s, e:e + 1, :], (G, SB)) for i in range(3)]

            def build(g, _, s=s, e=e, rk=rk, parts=parts):
                row = pl.multiple_of((boff[s * NE + e] + g) * G, G)
                hit = rk == rows16 + g * G
                for i in range(3):
                    pbuf[s, i, pl.ds(row, G), :] = jnp.where(hit, parts[i], 0.0).astype(BF16)
                return 0

            lax.fori_loop(0, ng[s * NE + e], build, 0)

        def clear(g, _, s=s):
            row = pl.multiple_of(g * G, G)
            for i in range(3):
                pbuf[s, i, pl.ds(row, G), :] = jnp.zeros((G, SB), BF16)
            return 0

        lax.fori_loop(nsb_g[s], -(-nsb_g[s] // (TM // G)) * (TM // G), clear, 0)
    kbuf[...] = jnp.zeros_like(kbuf)

    core = core_ref[0]

    def out_copies(c, s, slot):
        rel = core_ref[1 + s]
        keep = pl.multiple_of(core * 256, 256)
        give = pl.multiple_of(256 - core * 256, 256)
        out = []
        for i in range(CW // RC):
            cols = pl.ds(i * RC, RC)
            j = c * (CW // RC) + i
            out.append(pltpu.make_async_copy(abuf.at[slot, pl.ds(give, 256), cols], theirs.at[j, rel], osem.at[slot, i, 0]))
            out.append(pltpu.make_async_copy(abuf.at[slot, pl.ds(keep, 256), cols], mine.at[j, rel], osem.at[slot, i, 1]))
        return out

    def column(c, _):
        def expert(e, _):
            st = c * NE + e
            ws = st % 3
            w_copy(st, ws).wait()
            base = est[e] * G
            rows = est[e + 1] * G - base

            def work(row, size):
                row = pl.multiple_of(row, G)
                ebuf[pl.ds(row, size), :] = jnp.dot(hs[pl.ds(row, size), :], wbuf[ws], preferred_element_type=F32).astype(BF16)

            full = rows // TM

            def body(m, _):
                work(base + m * TM, TM)
                return 0

            lax.fori_loop(0, full, body, 0)
            rem = rows - full * TM
            for size in (128, 256):
                @pl.when((rem > size - 128) & (rem <= size))
                def _(size=size):
                    work(base + full * TM, size)

            @pl.when(st + 3 < steps)
            def _():
                w_copy(st + 3, ws).start()

            return 0

        lax.fori_loop(0, NE, expert, 0)

        def block(s, _):
            slot = s % 2

            def segment(e, _):
                def move(g, _):
                    row = pl.multiple_of((boff[s * NE + e] + g) * G, G)
                    src = pl.multiple_of((eoff[s * NE + e] + g) * G, G)
                    kbuf[pl.ds(row, G), :] = ebuf[pl.ds(src, G), :]
                    return 0

                return lax.fori_loop(0, ng[s * NE + e], move, 0)

            lax.fori_loop(0, NE, segment, 0)
            nk = (nsb_g[s] + TM // G - 1) // (TM // G)

            @pl.when(c * NSB + s >= 2)
            def _():
                for cp in out_copies(c, s, slot):
                    cp.wait()

            abuf[slot] = jnp.zeros((SB, CW), F32)

            def tile(kt, _):
                rows = pl.ds(pl.multiple_of(kt * TM, TM), TM)
                ek = kbuf[rows, :]
                for half in range(2):
                    toks = slice(half * 256, half * 256 + 256)
                    tot = abuf[slot, toks, :]
                    for i in range(3):
                        tot = tot + lax.dot_general(pbuf[s, i, rows, toks], ek, (((0,), (0,)), ((), ())), preferred_element_type=F32)
                    abuf[slot, toks, :] = tot
                return 0

            lax.fori_loop(0, nk, tile, 0)
            for cp in out_copies(c, s, slot):
                cp.start()
            return 0

        return lax.fori_loop(0, NSB, block, 0)

    lax.fori_loop(0, D // CW, column, 0)
    for s in (NSB - 2, NSB - 1):
        for cp in out_copies(D // CW - 1, s, s % 2):
            cp.wait()


def down_call(table, cnt, core, rank, wts, h, w2):
    any_spec = pl.BlockSpec(memory_space=pl.ANY)
    smem = pl.BlockSpec(memory_space=pltpu.SMEM)
    vmem = pl.BlockSpec(memory_space=pltpu.VMEM)
    out = jax.ShapeDtypeStruct((NC, NSB, 256, RC), F32)
    return pl.pallas_call(
        down_kernel,
        out_shape=(out, out),
        in_specs=[smem, smem, smem, vmem, vmem, any_spec, any_spec],
        out_specs=(any_spec, any_spec),
        scratch_shapes=[
            pltpu.VMEM((XR, FF), BF16),
            pltpu.VMEM((XR, CW), BF16),
            pltpu.VMEM((SBR, CW), BF16),
            pltpu.VMEM((NSB, 3, SBR, SB), BF16),
            pltpu.VMEM((3, FF, CW), BF16),
            pltpu.VMEM((2, SB, CW), F32),
            pltpu.VMEM((3, NSB, NE, SB), F32),
            pltpu.SMEM((NSB * NE,), jnp.int32),
            pltpu.SMEM((NSB * NE,), jnp.int32),
            pltpu.SMEM((NE + 1,), jnp.int32),
            pltpu.SMEM((NSB * NE,), jnp.int32),
            pltpu.SMEM((NSB,), jnp.int32),
            pltpu.SemaphoreType.DMA((1,)),
            pltpu.SemaphoreType.DMA((3,)),
            pltpu.SemaphoreType.DMA((2, CW // RC, 2)),
        ],
        compiler_params=pltpu.CompilerParams(vmem_limit_bytes=VMEM_LIMIT),
        cost_estimate=pl.CostEstimate(flops=40_000_000_000, bytes_accessed=100_000_000, transcendentals=0),
        name="down",
    )(table, cnt, core, rank, wts, h, w2)


def neighbours():
    me = lax.axis_index('ep')
    core = me + 1 - 2 * (me % 2)
    x = me + 2 - 4 * ((me // 2) % 2)
    y = me + 4 - 8 * (me // 4)
    return me, core, x, y


def remote(src, dst, send, recv, dev):
    return pltpu.make_async_remote_copy(src_ref=src, dst_ref=dst, send_sem=send, recv_sem=recv, device_id={'ep': dev}, device_id_type=pl.DeviceIdType.MESH)


def enter(others):
    barrier = pltpu.get_barrier_semaphore()
    for dev in others:
        pl.semaphore_signal(barrier, inc=1, device_id={'ep': dev}, device_id_type=pl.DeviceIdType.MESH)
    pl.semaphore_wait(barrier, len(others))


def gather_kernel(y_ref, gain_ref, wg_ref, ids_ref, w1, w3, w2, ball, wall_out, rank_ref, cnt_ref, pt, s_ref, b_ref, wts_ref, wall, ptbuf, cols_buf, w13buf, w2buf, acc, send, recv, wsend, wrecv, local, wsem, psem):
    me, pn, xn, yn = neighbours()
    diag = xn + yn - me
    half = T // 2

    def rows(dev, h):
        return pl.ds(pl.multiple_of(dev * T + h * half, half), half)

    def own(k, h, dev):
        return remote(b_ref.at[pl.ds(h * half, half), :], ball.at[rows(me, h), :], send.at[k], recv.at[k], dev)

    def relay(k, owner, h, dev):
        return remote(ball.at[rows(owner, h), :], ball.at[rows(owner, h), :], send.at[k], recv.at[k], dev)

    def w_copies(st, slot):
        cols = pl.ds(pl.multiple_of(st * SF, SF), SF)
        return (pltpu.make_async_copy(w1.at[:, cols], w13buf.at[slot, 0], wsem.at[slot, 0]),
                pltpu.make_async_copy(w3.at[:, cols], w13buf.at[slot, 1], wsem.at[slot, 1]),
                pltpu.make_async_copy(w2.at[cols, :], w2buf.at[slot], wsem.at[slot, 2]))

    for st in range(3):
        for c in w_copies(st, st):
            c.start()
    def norm(i, _):
        block = pl.ds(pl.multiple_of(i * 16, 16), 16)
        rows_f = y_ref[block, :].astype(F32)
        inv_rms = lax.rsqrt(jnp.mean(rows_f * rows_f, axis=-1, keepdims=True) + NORM_EPS)
        b_ref[block, :] = (rows_f * inv_rms * gain_ref[...].astype(F32)).astype(BF16)
        return 0

    lax.fori_loop(0, T // 16, norm, 0)
    logits = jnp.dot(b_ref[...], wg_ref[...], preferred_element_type=F32)
    raised = jnp.exp(logits - jnp.max(logits, axis=-1, keepdims=True))
    probs = raised / jnp.sum(raised, axis=-1, keepdims=True)
    ids = ids_ref[...]
    expert_id = lax.broadcasted_iota(jnp.int32, (T, EXPERTS), 1)
    chosen = ids[:, 0:1] == expert_id
    for k in range(1, ids.shape[1]):
        chosen = chosen | (ids[:, k:k + 1] == expert_id)
    gate_wts = jnp.where(chosen, ROUTE_SCALE * probs, -1.0)
    wts_ref[...] = jnp.concatenate([gate_wts, gate_wts], axis=1).T[:EXPERTS]
    others = [lax.rem(me + k, 8) for k in range(1, 8)]
    enter(others)
    first = [own(0, 0, xn), own(2, 1, yn), own(1, 1, xn), own(3, 0, yn), own(4, 0, pn), own(5, 1, pn)]
    for c in first:
        c.start()
    lanes = pl.ds(pl.multiple_of((me % 2) * T, T), T)
    small = []
    for k, dev in enumerate(others):
        small.append(remote(wts_ref.at[pl.ds(pl.multiple_of(dev * NE, NE), NE), :], wall.at[me // 2, :, lanes], wsend.at[k], wrecv.at[k], dev))
        small[-1].start()
    keep = [pltpu.make_async_copy(b_ref, ball.at[pl.ds(pl.multiple_of(me * T, T), T), :], local.at[0]),
            pltpu.make_async_copy(wts_ref.at[pl.ds(pl.multiple_of(me * NE, NE), NE), :], wall.at[me // 2, :, lanes], local.at[1])]
    for c in keep:
        c.start()
    acc[...] = jnp.zeros_like(acc)

    def step(st, _):
        slot = lax.rem(st, 3)
        for c in w_copies(st, slot):
            c.wait()
        x = b_ref[...]
        gate = jnp.dot(x, w13buf[slot, 0], preferred_element_type=F32)
        lin = jnp.dot(x, w13buf[slot, 1], preferred_element_type=F32)
        inner = (jax.nn.silu(gate) * lin).astype(BF16)
        for n in range(D // 512):
            cols = slice(n * 512, n * 512 + 512)
            acc[:, cols] += jnp.dot(inner, w2buf[slot, :, cols], preferred_element_type=F32)

        return 0

    def refill(st, _):
        step(st, 0)
        for c in w_copies(st + 3, lax.rem(st, 3)):
            c.start()
        return 0

    lax.fori_loop(0, 8, refill, 0)
    first[0].wait_recv()
    first[1].wait_recv()
    second = [relay(6, xn, 0, yn), relay(7, yn, 1, xn), relay(8, xn, 0, pn), relay(9, yn, 1, pn)]
    for c in second:
        c.start()
    lax.fori_loop(8, SHARED // SF - 3, refill, 0)
    lax.fori_loop(SHARED // SF - 3, SHARED // SF, step, 0)
    s_ref[...] = acc[...].astype(BF16)
    first[2].wait_recv()
    first[3].wait_recv()
    third = [relay(10, xn, 1, pn), relay(11, yn, 0, pn)]
    for c in third:
        c.start()
    for c in small:
        c.wait_recv()
    keep[1].wait()
    before = jnp.where(lax.broadcasted_iota(jnp.int32, (SB, SB), 0) < lax.broadcasted_iota(jnp.int32, (SB, SB), 1), 1.0, 0.0).astype(BF16)
    row = lax.broadcasted_iota(jnp.int32, (1, KC), 1)
    puts = []
    for s in range(NSB):
        slot = s % 2
        w = wall[s]
        wall_out[s] = w
        sel = jnp.where(w >= 0.0, 1.0, 0.0)
        rank = jnp.where(w >= 0.0, jnp.dot(sel.astype(BF16), before, preferred_element_type=F32), -1.0)
        rank_ref[s] = rank.astype(jnp.int32)
        count = jnp.sum(sel, axis=1, keepdims=True).astype(jnp.int32)
        cnt_ref[s] = jnp.broadcast_to(count, (NE, 128))
        wide = jnp.broadcast_to(count, (NE, KC))
        start = jnp.zeros((1, KC), jnp.int32)
        local_row = []
        for e in range(NE):
            n = wide[e:e + 1]
            at = row - start
            local_row.append(jnp.where((at >= 0) & (at < n), at, -2).astype(F32))
            start = start + (n + (G - 1)) // G * G
        pad = jnp.zeros((128 - NE, SB), F32)
        cols_buf[0] = jnp.concatenate([rank, pad], axis=0).T
        cols_buf[1] = jnp.concatenate([w, pad], axis=0).T
        if s >= 2:
            puts[s - 2].wait()

        def fill(tb, _, slot=slot, local_row=local_row):
            toks = pl.ds(pl.multiple_of(tb * 32, 32), 32)
            rk = cols_buf[0, toks, :]
            wt = cols_buf[1, toks, :]
            total = jnp.zeros((32, KC), F32)
            for e in range(NE):
                total = jnp.where(rk[:, e:e + 1] == local_row[e], wt[:, e:e + 1], total)
            hi = total.astype(BF16)
            rest = total - hi.astype(F32)
            mid = rest.astype(BF16)
            ptbuf[slot, 0, toks, :] = hi
            ptbuf[slot, 1, toks, :] = mid
            ptbuf[slot, 2, toks, :] = (rest - mid.astype(F32)).astype(BF16)
            return 0

        lax.fori_loop(0, SB // 32, fill, 0)
        puts.append(pltpu.make_async_copy(ptbuf.at[slot], pt.at[s], psem.at[slot]))
        puts[s].start()
    second[0].wait_recv()
    second[1].wait_recv()
    fourth = [relay(12, diag, 0, pn), relay(13, diag, 1, pn)]
    for c in fourth:
        c.start()
    for c in (first[4], first[5], second[2], second[3], *third, *fourth):
        c.wait_recv()
    for c in (*first, *second, *third, *fourth):
        c.wait_send()
    for c in small:
        c.wait_send()
    keep[0].wait()
    puts[2].wait()
    puts[3].wait()


def gather_call(y, gain, wg, ids, w1, w3, w2):
    any_spec = pl.BlockSpec(memory_space=pl.ANY)
    vmem = pl.BlockSpec(memory_space=pltpu.VMEM)
    return pl.pallas_call(
        gather_kernel,
        out_shape=(
            jax.ShapeDtypeStruct((8 * T, D), BF16),
            jax.ShapeDtypeStruct((NSB, NE, SB), F32),
            jax.ShapeDtypeStruct((NSB, NE, SB), jnp.int32),
            jax.ShapeDtypeStruct((NSB, NE, 128), jnp.int32),
            jax.ShapeDtypeStruct((NSB, 3, SB, KC), BF16),
            jax.ShapeDtypeStruct((T, D), BF16),
        ),
        in_specs=[vmem, vmem, vmem, vmem, any_spec, any_spec, any_spec],
        out_specs=(any_spec, vmem, vmem, vmem, any_spec, vmem),
        scratch_shapes=[
            pltpu.VMEM((T, D), BF16),
            pltpu.VMEM((EXPERTS, T), F32),
            pltpu.VMEM((NSB, NE, SB), F32),
            pltpu.VMEM((2, 3, SB, KC), BF16),
            pltpu.VMEM((2, SB, 128), F32),
            pltpu.VMEM((3, 2, D, SF), BF16),
            pltpu.VMEM((3, SF, D), BF16),
            pltpu.VMEM((T, D), F32),
            pltpu.SemaphoreType.DMA((14,)),
            pltpu.SemaphoreType.DMA((14,)),
            pltpu.SemaphoreType.DMA((7,)),
            pltpu.SemaphoreType.DMA((7,)),
            pltpu.SemaphoreType.DMA((2,)),
            pltpu.SemaphoreType.DMA((3, 3)),
            pltpu.SemaphoreType.DMA((2,)),
        ],
        compiler_params=pltpu.CompilerParams(collective_id=0, has_side_effects=True, vmem_limit_bytes=VMEM_LIMIT),
        cost_estimate=pl.CostEstimate(flops=12_000_000_000, bytes_accessed=60_000_000, transcendentals=0),
        name="gather",
    )(y, gain, wg, ids, w1, w3, w2)


def return_kernel(table, pt, h, w2, mine, theirs, y_ref, s_ref, out_ref, ptv, hv, wbuf, ebuf, kbuf, own, give, r1, r2x, r2y, r3x, r3y, send, recv, load, wsem, hsem, psem):
    me, pn, xn, yn = neighbours()
    half = T // 2
    top, low = pl.ds(0, half), pl.ds(half, half)

    def load_of(j):
        return (pltpu.make_async_copy(theirs.at[j], give.at[lax.rem(j, 3)], load.at[0, j]), pltpu.make_async_copy(mine.at[j], own.at[j], load.at[1, j]))

    def w_of(st):
        cols = pl.ds(pl.multiple_of((st // NE) * RC, RC), RC)
        return pltpu.make_async_copy(w2.at[lax.rem(st, NE), :, cols], wbuf.at[lax.rem(st, WS)], wsem.at[lax.rem(st, WS)])

    def core_of(j):
        return remote(give.at[lax.rem(j, 3)], r1.at[j], send.at[0, j], recv.at[0, j], pn)

    def x_of(j):
        return remote(own.at[j, pl.ds(1, 2), top, :], r2x.at[j], send.at[1, j], recv.at[1, j], xn)

    def y_of(j):
        return remote(own.at[j, pl.ds(2, 2), low, :], r2y.at[j], send.at[2, j], recv.at[2, j], yn)

    def y_last(j):
        return remote(own.at[j, 3, top, :], r3y.at[j], send.at[3, j], recv.at[3, j], yn)

    def x_last(j):
        return remote(own.at[j, 1, low, :], r3x.at[j], send.at[4, j], recv.at[4, j], xn)

    def each(body):
        def run(j, _):
            body(j)
            return 0

        lax.fori_loop(0, NC, run, 0)

    over = jnp.full((T, RC), table[NSB * NK], jnp.int32) > 0

    def begin(j):
        for c in load_of(j):
            c.start()

    def add_up(buf, at, first_tok):
        toks = pl.ds(pl.multiple_of(first_tok, T), T)

        def block(s, _):
            dx = lax.rem(lax.rem(s, 2) + lax.rem(me // 2, 2), 2)
            dy = lax.rem(s // 2 + me // 4, 2)
            place = dx + 3 * dy - 2 * dx * dy
            ek = kbuf[pl.ds(pl.multiple_of(s * KC, KC), KC), :]
            total = jnp.dot(ptv[s, 0, toks, :], ek, preferred_element_type=F32)
            for i in range(1, 3):
                total = total + jnp.dot(ptv[s, i, toks, :], ek, preferred_element_type=F32)
            buf[at, place] = jnp.where(over, buf[at, place], total)
            return 0

        lax.fori_loop(0, NSB, block, 0)

    def make(j):
        def expert(e, _):
            st = j * NE + e

            @pl.when(j == 0)
            def _():
                h_of(e).wait()

            w_of(st).wait()
            res = jnp.dot(hv[e], wbuf[lax.rem(st, WS)], preferred_element_type=F32).astype(BF16)
            ebuf[pl.ds(e * (LM // G), LM // G)] = res.reshape(LM // G, G, RC)

            @pl.when(st + WS < NC * NE)
            def _():
                w_of(st + WS).start()

            return 0

        lax.fori_loop(0, NE, expert, 0)

        def move(k, _):
            for i in range(8):
                kbuf[pl.ds(pl.multiple_of((k * 8 + i) * G, G), G), :] = ebuf[table[k * 8 + i]]
            return 0

        lax.fori_loop(0, NSB * NK // 8, move, 0)

        @pl.when(j == 0)
        def _():
            for c in pt_copies:
                c.wait()

        for c in load_of(j):
            c.wait()
        add_up(give, lax.rem(j, 3), T - lax.rem(me, 2) * T)
        core_of(j).start()
        add_up(own, j, lax.rem(me, 2) * T)

    def pair(j):
        core_of(j).wait_recv()
        own[j, 1:] = own[j, 1:] + r1[j, 1:]
        x_of(j).start()
        y_of(j).start()
        own[j, 0] = own[j, 0] + r1[j, 0]

    def onward(j):
        x_of(j).wait_recv()
        own[j, 3, :half] = own[j, 3, :half] + r2x[j, 1]
        y_last(j).start()
        y_of(j).wait_recv()
        own[j, 1, half:] = own[j, 1, half:] + r2y[j, 0]
        x_last(j).start()

    def finish(j):
        cols = pl.ds(pl.multiple_of(j * RC, RC), RC)
        y_last(j).wait_recv()
        x_last(j).wait_recv()
        base = y_ref[:, cols].astype(F32) + s_ref[:, cols].astype(F32)
        out_ref[:half, cols] = (base[:half] + (own[j, 0, :half] + r2x[j, 0] + r3y[j])).astype(BF16)
        out_ref[half:, cols] = (base[half:] + (own[j, 0, half:] + r2y[j, 1] + r3x[j])).astype(BF16)

    def drain(j):
        for c in (x_of(j), y_of(j), y_last(j), x_last(j)):
            c.wait_send()

    def h_of(e):
        return pltpu.make_async_copy(h.at[e, pl.ds(0, LM), :], hv.at[e], hsem.at[e])

    pt_copies = [pltpu.make_async_copy(pt.at[s], ptv.at[s], psem.at[s]) for s in range(NSB)]
    for e in range(NE):
        h_of(e).start()
        if e < WS:
            w_of(e).start()
    begin(0)
    begin(1)
    for c in pt_copies:
        c.start()
    ebuf[NOROW] = jnp.zeros((G, RC), BF16)
    enter([pn, xn, yn])

    def steady(j, _):
        @pl.when(j >= 2)
        def _():
            core_of(j - 2).wait_send()

        @pl.when((j >= 1) & (j + 1 < NC))
        def _():
            begin(j + 1)

        make(j)
        pair(j)

        @pl.when(j >= LAG)
        def _():
            onward(j - LAG)

        return 0

    lax.fori_loop(0, NC, steady, 0)

    def last(j, _):
        core_of(j).wait_send()
        onward(j)
        return 0

    lax.fori_loop(NC - LAG, NC, last, 0)
    each(finish)
    each(drain)


def return_call(table, pt, h, w2, mine, theirs, hidden, shared_out):
    any_spec = pl.BlockSpec(memory_space=pl.ANY)
    vmem = pl.BlockSpec(memory_space=pltpu.VMEM)
    half = T // 2
    return pl.pallas_call(
        return_kernel,
        out_shape=jax.ShapeDtypeStruct((T, D), BF16),
        in_specs=[pl.BlockSpec(memory_space=pltpu.SMEM), any_spec, any_spec, any_spec, any_spec, any_spec, vmem, vmem],
        out_specs=vmem,
        scratch_shapes=[
            pltpu.VMEM((NSB, 3, SB, KC), BF16),
            pltpu.VMEM((NE, LM, FF), BF16),
            pltpu.VMEM((WS, FF, RC), BF16),
            pltpu.VMEM((NOROW + 1, G, RC), BF16),
            pltpu.VMEM((NSB * KC, RC), BF16),
            pltpu.VMEM((NC, NSB, T, RC), F32),
            pltpu.VMEM((3, NSB, T, RC), F32),
            pltpu.VMEM((NC, NSB, T, RC), F32),
            pltpu.VMEM((NC, 2, half, RC), F32),
            pltpu.VMEM((NC, 2, half, RC), F32),
            pltpu.VMEM((NC, half, RC), F32),
            pltpu.VMEM((NC, half, RC), F32),
            pltpu.SemaphoreType.DMA((5, NC)),
            pltpu.SemaphoreType.DMA((5, NC)),
            pltpu.SemaphoreType.DMA((2, NC)),
            pltpu.SemaphoreType.DMA((WS,)),
            pltpu.SemaphoreType.DMA((NE,)),
            pltpu.SemaphoreType.DMA((NSB,)),
        ],
        compiler_params=pltpu.CompilerParams(collective_id=1, has_side_effects=True, vmem_limit_bytes=VMEM_LIMIT),
        name="return_sum",
    )(table, pt, h, w2, mine, theirs, hidden, shared_out)


def solution(mesh):
    tok_spec = P(('dp', 'ep'), None)
    expert_spec = P('ep', None, None)

    def local_fn(hidden, norm_gain, w_gate, w1_shared, w3_shared, w2_shared, w1_experts, w3_experts, w2_experts, topk_ids):
        ball, wsb, rank, counts, pt, shared_out = gather_call(hidden, norm_gain.reshape(1, D), w_gate, topk_ids, w1_shared, w3_shared, w2_shared)
        cnt = counts[:, :, 0]
        me = lax.axis_index('ep')
        chip, at = me // 2, jnp.arange(NSB)
        other_x, other_y = at % 2 != chip % 2, at // 2 != chip // 2
        place = jnp.where(other_x, jnp.where(other_y, 2, 1), jnp.where(other_y, 3, 0))
        core = jnp.concatenate([(me % 2)[None], place]).astype(jnp.int32)
        h, table = up_call(cnt, rank, ball, w1_experts, w3_experts)
        mine, theirs = down_call(table, cnt, core, rank, wsb, h, w2_experts)
        return return_call(table, pt, h, w2_experts, mine, theirs, hidden, shared_out)

    return jax.shard_map(local_fn, mesh=mesh, in_specs=(tok_spec, P(), P(), P(), P(), P(), expert_spec, expert_spec, expert_spec, tok_spec), out_specs=tok_spec, check_vma=False)
```
